128 devices in a mesh: tm: 16 (over z, y), roll: 8 (over x, core).
Axes of the slice: x: 4, y: 4, z: 4, core: 2. Of those that a mesh axis runs over, the one named last changes fastest.
Arguments:
- inputs: bfloat16 [8, 128, 32, 2048], P('roll', 'tm'), may hold values from -30 to 30
- cotangent: bfloat16 [8, 128, 32, 2048], P('roll', 'tm'), may hold values from -6 to 6
- memory_lists: int32 [8, 128, 8], P('roll', 'tm'), may hold values from -1 to 119, as said below
- w_query: bfloat16 [2048, 1024], replicated, may hold values from -1 to 1
- w_key: bfloat16 [2048, 1024], replicated, may hold values from -1 to 1
- w_value: bfloat16 [2048, 1024], replicated, may hold values from -0.125 to 0.125
- w_output: bfloat16 [1024, 2048], replicated, may hold values from -0.1875 to 0.1875
Outputs:
- attended: bfloat16 [8, 128, 32, 2048], P('roll', 'tm')
- grad_input: bfloat16 [8, 128, 32, 2048], P('roll', 'tm')
- grad_w_query: float32 [2048, 1024], P('tm')
- grad_w_key: float32 [2048, 1024], P('tm')
- grad_w_value: float32 [2048, 1024], P('tm')
- grad_w_output: float32 [1024, 2048], P('tm')
The draws below stay inside these ranges and needn't reach their ends.
Inputs may be any that keep to these rules, and one draw needn't show every extreme that they name: `memory_lists`: every entry is -1 or a frame of the same rollout that lies in an earlier block of 8 frames and before frame f - 4. The frames named in one list differ, and -1 entries come after them. The frames of one block name at most 3 distinct frames of any other block, and exactly 3 of the block just before theirs.
All inputs are finite; a program needn't handle non-finite values.
Results may differ from the reference program's by a relative error of at most 0.02.
Values may be sent and summed in bfloat16 or wider, within the bound.
No kernel may reach another device: no remote copies, remote signals or barrier semaphores. Data moves between devices by JAX's collectives and lax.ppermute only.
A program may use at most 192 MiB of HBM per device.

```python
import jax
import jax.numpy as jnp
from jax import lax

D = 2048
HEADS = 8
HEAD = 128
TPF = 32
BAND = 4
MEM = 8
CAP = 3
FR_DEV = 8
HD = 1024
FRAMES = 128
ROLLOUTS = 8
N_TM = 16


def draw_inputs(key, part):
    normal_rows = jax.random.normal(jax.random.fold_in(key, 3), (ROLLOUTS, FRAMES, TPF, D), jnp.float32)
    normal_rows = jnp.clip(normal_rows, -6.0, 6.0)
    return normal_rows.astype(jnp.bfloat16)


def projection_pair(key):
    former = jnp.clip(jax.random.normal(jax.random.fold_in(key, 21), (D, HD), jnp.float32), -4.0, 4.0)
    latter = jnp.clip(jax.random.normal(jax.random.fold_in(key, 22), (D, HD), jnp.float32), -4.0, 4.0)
    return (former * D ** (-0.5), latter * D ** (-0.5))


def draw_w_query(key, part):
    former, latter = projection_pair(key)
    return former.astype(jnp.bfloat16)


def draw_w_key(key, part):
    former, latter = projection_pair(key)
    blended = latter
    return blended.astype(jnp.bfloat16)


def one_rollout(key):
    blocks = FRAMES // FR_DEV
    frame = jnp.arange(FRAMES, dtype=jnp.int32)
    block_of = frame // FR_DEV
    within = frame % FR_DEV
    noise = jax.random.randint(jax.random.fold_in(key, 31), (blocks, blocks, FR_DEV), 0, 4096) * FR_DEV
    noise = noise + jnp.arange(FR_DEV, dtype=jnp.int32)
    ordering = jnp.argsort(noise, axis=2)
    chosen = jnp.argsort(ordering, axis=2) < CAP
    allowed = chosen[block_of[:, None], block_of[None, :], within[None, :]]
    allowed = allowed & (block_of[None, :] < block_of[:, None]) & (frame[None, :] < frame[:, None] - BAND)
    forced = allowed & (block_of[None, :] == block_of[:, None] - 1) & (within[:, None] == FR_DEV - 1)
    ranking = jax.random.randint(jax.random.fold_in(key, 32), (FRAMES, FRAMES), 0, 65536) * FRAMES
    ranking = ranking + frame[None, :] + forced.astype(jnp.int32) * 2 ** 28
    ranking = jnp.where(allowed, ranking, -1)
    best, picked = lax.top_k(ranking, MEM)
    return jnp.where(best >= 0, picked, -1).astype(jnp.int32)


def draw_memory_lists(key, part):
    return jax.vmap(one_rollout)(jax.random.split(key, ROLLOUTS))


def block_levels(rng, dims, cuts, least, top_value):
    def one(position, parts):
        steps = jax.random.uniform(jax.random.fold_in(jax.random.fold_in(rng, 6), position), (parts,), jnp.float32, least / len(cuts), top_value / len(cuts))
        return jnp.repeat(jnp.exp(steps), dims[position] // parts).reshape((-1,) + (1,) * (len(dims) - position - 1))

    factor_of = one(*cuts[0])
    for cut in cuts[1:]:
        factor_of = factor_of * one(*cut)
    return factor_of


def scatter_about(rng, dims, width, most, cuts=(), held_as=jnp.bfloat16):
    result = jax.random.normal(rng, dims, jnp.float32) * width
    if len(cuts) > 0:
        result = block_levels(rng, dims, cuts, -0.22, 0.18) * result
    return jnp.clip(result, min=-most, max=most).astype(held_as)


def setup_inputs(seed: int = 0) -> dict:
    keys = jax.random.split(jax.random.key(seed), 8)
    return {
        "inputs": draw_inputs(jax.random.fold_in(keys[7], 71), 0),
        "cotangent": scatter_about(keys[1], (ROLLOUTS, FRAMES, TPF, D), 1.0, 6.0, ((0, 8), (1, 16))),
        "memory_lists": draw_memory_lists(jax.random.fold_in(keys[7], 71), 0),
        "w_query": draw_w_query(jax.random.fold_in(keys[7], 71), 0),
        "w_key": draw_w_key(jax.random.fold_in(keys[7], 71), 0),
        "w_value": scatter_about(keys[5], (D, HD), D ** -0.5, 0.125),
        "w_output": scatter_about(keys[6], (HD, D), HD ** -0.5, 0.1875),
    }


masked_score = -1e30


def to_half(values):
    return lax.optimization_barrier(values.astype(jnp.bfloat16))


def widen(values):
    return values.astype(jnp.float32)


def dot_last(left, right):
    return lax.dot_general(left, right, (((1,), (1,)), ((), ())), preferred_element_type=jnp.float32)


def dot_first(left, right):
    return lax.dot_general(left, right, (((0,), (0,)), ((), ())), preferred_element_type=jnp.float32)


def attend(queries, keyset, key_valid, grad_heads):
    frame_count, key_count, frame_tokens, double_width = keyset.shape
    inner_width = double_width // 2
    score_scale = HEAD ** -0.5
    query_f = widen(queries).reshape(frame_count, frame_tokens, HEADS, HEAD)
    key_f = widen(keyset[..., :inner_width]).reshape(frame_count, key_count * frame_tokens, HEADS, HEAD)
    value_f = widen(keyset[..., inner_width:]).reshape(frame_count, key_count * frame_tokens, HEADS, HEAD)
    grad_f = widen(grad_heads).reshape(frame_count, frame_tokens, HEADS, HEAD)
    scores = jnp.einsum("fqhe,fkhe->fhqk", query_f, key_f) * score_scale
    key_mask = jnp.repeat(key_valid, frame_tokens, axis=1)[:, None, None, :]
    scores = jnp.where(key_mask, scores, masked_score)
    row_max = jnp.max(scores, axis=-1, keepdims=True)
    weights = jnp.exp(scores - row_max)
    weights = weights / jnp.sum(weights, axis=-1, keepdims=True)
    rounded = widen(to_half(weights))
    heads_out = to_half(jnp.einsum("fhqk,fkhe->fqhe", rounded, value_f))
    grad_prob = jnp.einsum("fqhe,fkhe->fhqk", grad_f, value_f)
    row_dot = jnp.sum(weights * grad_prob, axis=-1, keepdims=True)
    dscore = widen(to_half(weights * (grad_prob - row_dot)))
    grad_query = to_half(jnp.einsum("fhqk,fkhe->fqhe", dscore, key_f) * score_scale)
    grad_keys = jnp.einsum("fhqk,fqhe->fkhe", dscore, query_f) * score_scale
    grad_values = jnp.einsum("fhqk,fqhe->fkhe", rounded, grad_f)
    block_shape = (frame_count, key_count, frame_tokens, inner_width)
    grad_keyval = jnp.concatenate([grad_keys.reshape(block_shape), grad_values.reshape(block_shape)], axis=-1)
    return (heads_out.reshape(frame_count, frame_tokens, inner_width),
            grad_query.reshape(frame_count, frame_tokens, inner_width), grad_keyval)


def rollout_pass(inputs, cotangent, recalled, w_query, w_key, w_value, w_output):
    row_count = FRAMES * TPF
    flat_input = inputs.reshape(row_count, D)
    grad_flat = cotangent.reshape(row_count, D)
    queries = to_half(jnp.dot(flat_input, w_query, preferred_element_type=jnp.float32)).reshape(FRAMES, TPF, HD)
    key_rows = to_half(jnp.dot(flat_input, w_key, preferred_element_type=jnp.float32))
    value_rows = to_half(jnp.dot(flat_input, w_value, preferred_element_type=jnp.float32))
    keyval = jnp.concatenate([key_rows, value_rows], axis=1).reshape(FRAMES, TPF, 2 * HD)
    grad_heads = to_half(dot_last(grad_flat, w_output)).reshape(FRAMES, TPF, HD)
    offsets = jnp.arange(BAND + 1, dtype=jnp.int32) - BAND

    def one_block(running, block_index):
        first_frame = (block_index * FR_DEV).astype(jnp.int32)
        frame_ids = first_frame + jnp.arange(FR_DEV, dtype=jnp.int32)
        band_ids = frame_ids[:, None] + offsets[None, :]
        memory_ids = lax.dynamic_slice_in_dim(recalled, first_frame, FR_DEV, 0).astype(jnp.int32)
        all_ids = jnp.concatenate([band_ids, memory_ids], axis=1)
        key_valid = all_ids >= 0
        safe_ids = jnp.where(key_valid, all_ids, 0).astype(jnp.int32)
        keyset = keyval[safe_ids]
        block_queries = lax.dynamic_slice_in_dim(queries, first_frame, FR_DEV, 0)
        block_grads = lax.dynamic_slice_in_dim(grad_heads, first_frame, FR_DEV, 0)
        heads_out, grad_query, grad_keyval = attend(block_queries, keyset, key_valid, block_grads)
        band_part = grad_keyval[:, :BAND + 1].reshape(FR_DEV * (BAND + 1), TPF, 2 * HD)
        band_target = safe_ids[:, :BAND + 1].reshape(-1)
        own_mask = (band_target >= first_frame)[:, None, None]
        own_sum = jax.ops.segment_sum(jnp.where(own_mask, band_part, 0.0), band_target, FRAMES)
        prev_sum = jax.ops.segment_sum(jnp.where(own_mask, 0.0, band_part), band_target, FRAMES)
        memory_part = grad_keyval[:, BAND + 1:].reshape(FR_DEV * MEM, TPF, 2 * HD)
        memory_sum = jax.ops.segment_sum(memory_part, safe_ids[:, BAND + 1:].reshape(-1), FRAMES)
        running = running + own_sum + widen(to_half(prev_sum)) + widen(to_half(memory_sum))
        return running, (heads_out, grad_query)

    start = jnp.zeros((FRAMES, TPF, 2 * HD), jnp.float32)
    summed, (outs, grads) = lax.scan(one_block, start, jnp.arange(N_TM, dtype=jnp.int32))
    keyval_grad = to_half(summed)
    heads_rows = outs.reshape(row_count, HD)
    grad_query = grads.reshape(row_count, HD)
    grad_keys = keyval_grad[..., :HD].reshape(row_count, HD)
    grad_values = keyval_grad[..., HD:].reshape(row_count, HD)
    grad_input = to_half(dot_last(grad_query, w_query) + dot_last(grad_keys, w_key) + dot_last(grad_values, w_value))
    attended = to_half(jnp.dot(heads_rows, w_output, preferred_element_type=jnp.float32))
    rows_block = FR_DEV * TPF

    def block_grads(running, pieces):
        piece_input, piece_query, piece_keys, piece_values, piece_heads, piece_grad = pieces
        partials = (dot_first(piece_input, piece_query), dot_first(piece_input, piece_keys),
                    dot_first(piece_input, piece_values), dot_first(piece_heads, piece_grad))
        return tuple(total + widen(to_half(term)) for total, term in zip(running, partials)), None

    zero_in = jnp.zeros((D, HD), jnp.float32)
    zero_out = jnp.zeros((HD, D), jnp.float32)
    stacked = (flat_input.reshape(N_TM, rows_block, D), grad_query.reshape(N_TM, rows_block, HD),
               grad_keys.reshape(N_TM, rows_block, HD), grad_values.reshape(N_TM, rows_block, HD),
               heads_rows.reshape(N_TM, rows_block, HD), grad_flat.reshape(N_TM, rows_block, D))
    weight_grads, unused = lax.scan(block_grads, (zero_in, zero_in, zero_in, zero_out), stacked)
    return (attended.reshape(FRAMES, TPF, D), grad_input.reshape(FRAMES, TPF, D), weight_grads)


def reference(inputs, cotangent, memory_lists, w_query, w_key, w_value, w_output):
    zero_in = jnp.zeros((D, HD), jnp.float32)
    zero_out = jnp.zeros((HD, D), jnp.float32)

    def per_rollout(running, pieces):
        piece_input, piece_grad, recalled = pieces
        attended, grad_input, weight_grads = rollout_pass(piece_input, piece_grad, recalled,
                                                          w_query, w_key, w_value, w_output)
        return tuple(total + term for total, term in zip(running, weight_grads)), (attended, grad_input)

    totals, (attended, grad_input) = lax.scan(per_rollout, (zero_in, zero_in, zero_in, zero_out),
                                              (inputs, cotangent, memory_lists))
    return attended, grad_input, totals[0], totals[1], totals[2], totals[3]
```

```python
import functools

import jax
import jax.numpy as jnp
from jax import lax
from jax.experimental import pallas as pl
from jax.experimental.pallas import tpu as pltpu
from jax.sharding import PartitionSpec as P

HEADS = 8
HEAD = 128
BAND = 4
MEM = 8
CAP = 3
FRAMES = 8
TOK = 32
BLOCKS = 16
ROWS = FRAMES * TOK
SPARE = BLOCKS * CAP
masked_score = -1e30
f32, bf16 = jnp.float32, jnp.bfloat16
VMEM_LIMIT = 60 * 1024 * 1024


def params(n=1):
    return pltpu.CompilerParams(
        dimension_semantics=("arbitrary",) * n, vmem_limit_bytes=VMEM_LIMIT
    )


def dot_last(left, right):
    return lax.dot_general(left, right, (((1,), (1,)), ((), ())), preferred_element_type=f32)


def dot_first(left, right):
    return lax.dot_general(left, right, (((0,), (0,)), ((), ())), preferred_element_type=f32)


def dot(left, right):
    return lax.dot_general(left, right, (((1,), (0,)), ((), ())), preferred_element_type=f32)


def keyval_body(x_ref, wk_ref, wv_ref, out_ref):
    pieces = []
    for h in range(wk_ref.shape[1] // HEAD):
        pieces += [wk_ref[:, h * HEAD : (h + 1) * HEAD], wv_ref[:, h * HEAD : (h + 1) * HEAD]]
    out_ref[...] = dot(x_ref[...], jnp.concatenate(pieces, axis=1)).astype(bf16)


def keyval_rows(x, w_key, w_value):
    rows, width = x.shape
    inner = w_key.shape[1]
    cols = 256
    return pl.pallas_call(
        keyval_body,
        grid=(inner // cols,),
        in_specs=[
            pl.BlockSpec((rows, width), lambda j: (0, 0)),
            pl.BlockSpec((width, cols), lambda j: (0, j)),
            pl.BlockSpec((width, cols), lambda j: (0, j)),
        ],
        out_specs=pl.BlockSpec((rows, 2 * cols), lambda j: (0, j)),
        out_shape=jax.ShapeDtypeStruct((rows, 2 * inner), bf16),
        compiler_params=params(),
        name="keyval",
    )(x, w_key, w_value)


def send_body(pick_ref, kv_ref, out_ref, sem):
    def copy(i):
        at = pl.multiple_of(pick_ref[i] * TOK, TOK)
        return pltpu.make_async_copy(
            kv_ref.at[pl.ds(at, TOK), :], out_ref.at[pl.ds(i * TOK, TOK), :], sem.at[i]
        )

    for i in range(BLOCKS * CAP):
        copy(i).start()
    for i in range(BLOCKS * CAP):
        copy(i).wait()


def named_frames(pick, kv):
    rows, width = kv.shape
    return pl.pallas_call(
        send_body,
        grid_spec=pltpu.PrefetchScalarGridSpec(
            num_scalar_prefetch=1,
            grid=(1,),
            in_specs=[pl.BlockSpec((rows, width), lambda i, *_: (0, 0))],
            out_specs=pl.BlockSpec(memory_space=pl.ANY),
            scratch_shapes=[pltpu.SemaphoreType.DMA((BLOCKS * CAP,))],
        ),
        out_shape=jax.ShapeDtypeStruct((BLOCKS * CAP * TOK, width), bf16),
        compiler_params=params(),
        name="send",
    )(pick, kv)


def attend_body(
    read_ref, add_ref, bias_ref, q_ref, g_ref, own_ref, prev_ref, slot_ref,
    o_ref, dq_ref, down_ref, rim_ref, dslot_ref, acc_own, acc_prev, acc_slot,
):
    scale = HEAD ** (-0.5)
    acc_own[...] = jnp.zeros_like(acc_own)
    acc_prev[...] = jnp.zeros_like(acc_prev)
    acc_slot[...] = jnp.zeros_like(acc_slot)
    for f in range(FRAMES):
        rows = slice(f * TOK, (f + 1) * TOK)
        pieces = []
        if f < BAND:
            pieces.append(prev_ref[f * TOK : BAND * TOK, :])
        pieces.append(own_ref[max(f - BAND, 0) * TOK : (f + 1) * TOK, :])
        for m in range(MEM):
            at = pl.multiple_of(read_ref[f * MEM + m] * TOK, TOK)
            pieces.append(slot_ref[pl.ds(at, TOK), :])
        kv = jnp.concatenate(pieces, axis=0)
        k, v = kv[:, :HEAD], kv[:, HEAD:]
        q, g = q_ref[rows, :], g_ref[rows, :]
        s = dot_last(q, k) * scale + bias_ref[f : f + 1, :]
        e = jnp.exp(s - jnp.max(s, axis=1, keepdims=True))
        w = e / jnp.sum(e, axis=1, keepdims=True)
        half = w.astype(bf16)
        o_ref[rows, :] = dot(half, v).astype(bf16)
        gp = dot_last(g, v)
        ds = (w * (gp - jnp.sum(w * gp, axis=1, keepdims=True))).astype(bf16)
        dq_ref[rows, :] = (dot(ds, k) * scale).astype(bf16)
        dkv = jnp.concatenate([dot_first(ds, q) * scale, dot_first(half, g)], axis=1)
        start = 0
        if f < BAND:
            start = (BAND - f) * TOK
            acc_prev[f * TOK : BAND * TOK, :] += dkv[:start]
        acc_own[max(f - BAND, 0) * TOK : (f + 1) * TOK, :] += dkv[start : (BAND + 1) * TOK]
        spots = [pl.multiple_of(add_ref[f * MEM + m] * TOK, TOK) for m in range(MEM)]
        base = (BAND + 1) * TOK
        olds = [acc_slot[pl.ds(at, TOK), :] for at in spots]
        for m, at in enumerate(spots):
            acc_slot[pl.ds(at, TOK), :] = olds[m] + dkv[base + m * TOK : base + (m + 1) * TOK]
    down_ref[...] = acc_own[...]
    rim_ref[...] = acc_prev[...].astype(bf16)
    dslot_ref[...] = acc_slot[: SPARE * TOK, :].astype(bf16)


def attend(read, add, bias, q, g, own, prev, slots):
    heads = q.shape[1] // HEAD
    col = lambda rows, width: pl.BlockSpec((rows, width), lambda h, *_: (0, h))
    return pl.pallas_call(
        attend_body,
        grid_spec=pltpu.PrefetchScalarGridSpec(
            num_scalar_prefetch=2,
            grid=(heads,),
            in_specs=[
                pl.BlockSpec(bias.shape, lambda h, *_: (0, 0)),
                col(ROWS, HEAD), col(ROWS, HEAD),
                col(ROWS, 2 * HEAD), col(BAND * TOK, 2 * HEAD), col(SPARE * TOK, 2 * HEAD),
            ],
            out_specs=[
                col(ROWS, HEAD), col(ROWS, HEAD),
                col(ROWS, 2 * HEAD), col(BAND * TOK, 2 * HEAD), col(SPARE * TOK, 2 * HEAD),
            ],
            scratch_shapes=[
                pltpu.VMEM((ROWS, 2 * HEAD), f32),
                pltpu.VMEM((BAND * TOK, 2 * HEAD), f32),
                pltpu.VMEM(((SPARE + 1) * TOK, 2 * HEAD), f32),
            ],
        ),
        out_shape=[
            jax.ShapeDtypeStruct(q.shape, bf16),
            jax.ShapeDtypeStruct(q.shape, bf16),
            jax.ShapeDtypeStruct(own.shape, f32),
            jax.ShapeDtypeStruct(prev.shape, bf16),
            jax.ShapeDtypeStruct(slots.shape, bf16),
        ],
        compiler_params=params(),
        name="attend",
    )(read, add, bias, q, g, own, prev, slots)


def collect_body(pick_ref, own_ref, rim_ref, back_ref, dk_ref, dv_ref, acc):
    acc[:ROWS, :] = own_ref[...]
    acc[ROWS:, :] = jnp.zeros_like(acc[ROWS:, :])
    tail = slice((FRAMES - BAND) * TOK, ROWS)
    acc[tail, :] += rim_ref[...].astype(f32)
    for i in range(BLOCKS * CAP):
        at = pl.multiple_of(pick_ref[i] * TOK, TOK)
        acc[pl.ds(at, TOK), :] += back_ref[i * TOK : (i + 1) * TOK, :].astype(f32)
    for h in range(own_ref.shape[1] // (2 * HEAD)):
        dk_ref[:, h * HEAD : (h + 1) * HEAD] = acc[:ROWS, 2 * h * HEAD : (2 * h + 1) * HEAD].astype(bf16)
        dv_ref[:, h * HEAD : (h + 1) * HEAD] = acc[:ROWS, (2 * h + 1) * HEAD : (2 * h + 2) * HEAD].astype(bf16)


def collect(pick, own, rim, back):
    width = own.shape[1]
    cols = 512
    col = lambda rows, w: pl.BlockSpec((rows, w), lambda h, *_: (0, h))
    return pl.pallas_call(
        collect_body,
        grid_spec=pltpu.PrefetchScalarGridSpec(
            num_scalar_prefetch=1,
            grid=(width // cols,),
            in_specs=[col(ROWS, cols), col(BAND * TOK, cols), col(SPARE * TOK, cols)],
            out_specs=[col(ROWS, cols // 2), col(ROWS, cols // 2)],
            scratch_shapes=[pltpu.VMEM((ROWS + TOK, cols), f32)],
        ),
        out_shape=[jax.ShapeDtypeStruct((ROWS, width // 2), bf16)] * 2,
        compiler_params=params(),
        name="collect",
    )(pick, own, rim, back)


def partial_body(a_ref, b_ref, out_ref):
    out_ref[...] = dot_first(a_ref[...], b_ref[...]).astype(bf16)


def weight_partial(a, b):
    rows, m = a.shape
    n = b.shape[1]
    cut = 512 if m >= 2048 else 256
    return pl.pallas_call(
        partial_body,
        grid=(m // cut,),
        in_specs=[
            pl.BlockSpec((rows, cut), lambda i: (0, i)),
            pl.BlockSpec((rows, n), lambda i: (0, 0)),
        ],
        out_specs=pl.BlockSpec((cut, n), lambda i: (i, 0)),
        out_shape=jax.ShapeDtypeStruct((m, n), bf16),
        compiler_params=params(),
        name="wgrad",
    )(a, b)


def other_core(x):
    return lax.ppermute(x, "roll", [(i, i ^ 1) for i in range(lax.axis_size("roll"))])


def core_sum(kept, sent):
    return (kept.astype(f32) + other_core(sent).astype(f32)).astype(bf16)


def from_behind(block, distance):
    return lax.ppermute(
        block, "tm", [(i - distance, i) for i in range(BLOCKS) if 0 <= i - distance < BLOCKS]
    )


def exchange(x):
    rows = x.shape[0] // BLOCKS
    y = lax.all_to_all(
        x.reshape(BLOCKS, rows, x.shape[1]), "tm", split_axis=0, concat_axis=0, tiled=True
    )
    return y.reshape(x.shape)


def local(inputs, cotangent, memory_lists, w_query, w_key, w_value, w_output):
    model_width = inputs.shape[-1]
    inner = w_query.shape[1]
    position = lax.axis_index("tm")
    core = lax.axis_index("roll") % 2
    x = inputs.reshape(ROWS, model_width)
    cot = cotangent.reshape(ROWS, model_width)
    recalled = memory_lists[0]
    first_frame = position * FRAMES

    targets = jnp.arange(BLOCKS * FRAMES, dtype=jnp.int32)
    wanted = jnp.any(recalled.reshape(-1, 1) == targets[None, :], axis=0)
    wanted = wanted.astype(jnp.int32).reshape(BLOCKS, FRAMES)
    asked = lax.all_to_all(wanted, "tm", split_axis=0, concat_axis=0, tiled=True)

    keyval = keyval_rows(x, w_key, w_value)
    queries = jnp.dot(x, w_query, preferred_element_type=f32).astype(bf16)
    grad_heads = dot_last(cot, w_output).astype(bf16)
    before = from_behind(keyval[(FRAMES - BAND) * TOK :], 1)

    slot_rank = jnp.cumsum(wanted, axis=1) - 1
    slot_table = (jnp.arange(BLOCKS, dtype=jnp.int32)[:, None] * CAP + slot_rank).reshape(-1)
    mem_ok = recalled >= 0
    flat = jnp.where(mem_ok, recalled, 0).reshape(-1)
    hit = flat[:, None] == targets[None, :]
    slot_ids = jnp.sum(jnp.where(hit, slot_table[None, :], 0), axis=1)
    ok_flat = mem_ok.reshape(-1)
    read = jnp.clip(jnp.where(ok_flat, slot_ids, 0), 0, SPARE - 1)
    add = jnp.clip(jnp.where(ok_flat, slot_ids, SPARE), 0, SPARE)
    band_index = (
        jnp.arange(FRAMES, dtype=jnp.int32)[:, None] + jnp.arange(BAND + 1, dtype=jnp.int32)[None, :]
    )
    band_ok = first_frame + band_index - BAND >= 0
    key_valid = jnp.concatenate([band_ok, mem_ok], axis=1)
    bias = jnp.repeat(jnp.where(key_valid, 0.0, masked_score).astype(f32), TOK, axis=1)

    asked_rank = jnp.cumsum(asked, axis=1) - 1
    places = jnp.arange(CAP, dtype=jnp.int32)[None, :, None]
    chosen = (asked[:, None, :] > 0) & (asked_rank[:, None, :] == places)
    frame_no = jnp.arange(FRAMES, dtype=jnp.int32)[None, None, :]
    pick = jnp.sum(jnp.where(chosen, frame_no, 0), axis=2).reshape(-1)
    pick_add = jnp.where(jnp.any(chosen, axis=2).reshape(-1), pick, FRAMES)

    slots = exchange(named_frames(pick, keyval))
    heads_out, grad_query, own_grad, rim, slot_grad = attend(
        read, add, bias, queries, grad_heads, keyval, before, slots
    )
    returned = exchange(slot_grad)
    passed = from_behind(rim, -1)

    half_in, half_out = inner // 2, model_width // 2
    other = 1 - core
    q_keep = lax.dynamic_slice_in_dim(grad_query, core * half_in, half_in, 1)
    q_send = lax.dynamic_slice_in_dim(grad_query, other * half_in, half_in, 1)
    c_keep = lax.dynamic_slice_in_dim(cot, core * half_out, half_out, 1)
    c_send = lax.dynamic_slice_in_dim(cot, other * half_out, half_out, 1)
    sum_q = core_sum(weight_partial(x, q_keep), weight_partial(x, q_send))
    sum_o = core_sum(weight_partial(heads_out, c_keep), weight_partial(heads_out, c_send))
    share_q = lax.psum_scatter(sum_q, "tm", scatter_dimension=0, tiled=True)
    share_o = lax.psum_scatter(sum_o, "tm", scatter_dimension=0, tiled=True)
    attended = jnp.dot(heads_out, w_output, preferred_element_type=f32).astype(bf16)

    grad_keys, grad_values = collect(pick_add, own_grad, passed, returned)
    kv_keep = jnp.where(core == 0, grad_keys, grad_values)
    kv_send = jnp.where(core == 0, grad_values, grad_keys)
    sum_kv = core_sum(weight_partial(x, kv_keep), weight_partial(x, kv_send))
    share_kv = lax.psum_scatter(sum_kv, "tm", scatter_dimension=0, tiled=True)
    grad_input = (
        dot_last(grad_query, w_query) + dot_last(grad_keys, w_key) + dot_last(grad_values, w_value)
    ).astype(bf16)

    def over_chips(share):
        m, n = share.shape
        groups = [[c + 2 * i for i in range(4)] for c in range(2)]
        parts = lax.all_to_all(
            share.reshape(4, m // 4, n), "roll", split_axis=0, concat_axis=0, tiled=True,
            axis_index_groups=groups,
        )
        total = jnp.sum(parts.astype(f32), axis=0).astype(bf16)
        every = lax.all_gather(total, "roll", axis=0)
        return jnp.swapaxes(every.reshape(4, 2, m // 4, n), 0, 1).reshape(2, m, n).astype(f32)

    both_q = over_chips(share_q)
    both_o = over_chips(share_o)
    both_kv = over_chips(share_kv)
    total_q = jnp.concatenate([both_q[0], both_q[1]], axis=1)
    total_o = jnp.concatenate([both_o[0], both_o[1]], axis=1)
    shape = (1, FRAMES, TOK, model_width)
    return (
        attended.reshape(shape), grad_input.reshape(shape),
        total_q, both_kv[0], both_kv[1], total_o,
    )


def solution(mesh):
    block = P("roll", "tm", None, None)
    return jax.shard_map(
        local,
        mesh=mesh,
        in_specs=(block, block, P("roll", "tm", None), P(), P(), P(), P()),
        out_specs=(block, block, P("tm", None), P("tm", None), P("tm", None), P("tm", None)),
        check_vma=False,
    )
```

```python
import jax
import jax.numpy as jnp
from jax import lax
from jax.experimental import pallas as pl
from jax.experimental.pallas import tpu as pltpu
from jax.sharding import PartitionSpec as P

HEADS = 8
HEAD = 128
BAND = 4
MEM = 8
CAP = 3
FRAMES = 8
TOK = 32
BLOCKS = 16
ROWS = FRAMES * TOK
GROUPS = 2
GH = HEADS // GROUPS
GW = GH * 2 * HEAD
KEYS = (BAND + 1 + MEM) * TOK
CHIPS = 4
SPARE = BLOCKS * CAP
masked_score = -1e30
f32, bf16 = jnp.float32, jnp.bfloat16
VMEM_LIMIT = 60 * 1024 * 1024


def params(n=1):
    return pltpu.CompilerParams(
        dimension_semantics=("arbitrary",) * n, vmem_limit_bytes=VMEM_LIMIT
    )


def dot_last(left, right):
    return lax.dot_general(left, right, (((1,), (1,)), ((), ())), preferred_element_type=f32)


def dot_first(left, right):
    return lax.dot_general(left, right, (((0,), (0,)), ((), ())), preferred_element_type=f32)


def dot(left, right):
    return lax.dot_general(left, right, (((1,), (0,)), ((), ())), preferred_element_type=f32)


def keyval_body(x_ref, wk_ref, wv_ref, out_ref):
    pieces = []
    for h in range(wk_ref.shape[1] // HEAD):
        pieces += [wk_ref[:, h * HEAD : (h + 1) * HEAD], wv_ref[:, h * HEAD : (h + 1) * HEAD]]
    out_ref[...] = dot(x_ref[...], jnp.concatenate(pieces, axis=1)).astype(bf16)


def keyval_rows(x, w_key, w_value):
    rows, width = x.shape
    cols = 256
    steps = GW // (2 * cols)
    return pl.pallas_call(
        keyval_body,
        grid=(w_key.shape[1] // cols,),
        in_specs=[
            pl.BlockSpec((rows, width), lambda j: (0, 0)),
            pl.BlockSpec((width, cols), lambda j: (0, j)),
            pl.BlockSpec((width, cols), lambda j: (0, j)),
        ],
        out_specs=pl.BlockSpec((None, rows, 2 * cols), lambda j: (j // steps, 0, j % steps)),
        out_shape=jax.ShapeDtypeStruct((GROUPS, rows, GW), bf16),
        compiler_params=params(),
        name="keyval",
    )(x, w_key, w_value)


def send_body(pick_ref, kv_ref, out_ref, sem):
    def copy(i):
        at = pl.multiple_of(pick_ref[i] * TOK, TOK)
        return pltpu.make_async_copy(
            kv_ref.at[0, pl.ds(at, TOK), :], out_ref.at[pl.ds(i * TOK, TOK), :], sem.at[i]
        )

    for i in range(BLOCKS * CAP):
        copy(i).start()
    for i in range(BLOCKS * CAP):
        copy(i).wait()


def named_frames(pick, kv, group):
    return pl.pallas_call(
        send_body,
        grid_spec=pltpu.PrefetchScalarGridSpec(
            num_scalar_prefetch=1,
            grid=(1,),
            in_specs=[pl.BlockSpec((1, ROWS, GW), lambda i, *_: (group, 0, 0))],
            out_specs=pl.BlockSpec(memory_space=pl.ANY),
            scratch_shapes=[pltpu.SemaphoreType.DMA((BLOCKS * CAP,))],
        ),
        out_shape=jax.ShapeDtypeStruct((BLOCKS * CAP * TOK, GW), bf16),
        compiler_params=params(),
        name="send",
    )(pick, kv)


def attend_body(
    read_ref, add_ref, bias_ref, q_ref, g_ref, own_ref, prev_ref, slot_ref,
    o_ref, dq_ref, down_ref, rim_ref, dslot_ref,
    acc_own, acc_prev, acc_slot, kv_scr, s_scr, gp_scr, half_scr, ds_scr,
):
    scale = HEAD ** (-0.5)
    acc_own[...] = jnp.zeros_like(acc_own)
    acc_prev[...] = jnp.zeros_like(acc_prev)
    acc_slot[...] = jnp.zeros_like(acc_slot)
    spans = [slice(f * TOK, (f + 1) * TOK) for f in range(FRAMES)]
    for f, rows in enumerate(spans):
        at = 0
        if f < BAND:
            at = (BAND - f) * TOK
            kv_scr[f, :at, :] = prev_ref[f * TOK : BAND * TOK, :]
        kv_scr[f, at : (BAND + 1) * TOK, :] = own_ref[max(f - BAND, 0) * TOK : (f + 1) * TOK, :]
        for m in range(MEM):
            at = pl.multiple_of(read_ref[f * MEM + m] * TOK, TOK)
            kv_scr[f, (BAND + 1 + m) * TOK : (BAND + 2 + m) * TOK, :] = slot_ref[pl.ds(at, TOK), :]
    for f, rows in enumerate(spans):
        s_scr[rows, :] = dot_last(q_ref[rows, :], kv_scr[f, :, :HEAD]) * scale + bias_ref[f : f + 1, :]
        gp_scr[rows, :] = dot_last(g_ref[rows, :], kv_scr[f, :, HEAD:])
    for f, rows in enumerate(spans):
        s = s_scr[rows, :]
        gp = gp_scr[rows, :]
        e = jnp.exp(s - jnp.max(s, axis=1, keepdims=True))
        w = e * (1.0 / jnp.sum(e, axis=1, keepdims=True))
        half_scr[rows, :] = w.astype(bf16)
        ds_scr[rows, :] = (w * (gp - jnp.sum(w * gp, axis=1, keepdims=True))).astype(bf16)
    for f, rows in enumerate(spans):
        o_ref[rows, :] = dot(half_scr[rows, :], kv_scr[f, :, HEAD:]).astype(bf16)
        dq_ref[rows, :] = (dot(ds_scr[rows, :], kv_scr[f, :, :HEAD]) * scale).astype(bf16)
    for f, rows in enumerate(spans):
        dk = dot_first(ds_scr[rows, :], q_ref[rows, :]) * scale
        dv = dot_first(half_scr[rows, :], g_ref[rows, :])
        start = 0
        own = slice(max(f - BAND, 0) * TOK, (f + 1) * TOK)
        if f < BAND:
            start = (BAND - f) * TOK
            prev = slice(f * TOK, BAND * TOK)
            acc_prev[prev, :HEAD] += dk[:start]
            acc_prev[prev, HEAD:] += dv[:start]
        acc_own[own, :HEAD] += dk[start : (BAND + 1) * TOK]
        acc_own[own, HEAD:] += dv[start : (BAND + 1) * TOK]
        spots = [pl.multiple_of(add_ref[f * MEM + m] * TOK, TOK) for m in range(MEM)]
        base = (BAND + 1) * TOK
        for d, cols in ((dk, slice(0, HEAD)), (dv, slice(HEAD, 2 * HEAD))):
            olds = [acc_slot[pl.ds(at, TOK), cols] for at in spots]
            for m, at in enumerate(spots):
                acc_slot[pl.ds(at, TOK), cols] = olds[m] + d[base + m * TOK : base + (m + 1) * TOK]
    down_ref[...] = acc_own[...]
    rim_ref[...] = acc_prev[...].astype(bf16)
    dslot_ref[...] = acc_slot[: SPARE * TOK, :].astype(bf16)


def attend(read, add, bias, q, g, own, prev, slots, group):
    first = group * GH
    col = lambda rows, width: pl.BlockSpec((rows, width), lambda h, *_: (0, h))
    shifted = pl.BlockSpec((ROWS, HEAD), lambda h, *_: (0, h + first))
    grouped = lambda rows: pl.BlockSpec((None, rows, 2 * HEAD), lambda h, *_: (group, 0, h))
    return pl.pallas_call(
        attend_body,
        grid_spec=pltpu.PrefetchScalarGridSpec(
            num_scalar_prefetch=2,
            grid=(GH,),
            in_specs=[
                pl.BlockSpec(bias.shape, lambda h, *_: (0, 0)),
                shifted, shifted, grouped(ROWS), grouped(BAND * TOK), col(SPARE * TOK, 2 * HEAD),
            ],
            out_specs=[
                col(ROWS, HEAD), col(ROWS, HEAD),
                col(ROWS, 2 * HEAD), col(BAND * TOK, 2 * HEAD), col(SPARE * TOK, 2 * HEAD),
            ],
            scratch_shapes=[
                pltpu.VMEM((ROWS, 2 * HEAD), f32),
                pltpu.VMEM((BAND * TOK, 2 * HEAD), f32),
                pltpu.VMEM(((SPARE + 1) * TOK, 2 * HEAD), f32),
                pltpu.VMEM((FRAMES, KEYS, 2 * HEAD), bf16),
                pltpu.VMEM((ROWS, KEYS), f32),
                pltpu.VMEM((ROWS, KEYS), f32),
                pltpu.VMEM((ROWS, KEYS), bf16),
                pltpu.VMEM((ROWS, KEYS), bf16),
            ],
        ),
        out_shape=[
            jax.ShapeDtypeStruct((ROWS, GH * HEAD), bf16),
            jax.ShapeDtypeStruct((ROWS, GH * HEAD), bf16),
            jax.ShapeDtypeStruct((ROWS, GW), f32),
            jax.ShapeDtypeStruct((BAND * TOK, GW), bf16),
            jax.ShapeDtypeStruct((SPARE * TOK, GW), bf16),
        ],
        compiler_params=params(),
        name="attend",
    )(read, add, bias, q, g, own, prev, slots)


def collect_body(pick_ref, own_ref, rim_ref, back_ref, dk_ref, dv_ref, acc):
    acc[:ROWS, :] = own_ref[...]
    acc[ROWS:, :] = jnp.zeros_like(acc[ROWS:, :])
    tail = slice((FRAMES - BAND) * TOK, ROWS)
    acc[tail, :] += rim_ref[...].astype(f32)
    for i in range(BLOCKS * CAP):
        at = pl.multiple_of(pick_ref[i] * TOK, TOK)
        acc[pl.ds(at, TOK), :] += back_ref[i * TOK : (i + 1) * TOK, :].astype(f32)
    for h in range(own_ref.shape[1] // (2 * HEAD)):
        dk_ref[:, h * HEAD : (h + 1) * HEAD] = acc[:ROWS, 2 * h * HEAD : (2 * h + 1) * HEAD].astype(bf16)
        dv_ref[:, h * HEAD : (h + 1) * HEAD] = acc[:ROWS, (2 * h + 1) * HEAD : (2 * h + 2) * HEAD].astype(bf16)


def collect(pick, own, rim, back):
    width = own.shape[1]
    cols = 512
    col = lambda rows, w: pl.BlockSpec((rows, w), lambda h, *_: (0, h))
    return pl.pallas_call(
        collect_body,
        grid_spec=pltpu.PrefetchScalarGridSpec(
            num_scalar_prefetch=1,
            grid=(width // cols,),
            in_specs=[col(ROWS, cols), col(BAND * TOK, cols), col(SPARE * TOK, cols)],
            out_specs=[col(ROWS, cols // 2), col(ROWS, cols // 2)],
            scratch_shapes=[pltpu.VMEM((ROWS + TOK, cols), f32)],
        ),
        out_shape=[jax.ShapeDtypeStruct((ROWS, width // 2), bf16)] * 2,
        compiler_params=params(),
        name="collect",
    )(pick, own, rim, back)


def keyval_partial(x, g, got=None, chips_first=True):
    rows, m = x.shape
    n = g.shape[1]
    shard, cut = m // BLOCKS, 512
    piece = shard // CHIPS
    if chips_first:
        shape = (CHIPS, BLOCKS, piece, n)
        spec = pl.BlockSpec((CHIPS, cut // shard, piece, n), lambda i: (0, i, 0, 0))
    else:
        shape = (BLOCKS, shard, n)
        spec = pl.BlockSpec((cut // shard, shard, n), lambda i: (i, 0, 0))

    def body(a_ref, b_ref, *refs):
        out_ref = refs[-1]
        total = dot_first(a_ref[...], b_ref[...])
        for t in range(cut // shard):
            for c in range(CHIPS if chips_first else 1):
                size = piece if chips_first else shard
                at = t * shard + c * size
                where = (c, t) if chips_first else (t,)
                part = total[at : at + size]
                if len(refs) == 2:
                    part = part + refs[0][where].astype(f32)
                out_ref[where] = part.astype(bf16)

    return pl.pallas_call(
        body,
        grid=(m // cut,),
        in_specs=[
            pl.BlockSpec((rows, cut), lambda i: (0, i)),
            pl.BlockSpec((rows, n), lambda i: (0, 0)),
        ] + [spec] * (got is not None),
        out_specs=spec,
        out_shape=jax.ShapeDtypeStruct(shape, bf16),
        compiler_params=params(),
        name="keyval_partial",
    )(x, g, *([] if got is None else [got]))


def query_output_partial(x, q, heads, cot, got=None):
    rows, m = x.shape
    n = q.shape[1]
    inner = heads.shape[1]
    per = 4
    q_shard, o_shard = m // BLOCKS, inner // BLOCKS
    q_piece, o_piece = q_shard // CHIPS, o_shard // CHIPS
    height = q_piece + 2 * o_piece
    spec = pl.BlockSpec((CHIPS, per, height, n), lambda i: (0, i, 0, 0))

    def body(x_ref, q_ref, h_ref, c_ref, *refs):
        out_ref = refs[-1]
        dq = dot_first(x_ref[...], q_ref[...])
        do = dot_first(h_ref[...], c_ref[...])
        for t in range(per):
            for c in range(CHIPS):
                at = t * q_shard + c * q_piece
                parts = [dq[at : at + q_piece]]
                at = t * o_shard + c * o_piece
                parts += [do[at : at + o_piece, :n], do[at : at + o_piece, n:]]
                part = jnp.concatenate(parts, axis=0)
                if len(refs) == 2:
                    part = part + refs[0][c, t].astype(f32)
                out_ref[c, t] = part.astype(bf16)

    return pl.pallas_call(
        body,
        grid=(BLOCKS // per,),
        in_specs=[
            pl.BlockSpec((rows, per * q_shard), lambda i: (0, i)),
            pl.BlockSpec((rows, n), lambda i: (0, 0)),
            pl.BlockSpec((rows, per * o_shard), lambda i: (0, i)),
            pl.BlockSpec((rows, 2 * n), lambda i: (0, 0)),
        ] + [spec] * (got is not None),
        out_specs=spec,
        out_shape=jax.ShapeDtypeStruct((CHIPS, BLOCKS, height, n), bf16),
        compiler_params=params(),
        name="query_output_partial",
    )(x, q, heads, cot, *([] if got is None else [got]))


def other_core(x):
    return lax.ppermute(x, "roll", [(i, i ^ 1) for i in range(lax.axis_size("roll"))])


def from_behind(block, distance):
    return lax.ppermute(
        block, "tm", [(i - distance, i) for i in range(BLOCKS) if 0 <= i - distance < BLOCKS]
    )


def exchange(x, axis="tm", groups=None):
    return lax.all_to_all(
        x, axis, split_axis=0, concat_axis=0, tiled=True, axis_index_groups=groups
    )


def summed(parts):
    return jnp.sum(parts.astype(f32), axis=0).astype(bf16)


def over_chips(x):
    return summed(exchange(x, "roll", [[c + 2 * i for i in range(CHIPS)] for c in range(2)]))


def over_blocks(x):
    return summed(exchange(x))


def everyone(x):
    parts = exchange(jnp.broadcast_to(x, (2 * CHIPS, *x.shape)), "roll")
    return parts.reshape(CHIPS, 2, *x.shape)


def slots_exchange(x):
    return exchange(x.reshape(BLOCKS, CAP * TOK, GW)).reshape(x.shape)


def local(inputs, cotangent, memory_lists, w_query, w_key, w_value, w_output):
    model_width = inputs.shape[-1]
    inner = w_query.shape[1]
    position = lax.axis_index("tm")
    core = lax.axis_index("roll") % 2
    first_core = core == 0
    x = inputs.reshape(ROWS, model_width)
    cot = cotangent.reshape(ROWS, model_width)
    recalled = memory_lists[0]
    first_frame = position * FRAMES

    targets = jnp.arange(BLOCKS * FRAMES, dtype=jnp.int32)
    wanted = jnp.any(recalled.reshape(-1, 1) == targets[None, :], axis=0)
    wanted = wanted.astype(jnp.int32).reshape(BLOCKS, FRAMES)
    asked = exchange(wanted)

    keyval = keyval_rows(x, w_key, w_value)
    before = from_behind(keyval[:, (FRAMES - BAND) * TOK :], 1)
    queries = jnp.dot(x, w_query, preferred_element_type=f32).astype(bf16)
    grad_heads = dot_last(cot, w_output).astype(bf16)

    slot_rank = jnp.cumsum(wanted, axis=1) - 1
    slot_table = (jnp.arange(BLOCKS, dtype=jnp.int32)[:, None] * CAP + slot_rank).reshape(-1)
    mem_ok = recalled >= 0
    flat = jnp.where(mem_ok, recalled, 0).reshape(-1)
    hit = flat[:, None] == targets[None, :]
    slot_ids = jnp.sum(jnp.where(hit, slot_table[None, :], 0), axis=1)
    ok_flat = mem_ok.reshape(-1)
    read = jnp.clip(jnp.where(ok_flat, slot_ids, 0), 0, SPARE - 1)
    add = jnp.clip(jnp.where(ok_flat, slot_ids, SPARE), 0, SPARE)
    band_index = (
        jnp.arange(FRAMES, dtype=jnp.int32)[:, None] + jnp.arange(BAND + 1, dtype=jnp.int32)[None, :]
    )
    band_ok = first_frame + band_index - BAND >= 0
    key_valid = jnp.concatenate([band_ok, mem_ok], axis=1)
    bias = jnp.repeat(jnp.where(key_valid, 0.0, masked_score).astype(f32), TOK, axis=1)

    asked_rank = jnp.cumsum(asked, axis=1) - 1
    places = jnp.arange(CAP, dtype=jnp.int32)[None, :, None]
    chosen = (asked[:, None, :] > 0) & (asked_rank[:, None, :] == places)
    frame_no = jnp.arange(FRAMES, dtype=jnp.int32)[None, None, :]
    pick = jnp.sum(jnp.where(chosen, frame_no, 0), axis=2).reshape(-1)
    pick_add = jnp.where(jnp.any(chosen, axis=2).reshape(-1), pick, FRAMES)

    slots = [slots_exchange(named_frames(pick, keyval, g)) for g in range(GROUPS)]
    heads, dqs, owns, passed, returned = [], [], [], [], []
    for g in range(GROUPS):
        heads_g, dq_g, own_g, rim_g, dslot_g = attend(
            read, add, bias, queries, grad_heads, keyval, before, slots[g], g
        )
        returned.append(slots_exchange(dslot_g))
        passed.append(from_behind(rim_g, -1))
        heads.append(heads_g)
        dqs.append(dq_g)
        owns.append(own_g)

    heads_out = jnp.concatenate(heads, axis=1)
    grad_query = jnp.concatenate(dqs, axis=1)
    half_out = model_width // 2
    q_keep, q_send = jnp.where(first_core, dqs[0], dqs[1]), jnp.where(first_core, dqs[1], dqs[0])
    c_keep = jnp.where(first_core, cot[:, :half_out], cot[:, half_out:])
    c_send = jnp.where(first_core, cot[:, half_out:], cot[:, :half_out])
    got = other_core(query_output_partial(x, q_send, heads_out, c_send))
    share = over_blocks(over_chips(query_output_partial(x, q_keep, heads_out, c_keep, got)))
    both = everyone(share).astype(f32)
    piece = model_width // BLOCKS // CHIPS
    total_q = jnp.concatenate([both[:, c, :piece].reshape(-1, inner // 2) for c in range(2)], axis=1)
    o_piece = piece // 2
    total_o = jnp.concatenate(
        [
            both[:, c, piece + k * o_piece : piece + (k + 1) * o_piece].reshape(-1, inner // 2)
            for c in range(2)
            for k in range(2)
        ],
        axis=1,
    )
    attended = jnp.dot(heads_out, w_output, preferred_element_type=f32).astype(bf16)
    grad_input = dot_last(grad_query, w_query)

    k_cols, v_cols = [], []
    for g in range(GROUPS):
        dk, dv = collect(pick_add, owns[g], passed[g], returned[g])
        cols = slice(g * GH * HEAD, (g + 1) * GH * HEAD)
        grad_input = grad_input + dot_last(dk, w_key[:, cols]) + dot_last(dv, w_value[:, cols])
        keep, send = jnp.where(first_core, dk, dv), jnp.where(first_core, dv, dk)
        early = g < GROUPS - 1
        got = other_core(keyval_partial(x, send, None, early))
        total = keyval_partial(x, keep, got, early)
        if early:
            both = everyone(over_blocks(over_chips(total))).astype(f32)
            both = jnp.swapaxes(both, 0, 1).reshape(2, -1, total.shape[-1])
        else:
            both = jnp.sum(everyone(over_blocks(total)).astype(f32), axis=0)
        k_cols.append(both[0])
        v_cols.append(both[1])
    shape = (1, FRAMES, TOK, model_width)
    return (
        attended.reshape(shape),
        grad_input.astype(bf16).reshape(shape),
        total_q,
        jnp.concatenate(k_cols, axis=1),
        jnp.concatenate(v_cols, axis=1),
        total_o,
    )


def solution(mesh):
    block = P("roll", "tm", None, None)
    return jax.shard_map(
        local,
        mesh=mesh,
        in_specs=(block, block, P("roll", "tm", None), P(), P(), P(), P()),
        out_specs=(block, block, P("tm", None), P("tm", None), P("tm", None), P("tm", None)),
        check_vma=False,
    )
```

```python
import jax
import jax.numpy as jnp
from jax import lax
from jax.experimental import pallas as pl
from jax.experimental.pallas import tpu as pltpu
from jax.sharding import PartitionSpec as P


HEAD = 128
BAND = 4
MEM = 8
CAP = 3
FRAMES = 8
TOK = 32
BLOCKS = 16
ROWS = FRAMES * TOK
SPLIT = (4, 4)
KEYS = (BAND + 1 + MEM) * TOK
CHIPS = 4
SPARE = BLOCKS * CAP
masked_score = -1e30
f32, bf16 = jnp.float32, jnp.bfloat16
VMEM_LIMIT = 60 * 1024 * 1024


def params(n=1):
    return pltpu.CompilerParams(
        dimension_semantics=("arbitrary",) * n, vmem_limit_bytes=VMEM_LIMIT
    )


def dot_last(left, right):
    return lax.dot_general(left, right, (((1,), (1,)), ((), ())), preferred_element_type=f32)


def dot_first(left, right):
    return lax.dot_general(left, right, (((0,), (0,)), ((), ())), preferred_element_type=f32)


def dot(left, right):
    return lax.dot_general(left, right, (((1,), (0,)), ((), ())), preferred_element_type=f32)


def keyval_body(x_ref, wk_ref, wv_ref, out_ref):
    pieces = []
    for h in range(wk_ref.shape[1] // HEAD):
        pieces += [wk_ref[:, h * HEAD : (h + 1) * HEAD], wv_ref[:, h * HEAD : (h + 1) * HEAD]]
    out_ref[...] = dot(x_ref[...], jnp.concatenate(pieces, axis=1)).astype(bf16)


def keyval_rows(x, w_key, w_value):
    rows, width = x.shape
    cols = 256
    return pl.pallas_call(
        keyval_body,
        grid=(w_key.shape[1] // cols,),
        in_specs=[
            pl.BlockSpec((rows, width), lambda j: (0, 0)),
            pl.BlockSpec((width, cols), lambda j: (0, j)),
            pl.BlockSpec((width, cols), lambda j: (0, j)),
        ],
        out_specs=pl.BlockSpec((rows, 2 * cols), lambda j: (0, j)),
        out_shape=jax.ShapeDtypeStruct((rows, 2 * w_key.shape[1]), bf16),
        compiler_params=params(),
        name="keyval",
    )(x, w_key, w_value)


def send_body(pick_ref, kv_ref, out_ref, sem):
    def copy(i):
        at = pl.multiple_of(pick_ref[i] * TOK, TOK)
        return pltpu.make_async_copy(
            kv_ref.at[pl.ds(at, TOK), :], out_ref.at[pl.ds(i * TOK, TOK), :], sem.at[i]
        )

    for i in range(BLOCKS * CAP):
        copy(i).start()
    for i in range(BLOCKS * CAP):
        copy(i).wait()


def named_frames(pick, kv):
    width = kv.shape[1]
    return pl.pallas_call(
        send_body,
        grid_spec=pltpu.PrefetchScalarGridSpec(
            num_scalar_prefetch=1,
            grid=(1,),
            in_specs=[pl.BlockSpec((ROWS, width), lambda i, *_: (0, 0))],
            out_specs=pl.BlockSpec(memory_space=pl.ANY),
            scratch_shapes=[pltpu.SemaphoreType.DMA((BLOCKS * CAP,))],
        ),
        out_shape=jax.ShapeDtypeStruct((BLOCKS * CAP * TOK, width), bf16),
        compiler_params=params(),
        name="send",
    )(pick, kv)


def attend_body(
    read_ref, add_ref, bias_ref, q_ref, g_ref, own_ref, prev_ref, slot_ref,
    o_ref, dq_ref, down_ref, rim_ref, dslot_ref,
    acc_own, acc_prev, acc_slot, kv_scr, s_scr, gp_scr, half_scr, ds_scr,
):
    scale = HEAD ** (-0.5)
    acc_own[...] = jnp.zeros_like(acc_own)
    acc_prev[...] = jnp.zeros_like(acc_prev)
    acc_slot[...] = jnp.zeros_like(acc_slot)
    spans = [slice(f * TOK, (f + 1) * TOK) for f in range(FRAMES)]
    for f, rows in enumerate(spans):
        at = 0
        if f < BAND:
            at = (BAND - f) * TOK
            kv_scr[f, :at, :] = prev_ref[f * TOK : BAND * TOK, :]
        kv_scr[f, at : (BAND + 1) * TOK, :] = own_ref[max(f - BAND, 0) * TOK : (f + 1) * TOK, :]
        for m in range(MEM):
            at = pl.multiple_of(read_ref[f * MEM + m] * TOK, TOK)
            kv_scr[f, (BAND + 1 + m) * TOK : (BAND + 2 + m) * TOK, :] = slot_ref[pl.ds(at, TOK), :]
    for f, rows in enumerate(spans):
        s_scr[rows, :] = dot_last(q_ref[rows, :], kv_scr[f, :, :HEAD]) * scale + bias_ref[f : f + 1, :]
        gp_scr[rows, :] = dot_last(g_ref[rows, :], kv_scr[f, :, HEAD:])
    for rows in spans:
        s = s_scr[rows, :]
        gp = gp_scr[rows, :]
        e = jnp.exp(s - jnp.max(s, axis=1, keepdims=True))
        w = e * (1.0 / jnp.sum(e, axis=1, keepdims=True))
        half_scr[rows, :] = w.astype(bf16)
        ds_scr[rows, :] = (w * (gp - jnp.sum(w * gp, axis=1, keepdims=True))).astype(bf16)
    for f, rows in enumerate(spans):
        o_ref[rows, :] = dot(half_scr[rows, :], kv_scr[f, :, HEAD:]).astype(bf16)
        dq_ref[rows, :] = (dot(ds_scr[rows, :], kv_scr[f, :, :HEAD]) * scale).astype(bf16)
    for f, rows in enumerate(spans):
        dk = dot_first(ds_scr[rows, :], q_ref[rows, :]) * scale
        dv = dot_first(half_scr[rows, :], g_ref[rows, :])
        start = 0
        own = slice(max(f - BAND, 0) * TOK, (f + 1) * TOK)
        if f < BAND:
            start = (BAND - f) * TOK
            prev = slice(f * TOK, BAND * TOK)
            acc_prev[prev, :HEAD] += dk[:start]
            acc_prev[prev, HEAD:] += dv[:start]
        acc_own[own, :HEAD] += dk[start : (BAND + 1) * TOK]
        acc_own[own, HEAD:] += dv[start : (BAND + 1) * TOK]
        spots = [pl.multiple_of(add_ref[f * MEM + m] * TOK, TOK) for m in range(MEM)]
        base = (BAND + 1) * TOK
        for d, cols in ((dk, slice(0, HEAD)), (dv, slice(HEAD, 2 * HEAD))):
            olds = [acc_slot[pl.ds(at, TOK), cols] for at in spots]
            for m, at in enumerate(spots):
                acc_slot[pl.ds(at, TOK), cols] = olds[m] + d[base + m * TOK : base + (m + 1) * TOK]
    down_ref[...] = acc_own[...]
    rim_ref[...] = acc_prev[...].astype(bf16)
    dslot_ref[...] = acc_slot[: SPARE * TOK, :].astype(bf16)


def attend(read, add, bias, q, g, own, prev, slots, first, heads):
    col = lambda rows, width: pl.BlockSpec((rows, width), lambda h, *_: (0, h))
    src = lambda rows, width: pl.BlockSpec((rows, width), lambda h, *_: (0, h + first))
    return pl.pallas_call(
        attend_body,
        grid_spec=pltpu.PrefetchScalarGridSpec(
            num_scalar_prefetch=2,
            grid=(heads,),
            in_specs=[
                pl.BlockSpec(bias.shape, lambda h, *_: (0, 0)),
                src(ROWS, HEAD), src(ROWS, HEAD),
                src(ROWS, 2 * HEAD), src(BAND * TOK, 2 * HEAD), src(SPARE * TOK, 2 * HEAD),
            ],
            out_specs=[
                col(ROWS, HEAD), col(ROWS, HEAD),
                col(ROWS, 2 * HEAD), col(BAND * TOK, 2 * HEAD), col(SPARE * TOK, 2 * HEAD),
            ],
            scratch_shapes=[
                pltpu.VMEM((ROWS, 2 * HEAD), f32),
                pltpu.VMEM((BAND * TOK, 2 * HEAD), f32),
                pltpu.VMEM(((SPARE + 1) * TOK, 2 * HEAD), f32),
                pltpu.VMEM((FRAMES, KEYS, 2 * HEAD), bf16),
                pltpu.VMEM((ROWS, KEYS), f32),
                pltpu.VMEM((ROWS, KEYS), f32),
                pltpu.VMEM((ROWS, KEYS), bf16),
                pltpu.VMEM((ROWS, KEYS), bf16),
            ],
        ),
        out_shape=[
            jax.ShapeDtypeStruct((ROWS, heads * HEAD), bf16),
            jax.ShapeDtypeStruct((ROWS, heads * HEAD), bf16),
            jax.ShapeDtypeStruct((ROWS, 2 * heads * HEAD), f32),
            jax.ShapeDtypeStruct((BAND * TOK, 2 * heads * HEAD), bf16),
            jax.ShapeDtypeStruct((SPARE * TOK, 2 * heads * HEAD), bf16),
        ],
        compiler_params=params(),
        name="attend",
    )(read, add, bias, q, g, own, prev, slots)


def collect_body(pick_ref, own_ref, rim_ref, back_ref, out_ref, acc):
    acc[:ROWS, :] = own_ref[...]
    acc[ROWS:, :] = jnp.zeros_like(acc[ROWS:, :])
    tail = slice((FRAMES - BAND) * TOK, ROWS)
    acc[tail, :] += rim_ref[...].astype(f32)
    for i in range(BLOCKS * CAP):
        at = pl.multiple_of(pick_ref[i] * TOK, TOK)
        acc[pl.ds(at, TOK), :] += back_ref[i * TOK : (i + 1) * TOK, :].astype(f32)
    for h in range(own_ref.shape[1] // (2 * HEAD)):
        for kind in range(2):
            left = (2 * h + kind) * HEAD
            out_ref[kind, :, h * HEAD : (h + 1) * HEAD] = acc[:ROWS, left : left + HEAD].astype(bf16)


def collect(pick, own, rim, back):
    width = own.shape[1]
    cols = min(512, width)
    col = lambda rows, w: pl.BlockSpec((rows, w), lambda h, *_: (0, h))
    return pl.pallas_call(
        collect_body,
        grid_spec=pltpu.PrefetchScalarGridSpec(
            num_scalar_prefetch=1,
            grid=(width // cols,),
            in_specs=[col(ROWS, cols), col(BAND * TOK, cols), col(SPARE * TOK, cols)],
            out_specs=pl.BlockSpec((2, ROWS, cols // 2), lambda h, *_: (0, 0, h)),
            scratch_shapes=[pltpu.VMEM((ROWS + TOK, cols), f32)],
        ),
        out_shape=jax.ShapeDtypeStruct((2, ROWS, width // 2), bf16),
        compiler_params=params(),
        name="collect",
    )(pick, own, rim, back)


def taken(right):
    if right.ndim == 3:
        rows, n = right.shape[1:]
        return n, pl.BlockSpec((None, rows, n), lambda i, s, *_: (s[1], 0, 0))
    rows, n = right.shape
    return n // 2, pl.BlockSpec((rows, n // 2), lambda i, s, *_: (0, s[1]))


def partial_call(pairs, shards, width, scalars, got=None):
    per = 4
    cuts = [taken(right) for _, right in pairs]
    height = sum(s // CHIPS * (n // width) for (n, _), s in zip(cuts, shards))
    rows = pairs[0][0].shape[0]
    keep = got is not None

    def body(chip_ref, *refs):
        factors, refs = refs[: 2 * len(pairs)], refs[2 * len(pairs) :]
        totals = refs[-len(pairs) :]
        for k, total in enumerate(totals):
            total[...] = dot_first(factors[2 * k][...], factors[2 * k + 1][...])
        for t in range(per):
            for d in range(CHIPS):
                c = lax.rem(chip_ref[0] + d, CHIPS) if keep else d
                at = 0
                for total, shard in zip(totals, shards):
                    piece = shard // CHIPS
                    first = t * shard + c * piece
                    if keep:
                        first = pl.multiple_of(first, piece)
                    for left in range(0, total.shape[1], width):
                        part = total[pl.ds(first, piece), left : left + width]
                        here = slice(at, at + piece)
                        if keep:
                            part = part + refs[0][c, t, here, :].astype(f32)
                            refs[1 + d][t, here, :] = part.astype(bf16)
                        else:
                            refs[0][c, t, here, :] = part.astype(bf16)
                        at += piece

    whole = pl.BlockSpec((CHIPS, per, height, width), lambda i, *_: (0, i, 0, 0))
    one = pl.BlockSpec((per, height, width), lambda i, *_: (i, 0, 0))
    in_specs, operands = [], []
    for (left, right), shard, (_, spec) in zip(pairs, shards, cuts):
        in_specs += [pl.BlockSpec((rows, per * shard), lambda i, *_: (0, i)), spec]
        operands += [left, right]
    if keep:
        in_specs.append(whole)
        operands.append(got)
        out_specs = [one] * CHIPS
        out_shape = [jax.ShapeDtypeStruct((BLOCKS, height, width), bf16)] * CHIPS
    else:
        out_specs = whole
        out_shape = jax.ShapeDtypeStruct((CHIPS, BLOCKS, height, width), bf16)
    return pl.pallas_call(
        body,
        grid_spec=pltpu.PrefetchScalarGridSpec(
            num_scalar_prefetch=1,
            grid=(BLOCKS // per,),
            in_specs=in_specs,
            out_specs=out_specs,
            scratch_shapes=[
                pltpu.VMEM((per * s, n), f32) for (n, _), s in zip(cuts, shards)
            ],
        ),
        out_shape=out_shape,
        compiler_params=params(),
    )(scalars, *operands)


def last_partial(x, g, scalars, got=None):
    rows, m = x.shape
    n, right = taken(g)
    shard, per = m // BLOCKS, 4
    spec = pl.BlockSpec((per, shard, n), lambda i, *_: (i, 0, 0))

    def body(s_ref, a_ref, b_ref, *refs):
        total = dot_first(a_ref[...], b_ref[...])
        for t in range(per):
            part = total[t * shard : (t + 1) * shard]
            if got is not None:
                part = part + refs[0][t].astype(f32)
            refs[-1][t] = part.astype(bf16)

    return pl.pallas_call(
        body,
        grid_spec=pltpu.PrefetchScalarGridSpec(
            num_scalar_prefetch=1,
            grid=(BLOCKS // per,),
            in_specs=[pl.BlockSpec((rows, per * shard), lambda i, *_: (0, i)), right]
            + [spec] * (got is not None),
            out_specs=spec,
        ),
        out_shape=jax.ShapeDtypeStruct((BLOCKS, shard, n), bf16),
        compiler_params=params(),
        name="last_partial",
    )(scalars, x, g, *([] if got is None else [got]))


def other_core(x):
    return lax.ppermute(x, "roll", [(i, i ^ 1) for i in range(lax.axis_size("roll"))])


def from_behind(block, distance):
    return lax.ppermute(
        block, "tm", [(i - distance, i) for i in range(BLOCKS) if 0 <= i - distance < BLOCKS]
    )


def exchange(x, axis="tm", groups=None):
    return lax.all_to_all(
        x, axis, split_axis=0, concat_axis=0, tiled=True, axis_index_groups=groups
    )


def summed(parts):
    return jnp.sum(parts.astype(f32), axis=0).astype(bf16)


def over_chips(pieces):
    total = pieces[0].astype(f32)
    n = 2 * CHIPS
    for d in range(1, CHIPS):
        got = lax.ppermute(pieces[d], "roll", [(i, (i + 2 * d) % n) for i in range(n)])
        total = total + got.astype(f32)
    return total.astype(bf16)


def everyone(x):
    parts = exchange(jnp.broadcast_to(x, (2 * CHIPS, *x.shape)), "roll")
    return parts.reshape(CHIPS, 2, *x.shape)


def slots_exchange(x):
    return exchange(x.reshape(BLOCKS, CAP * TOK, x.shape[1])).reshape(x.shape)


def step(inputs, cotangent, memory_lists, w_query, w_key, w_value, w_output):
    model_width = inputs.shape[-1]
    inner = w_query.shape[1]
    half = inner // 2
    position = lax.axis_index("tm")
    core = lax.axis_index("roll") % 2
    chip = lax.axis_index("roll") // 2
    keeping = jnp.stack([chip, core]).astype(jnp.int32)
    sending = jnp.stack([chip, 1 - core]).astype(jnp.int32)
    x = inputs.reshape(ROWS, model_width)
    cot = cotangent.reshape(ROWS, model_width)
    recalled = memory_lists[0]
    first_frame = position * FRAMES

    targets = jnp.arange(BLOCKS * FRAMES, dtype=jnp.int32)
    wanted = jnp.any(recalled.reshape(-1, 1) == targets[None, :], axis=0)
    wanted = wanted.astype(jnp.int32).reshape(BLOCKS, FRAMES)
    asked = exchange(wanted)

    keyval = keyval_rows(x, w_key, w_value)
    before = from_behind(keyval[(FRAMES - BAND) * TOK :], 1)
    queries = jnp.dot(x, w_query, preferred_element_type=f32).astype(bf16)
    grad_heads = dot_last(cot, w_output).astype(bf16)

    slot_rank = jnp.cumsum(wanted, axis=1) - 1
    slot_table = (jnp.arange(BLOCKS, dtype=jnp.int32)[:, None] * CAP + slot_rank).reshape(-1)
    mem_ok = recalled >= 0
    flat = jnp.where(mem_ok, recalled, 0).reshape(-1)
    hit = flat[:, None] == targets[None, :]
    slot_ids = jnp.sum(jnp.where(hit, slot_table[None, :], 0), axis=1)
    ok_flat = mem_ok.reshape(-1)
    read = jnp.clip(jnp.where(ok_flat, slot_ids, 0), 0, SPARE - 1)
    add = jnp.clip(jnp.where(ok_flat, slot_ids, SPARE), 0, SPARE)
    band_index = (
        jnp.arange(FRAMES, dtype=jnp.int32)[:, None] + jnp.arange(BAND + 1, dtype=jnp.int32)[None, :]
    )
    band_ok = first_frame + band_index - BAND >= 0
    key_valid = jnp.concatenate([band_ok, mem_ok], axis=1)
    bias = jnp.repeat(jnp.where(key_valid, 0.0, masked_score).astype(f32), TOK, axis=1)

    asked_rank = jnp.cumsum(asked, axis=1) - 1
    places = jnp.arange(CAP, dtype=jnp.int32)[None, :, None]
    chosen = (asked[:, None, :] > 0) & (asked_rank[:, None, :] == places)
    frame_no = jnp.arange(FRAMES, dtype=jnp.int32)[None, None, :]
    pick = jnp.sum(jnp.where(chosen, frame_no, 0), axis=2).reshape(-1)
    pick_add = jnp.where(jnp.any(chosen, axis=2).reshape(-1), pick, FRAMES)

    outgoing = named_frames(pick, keyval)
    slots = slots_exchange(outgoing)
    heads, dqs, owns, passed, returned = [], [], [], [], []
    first = 0
    for count in SPLIT:
        heads_g, dq_g, own_g, rim_g, dslot_g = attend(
            read, add, bias, queries, grad_heads, keyval, before, slots, first, count
        )
        passed.append(from_behind(rim_g, -1))
        returned.append(slots_exchange(dslot_g))
        heads.append(heads_g)
        dqs.append(dq_g)
        owns.append(own_g)
        first += count

    heads_out = jnp.concatenate(heads, axis=1)
    grad_query = jnp.concatenate(dqs, axis=1)
    shards = [model_width // BLOCKS, inner // BLOCKS]
    sent = partial_call([(x, grad_query), (heads_out, cot)], shards, half, sending)
    got = other_core(sent)
    kept = partial_call([(x, grad_query), (heads_out, cot)], shards, half, keeping, got)
    sum_qo = over_chips(kept)
    attended = jnp.dot(heads_out, w_output, preferred_element_type=f32).astype(bf16)
    grad_input = dot_last(grad_query, w_query)

    dks, dvs = [], []
    for g, count in enumerate(SPLIT):
        dkv = collect(pick_add, owns[g], passed[g], returned[g])
        dks.append(dkv[0])
        dvs.append(dkv[1])
        width = count * HEAD
        if g == 0:
            sent = partial_call([(x, dkv)], shards[:1], width, sending)
            got = other_core(sent)
            kept = partial_call([(x, dkv)], shards[:1], width, keeping, got)
            sum_kv = over_chips(kept)
            early = summed(exchange(jnp.concatenate([sum_qo, sum_kv], axis=1)))
        else:
            sent = last_partial(x, dkv, sending)
            got = other_core(sent)
            kept = last_partial(x, dkv, keeping, got)
            late = summed(exchange(kept))
    both = everyone(jnp.concatenate([early, late], axis=0)).astype(f32)
    piece = model_width // BLOCKS // CHIPS
    o_piece = inner // BLOCKS // CHIPS
    total_q = jnp.concatenate([both[:, c, :piece].reshape(-1, half) for c in range(2)], axis=1)
    total_o = jnp.concatenate(
        [
            both[:, c, piece + k * o_piece : piece + (k + 1) * o_piece].reshape(-1, half)
            for c in range(2)
            for k in range(2)
        ],
        axis=1,
    )
    at = piece + 2 * o_piece
    kv_first = both[:, :, at : at + piece]
    kv_last = jnp.sum(both[:, :, at + piece :], axis=0)
    total_k, total_v = (
        jnp.concatenate([kv_first[:, c].reshape(-1, half), kv_last[c]], axis=1) for c in range(2)
    )
    grad_input = (
        grad_input
        + dot_last(jnp.concatenate(dks, axis=1), w_key)
        + dot_last(jnp.concatenate(dvs, axis=1), w_value)
    )
    shape = (1, FRAMES, TOK, model_width)
    return (
        attended.reshape(shape),
        grad_input.astype(bf16).reshape(shape),
        total_q,
        total_k,
        total_v,
        total_o,
    )


def solution(mesh):
    block = P("roll", "tm", None, None)
    return jax.shard_map(
        step,
        mesh=mesh,
        in_specs=(block, block, P("roll", "tm", None), P(), P(), P(), P()),
        out_specs=(block, block, P("tm", None), P("tm", None), P("tm", None), P("tm", None)),
        check_vma=False,
    )
```

```python
import jax
import jax.numpy as jnp
from jax import lax
from jax.experimental import pallas as pl
from jax.experimental.pallas import tpu as pltpu
from jax.sharding import PartitionSpec as P


HEAD = 128
BAND = 4
MEM = 8
CAP = 3
FRAMES = 8
TOK = 32
BLOCKS = 16
ROWS = FRAMES * TOK
SPLIT = (4, 4)
KEYS = (BAND + 1 + MEM) * TOK
CHIPS = 4
SPARE = BLOCKS * CAP
masked_score = -1e30
f32, bf16 = jnp.float32, jnp.bfloat16
VMEM_LIMIT = 60 * 1024 * 1024


def params(n=1):
    return pltpu.CompilerParams(
        dimension_semantics=("arbitrary",) * n, vmem_limit_bytes=VMEM_LIMIT
    )


def dot_last(left, right):
    return lax.dot_general(left, right, (((1,), (1,)), ((), ())), preferred_element_type=f32)


def dot_first(left, right):
    return lax.dot_general(left, right, (((0,), (0,)), ((), ())), preferred_element_type=f32)


def dot(left, right):
    return lax.dot_general(left, right, (((1,), (0,)), ((), ())), preferred_element_type=f32)


def keyval_body(x_ref, wk_ref, wv_ref, out_ref):
    pieces = []
    for h in range(wk_ref.shape[1] // HEAD):
        pieces += [wk_ref[:, h * HEAD : (h + 1) * HEAD], wv_ref[:, h * HEAD : (h + 1) * HEAD]]
    out_ref[...] = dot(x_ref[...], jnp.concatenate(pieces, axis=1)).astype(bf16)


def keyval_rows(x, w_key, w_value):
    rows, width = x.shape
    cols = 256
    return pl.pallas_call(
        keyval_body,
        grid=(w_key.shape[1] // cols,),
        in_specs=[
            pl.BlockSpec((rows, width), lambda j: (0, 0)),
            pl.BlockSpec((width, cols), lambda j: (0, j)),
            pl.BlockSpec((width, cols), lambda j: (0, j)),
        ],
        out_specs=pl.BlockSpec((rows, 2 * cols), lambda j: (0, j)),
        out_shape=jax.ShapeDtypeStruct((rows, 2 * w_key.shape[1]), bf16),
        compiler_params=params(),
        name="keyval",
    )(x, w_key, w_value)


def send_body(pick_ref, kv_ref, out_ref, sem):
    def copy(i):
        at = pl.multiple_of(pick_ref[i] * TOK, TOK)
        return pltpu.make_async_copy(
            kv_ref.at[pl.ds(at, TOK), :], out_ref.at[pl.ds(i * TOK, TOK), :], sem.at[i]
        )

    for i in range(BLOCKS * CAP):
        copy(i).start()
    for i in range(BLOCKS * CAP):
        copy(i).wait()


def named_frames(pick, kv):
    width = kv.shape[1]
    return pl.pallas_call(
        send_body,
        grid_spec=pltpu.PrefetchScalarGridSpec(
            num_scalar_prefetch=1,
            grid=(1,),
            in_specs=[pl.BlockSpec((ROWS, width), lambda i, *_: (0, 0))],
            out_specs=pl.BlockSpec(memory_space=pl.ANY),
            scratch_shapes=[pltpu.SemaphoreType.DMA((BLOCKS * CAP,))],
        ),
        out_shape=jax.ShapeDtypeStruct((BLOCKS * CAP * TOK, width), bf16),
        compiler_params=params(),
        name="send",
    )(pick, kv)


def attend_body(
    read_ref, add_ref, bias_ref, q_ref, g_ref, own_ref, prev_ref, slot_ref,
    o_ref, dq_ref, down_ref, rim_ref, dslot_ref,
    acc_own, acc_prev, acc_slot, kv_scr, s_scr, gp_scr, half_scr, ds_scr,
):
    scale = HEAD ** (-0.5)
    acc_own[...] = jnp.zeros_like(acc_own)
    acc_prev[...] = jnp.zeros_like(acc_prev)
    acc_slot[...] = jnp.zeros_like(acc_slot)
    spans = [slice(f * TOK, (f + 1) * TOK) for f in range(FRAMES)]
    for f, rows in enumerate(spans):
        at = 0
        if f < BAND:
            at = (BAND - f) * TOK
            kv_scr[f, :at, :] = prev_ref[f * TOK : BAND * TOK, :]
        kv_scr[f, at : (BAND + 1) * TOK, :] = own_ref[max(f - BAND, 0) * TOK : (f + 1) * TOK, :]
        for m in range(MEM):
            at = pl.multiple_of(read_ref[f * MEM + m] * TOK, TOK)
            kv_scr[f, (BAND + 1 + m) * TOK : (BAND + 2 + m) * TOK, :] = slot_ref[pl.ds(at, TOK), :]
    for f, rows in enumerate(spans):
        s_scr[rows, :] = dot_last(q_ref[rows, :], kv_scr[f, :, :HEAD]) * scale + bias_ref[f : f + 1, :]
        gp_scr[rows, :] = dot_last(g_ref[rows, :], kv_scr[f, :, HEAD:])
    for rows in spans:
        s = s_scr[rows, :]
        gp = gp_scr[rows, :]
        e = jnp.exp(s - jnp.max(s, axis=1, keepdims=True))
        w = e * (1.0 / jnp.sum(e, axis=1, keepdims=True))
        half_scr[rows, :] = w.astype(bf16)
        ds_scr[rows, :] = (w * (gp - jnp.sum(w * gp, axis=1, keepdims=True))).astype(bf16)
    for f, rows in enumerate(spans):
        o_ref[rows, :] = dot(half_scr[rows, :], kv_scr[f, :, HEAD:]).astype(bf16)
        dq_ref[rows, :] = (dot(ds_scr[rows, :], kv_scr[f, :, :HEAD]) * scale).astype(bf16)
    for f, rows in enumerate(spans):
        dk = dot_first(ds_scr[rows, :], q_ref[rows, :]) * scale
        dv = dot_first(half_scr[rows, :], g_ref[rows, :])
        start = 0
        own = slice(max(f - BAND, 0) * TOK, (f + 1) * TOK)
        if f < BAND:
            start = (BAND - f) * TOK
            prev = slice(f * TOK, BAND * TOK)
            acc_prev[prev, :HEAD] += dk[:start]
            acc_prev[prev, HEAD:] += dv[:start]
        acc_own[own, :HEAD] += dk[start : (BAND + 1) * TOK]
        acc_own[own, HEAD:] += dv[start : (BAND + 1) * TOK]
        spots = [pl.multiple_of(add_ref[f * MEM + m] * TOK, TOK) for m in range(MEM)]
        base = (BAND + 1) * TOK
        for d, cols in ((dk, slice(0, HEAD)), (dv, slice(HEAD, 2 * HEAD))):
            olds = [acc_slot[pl.ds(at, TOK), cols] for at in spots]
            for m, at in enumerate(spots):
                acc_slot[pl.ds(at, TOK), cols] = olds[m] + d[base + m * TOK : base + (m + 1) * TOK]
    down_ref[...] = acc_own[...]
    rim_ref[...] = acc_prev[...].astype(bf16)
    dslot_ref[...] = acc_slot[: SPARE * TOK, :].astype(bf16)


def attend(read, add, bias, q, g, own, prev, slots, first, heads):
    col = lambda rows, width: pl.BlockSpec((rows, width), lambda h, *_: (0, h))
    src = lambda rows, width: pl.BlockSpec((rows, width), lambda h, *_: (0, h + first))
    return pl.pallas_call(
        attend_body,
        grid_spec=pltpu.PrefetchScalarGridSpec(
            num_scalar_prefetch=2,
            grid=(heads,),
            in_specs=[
                pl.BlockSpec(bias.shape, lambda h, *_: (0, 0)),
                src(ROWS, HEAD), src(ROWS, HEAD),
                src(ROWS, 2 * HEAD), src(BAND * TOK, 2 * HEAD), src(SPARE * TOK, 2 * HEAD),
            ],
            out_specs=[
                col(ROWS, HEAD), col(ROWS, HEAD),
                col(ROWS, 2 * HEAD), col(BAND * TOK, 2 * HEAD), col(SPARE * TOK, 2 * HEAD),
            ],
            scratch_shapes=[
                pltpu.VMEM((ROWS, 2 * HEAD), f32),
                pltpu.VMEM((BAND * TOK, 2 * HEAD), f32),
                pltpu.VMEM(((SPARE + 1) * TOK, 2 * HEAD), f32),
                pltpu.VMEM((FRAMES, KEYS, 2 * HEAD), bf16),
                pltpu.VMEM((ROWS, KEYS), f32),
                pltpu.VMEM((ROWS, KEYS), f32),
                pltpu.VMEM((ROWS, KEYS), bf16),
                pltpu.VMEM((ROWS, KEYS), bf16),
            ],
        ),
        out_shape=[
            jax.ShapeDtypeStruct((ROWS, heads * HEAD), bf16),
            jax.ShapeDtypeStruct((ROWS, heads * HEAD), bf16),
            jax.ShapeDtypeStruct((ROWS, 2 * heads * HEAD), f32),
            jax.ShapeDtypeStruct((BAND * TOK, 2 * heads * HEAD), bf16),
            jax.ShapeDtypeStruct((SPARE * TOK, 2 * heads * HEAD), bf16),
        ],
        compiler_params=params(),
        name="attend",
    )(read, add, bias, q, g, own, prev, slots)


def collect_body(pick_ref, own_ref, rim_ref, back_ref, out_ref, acc):
    acc[:ROWS, :] = own_ref[...]
    acc[ROWS:, :] = jnp.zeros_like(acc[ROWS:, :])
    tail = slice((FRAMES - BAND) * TOK, ROWS)
    acc[tail, :] += rim_ref[...].astype(f32)
    for i in range(BLOCKS * CAP):
        at = pl.multiple_of(pick_ref[i] * TOK, TOK)
        acc[pl.ds(at, TOK), :] += back_ref[i * TOK : (i + 1) * TOK, :].astype(f32)
    for h in range(own_ref.shape[1] // (2 * HEAD)):
        for kind in range(2):
            left = (2 * h + kind) * HEAD
            out_ref[kind, :, h * HEAD : (h + 1) * HEAD] = acc[:ROWS, left : left + HEAD].astype(bf16)


def collect(pick, own, rim, back):
    width = own.shape[1]
    cols = min(512, width)
    col = lambda rows, w: pl.BlockSpec((rows, w), lambda h, *_: (0, h))
    return pl.pallas_call(
        collect_body,
        grid_spec=pltpu.PrefetchScalarGridSpec(
            num_scalar_prefetch=1,
            grid=(width // cols,),
            in_specs=[col(ROWS, cols), col(BAND * TOK, cols), col(SPARE * TOK, cols)],
            out_specs=pl.BlockSpec((2, ROWS, cols // 2), lambda h, *_: (0, 0, h)),
            scratch_shapes=[pltpu.VMEM((ROWS + TOK, cols), f32)],
        ),
        out_shape=jax.ShapeDtypeStruct((2, ROWS, width // 2), bf16),
        compiler_params=params(),
        name="collect",
    )(pick, own, rim, back)


LANES = 512


def taken(right):
    if right.ndim == 3:
        rows, n = right.shape[1:]
        return n, pl.BlockSpec((None, rows, n), lambda i, s, *_: (s[1], 0, 0))
    rows, n = right.shape
    return n // 2, pl.BlockSpec((rows, n // 2), lambda i, s, *_: (0, s[1]))


def packed_rows(rows, n):
    return rows * n // LANES


def packed(part):
    rows, n = part.shape
    if n >= LANES:
        return jnp.concatenate([part[:, at : at + LANES] for at in range(0, n, LANES)], axis=0)
    return jnp.concatenate([part[: rows // 2], part[rows // 2 :]], axis=1)


def unpacked(x, n):
    if n >= LANES:
        return jnp.concatenate(jnp.split(x, n // LANES, axis=-2), axis=-1)
    return jnp.concatenate([x[..., :n], x[..., n:]], axis=-2)


def partial_call(pairs, scalars, got=None, by_chip=True, extra=None):
    per = 4
    steps = BLOCKS // per
    chips = CHIPS if by_chip else 1
    cuts = [taken(right) for _, right in pairs]
    across = [left.shape[0] == right.shape[-2] for left, right in pairs]
    shards = [left.shape[1 if a else 0] // BLOCKS for (left, _), a in zip(pairs, across)]
    height = sum(packed_rows(s // chips, n) for (n, _), s in zip(cuts, shards))
    keep = got is not None

    def body(chip_ref, *refs):
        factors, refs = refs[: 2 * len(pairs)], refs[2 * len(pairs) :]
        totals = refs[-len(pairs) :]
        for k, total in enumerate(totals):
            product = dot_first if across[k] else dot
            total[...] = product(factors[2 * k][...], factors[2 * k + 1][...])

        def write(half):
            for t in range(per):
                for d in range(chips):
                    c = lax.rem(chip_ref[0] + d, CHIPS) if keep and by_chip else d
                    parts = []
                    for total, shard in zip(totals, shards):
                        piece = shard // chips
                        first = t * shard + c * piece
                        if keep and by_chip:
                            first = pl.multiple_of(first, piece)
                        parts.append(packed(total[pl.ds(first, piece), :]))
                    part = parts[0] if len(parts) == 1 else jnp.concatenate(parts, axis=0)
                    if not by_chip:
                        if keep:
                            part = part + refs[0][t].astype(f32)
                        out_ref = refs[-1 - len(totals)]
                        if extra is None:
                            out_ref[t] = part.astype(bf16)
                        else:
                            more = extra.shape[1]
                            out_ref[t, :more, :] = refs[1][t]
                            out_ref[t, more:, :] = part.astype(bf16)
                    elif keep:
                        part = part + refs[0][c, t].astype(f32)
                        refs[1 + 2 * d + half][t] = part.astype(bf16)
                    else:
                        refs[0][c, t] = part.astype(bf16)

        if keep and by_chip:
            early = pl.program_id(0) < steps // 2
            pl.when(early)(lambda: write(0))
            pl.when(jnp.logical_not(early))(lambda: write(1))
        else:
            write(0)

    if by_chip:
        whole = pl.BlockSpec((CHIPS, per, height, LANES), lambda i, *_: (0, i, 0, 0))
        shape = (CHIPS, BLOCKS, height, LANES)
    else:
        whole = pl.BlockSpec((per, height, LANES), lambda i, *_: (i, 0, 0))
        shape = (BLOCKS, height, LANES)
    in_specs, operands = [], []
    for (left, right), shard, (_, spec), a in zip(pairs, shards, cuts, across):
        if a:
            in_specs += [pl.BlockSpec((left.shape[0], per * shard), lambda i, *_: (0, i)), spec]
        else:
            in_specs += [pl.BlockSpec((per * shard, left.shape[1]), lambda i, *_: (i, 0)), spec]
        operands += [left, right]
    out_specs, out_shape = whole, jax.ShapeDtypeStruct(shape, bf16)
    if keep:
        in_specs.append(whole)
        operands.append(got)
        if extra is not None:
            more = extra.shape[1]
            in_specs.append(pl.BlockSpec((per, more, LANES), lambda i, *_: (i, 0, 0)))
            operands.append(extra)
            out_specs = pl.BlockSpec((per, more + height, LANES), lambda i, *_: (i, 0, 0))
            out_shape = jax.ShapeDtypeStruct((BLOCKS, more + height, LANES), bf16)
        if by_chip:
            halves = [
                pl.BlockSpec((per, height, LANES), lambda i, *_: (jnp.minimum(i, steps // 2 - 1), 0, 0)),
                pl.BlockSpec((per, height, LANES), lambda i, *_: (jnp.maximum(i - steps // 2, 0), 0, 0)),
            ]
            out_specs = halves * CHIPS
            out_shape = [jax.ShapeDtypeStruct((BLOCKS // 2, height, LANES), bf16)] * (2 * CHIPS)
    return pl.pallas_call(
        body,
        grid_spec=pltpu.PrefetchScalarGridSpec(
            num_scalar_prefetch=1,
            grid=(steps,),
            in_specs=in_specs,
            out_specs=out_specs,
            scratch_shapes=[
                pltpu.VMEM((per * s, n), f32) for (n, _), s in zip(cuts, shards)
            ],
        ),
        out_shape=out_shape,
        compiler_params=params(),
    )(scalars, *operands)


def other_core(x):
    return lax.ppermute(x, "roll", [(i, i ^ 1) for i in range(lax.axis_size("roll"))])


def from_behind(block, distance):
    return lax.ppermute(
        block, "tm", [(i - distance, i) for i in range(BLOCKS) if 0 <= i - distance < BLOCKS]
    )


def exchange(x, axis="tm", groups=None):
    return lax.all_to_all(
        x, axis, split_axis=0, concat_axis=0, tiled=True, axis_index_groups=groups
    )


def summed(parts):
    return jnp.sum(parts.astype(f32), axis=0).astype(bf16)


def along_chips(x, d):
    n = 2 * CHIPS
    return lax.ppermute(x, "roll", [(i, (i + 2 * d) % n) for i in range(n)])


def plus(a, b):
    return (a.astype(f32) + b.astype(f32)).astype(bf16)


def over_chips(pieces):
    own0, own1, next0, next1, far0, far1, last0, last1 = pieces
    up, down = along_chips(far0, 1), along_chips(far1, -1)
    from_next, from_last = along_chips(next1, 1), along_chips(last0, -1)
    came0 = along_chips(plus(next0, up), 1)
    came1 = along_chips(plus(last1, down), -1)
    half0 = own0.astype(f32) + from_last.astype(f32) + came0.astype(f32)
    half1 = own1.astype(f32) + from_next.astype(f32) + came1.astype(f32)
    return jnp.concatenate([half0.astype(bf16), half1.astype(bf16)], axis=0)


def everyone(x):
    parts = exchange(jnp.broadcast_to(x, (2 * CHIPS, *x.shape)), "roll")
    return parts.reshape(CHIPS, 2, *x.shape)


def slots_exchange(x):
    return exchange(x.reshape(BLOCKS, CAP * TOK, x.shape[1])).reshape(x.shape)


def step(inputs, cotangent, memory_lists, w_query, w_key, w_value, w_output):
    model_width = inputs.shape[-1]
    inner = w_query.shape[1]
    half = inner // 2
    position = lax.axis_index("tm")
    core = lax.axis_index("roll") % 2
    chip = lax.axis_index("roll") // 2
    keeping = jnp.stack([chip, core]).astype(jnp.int32)
    sending = jnp.stack([chip, 1 - core]).astype(jnp.int32)
    x = inputs.reshape(ROWS, model_width)
    cot = cotangent.reshape(ROWS, model_width)
    x_t = x.T
    recalled = memory_lists[0]
    first_frame = position * FRAMES

    targets = jnp.arange(BLOCKS * FRAMES, dtype=jnp.int32)
    wanted = jnp.any(recalled.reshape(-1, 1) == targets[None, :], axis=0)
    wanted = wanted.astype(jnp.int32).reshape(BLOCKS, FRAMES)
    asked = exchange(wanted)

    keyval = keyval_rows(x, w_key, w_value)
    before = from_behind(keyval[(FRAMES - BAND) * TOK :], 1)
    queries = jnp.dot(x, w_query, preferred_element_type=f32).astype(bf16)
    grad_heads = dot_last(cot, w_output).astype(bf16)

    slot_rank = jnp.cumsum(wanted, axis=1) - 1
    slot_table = (jnp.arange(BLOCKS, dtype=jnp.int32)[:, None] * CAP + slot_rank).reshape(-1)
    mem_ok = recalled >= 0
    flat = jnp.where(mem_ok, recalled, 0).reshape(-1)
    hit = flat[:, None] == targets[None, :]
    slot_ids = jnp.sum(jnp.where(hit, slot_table[None, :], 0), axis=1)
    ok_flat = mem_ok.reshape(-1)
    read = jnp.clip(jnp.where(ok_flat, slot_ids, 0), 0, SPARE - 1)
    add = jnp.clip(jnp.where(ok_flat, slot_ids, SPARE), 0, SPARE)
    band_index = (
        jnp.arange(FRAMES, dtype=jnp.int32)[:, None] + jnp.arange(BAND + 1, dtype=jnp.int32)[None, :]
    )
    band_ok = first_frame + band_index - BAND >= 0
    key_valid = jnp.concatenate([band_ok, mem_ok], axis=1)
    bias = jnp.repeat(jnp.where(key_valid, 0.0, masked_score).astype(f32), TOK, axis=1)

    asked_rank = jnp.cumsum(asked, axis=1) - 1
    places = jnp.arange(CAP, dtype=jnp.int32)[None, :, None]
    chosen = (asked[:, None, :] > 0) & (asked_rank[:, None, :] == places)
    frame_no = jnp.arange(FRAMES, dtype=jnp.int32)[None, None, :]
    pick = jnp.sum(jnp.where(chosen, frame_no, 0), axis=2).reshape(-1)
    pick_add = jnp.where(jnp.any(chosen, axis=2).reshape(-1), pick, FRAMES)

    outgoing = named_frames(pick, keyval)
    slots = slots_exchange(outgoing)
    heads, dqs, owns, passed, returned = [], [], [], [], []
    first = 0
    for count in SPLIT:
        heads_g, dq_g, own_g, rim_g, dslot_g = attend(
            read, add, bias, queries, grad_heads, keyval, before, slots, first, count
        )
        passed.append(from_behind(rim_g, -1))
        returned.append(slots_exchange(dslot_g))
        heads.append(heads_g)
        dqs.append(dq_g)
        owns.append(own_g)
        first += count

    heads_out = jnp.concatenate(heads, axis=1)
    grad_query = jnp.concatenate(dqs, axis=1)
    sent = partial_call([(x_t, grad_query), (heads_out, cot)], sending)
    got = other_core(sent)
    kept = partial_call([(x_t, grad_query), (heads_out, cot)], keeping, got)
    sum_qo = over_chips(kept)
    share_qo = summed(exchange(sum_qo))
    both = everyone(share_qo).astype(f32)
    attended = jnp.dot(heads_out, w_output, preferred_element_type=f32).astype(bf16)
    grad_input = dot_last(grad_query, w_query)
    piece = model_width // BLOCKS // CHIPS
    q_rows = packed_rows(piece, half)
    total_q, total_o = (
        jnp.concatenate([cut[:, c].reshape(-1, cut.shape[-1]) for c in range(2)], axis=1)
        for cut in (
            unpacked(both[:, :, :q_rows], half),
            unpacked(both[:, :, q_rows:], model_width // 2),
        )
    )

    dks, dvs, sums = [], [], []
    for g, count in enumerate(SPLIT):
        last = g == len(SPLIT) - 1
        dkv = collect(pick_add, owns[g], passed[g], returned[g])
        dks.append(dkv[0])
        dvs.append(dkv[1])
        sent = partial_call([(x_t, dkv)], sending, by_chip=not last)
        got = other_core(sent)
        extra = jnp.concatenate(sums, axis=1) if last else None
        kept = partial_call([(x_t, dkv)], keeping, got, not last, extra)
        if not last:
            sums.append(over_chips(kept))
    late = summed(exchange(kept))
    both = everyone(late).astype(f32)
    at, cols = 0, []
    for g, count in enumerate(SPLIT):
        width = count * HEAD
        if g < len(SPLIT) - 1:
            size = packed_rows(piece, width)
            cut = unpacked(both[:, :, at : at + size], width)
            cols.append([cut[:, c].reshape(-1, width) for c in range(2)])
            at += size
        else:
            cols.append(unpacked(jnp.sum(both[:, :, at:], axis=0), width))
    total_k, total_v = (jnp.concatenate([c[kind] for c in cols], axis=1) for kind in range(2))
    grad_input = (
        grad_input
        + dot_last(jnp.concatenate(dks, axis=1), w_key)
        + dot_last(jnp.concatenate(dvs, axis=1), w_value)
    )
    shape = (1, FRAMES, TOK, model_width)
    return (
        attended.reshape(shape),
        grad_input.astype(bf16).reshape(shape),
        total_q,
        total_k,
        total_v,
        total_o,
    )


def solution(mesh):
    block = P("roll", "tm", None, None)
    return jax.shard_map(
        step,
        mesh=mesh,
        in_specs=(block, block, P("roll", "tm", None), P(), P(), P(), P()),
        out_specs=(block, block, P("tm", None), P("tm", None), P("tm", None), P("tm", None)),
        check_vma=False,
    )
```

```python
import jax
import jax.numpy as jnp
from jax import lax
from jax.experimental import pallas as pl
from jax.experimental.pallas import tpu as pltpu
from jax.sharding import PartitionSpec as P


HEADS = 8
HEAD = 128
BAND = 4
MEM = 8
CAP = 3
FRAMES = 8
TOK = 32
BLOCKS = 16
ROWS = FRAMES * TOK
SPLIT = (5, 3)
KEYS = (BAND + 1 + MEM) * TOK
CHIPS = 4
SPARE = BLOCKS * CAP
masked_score = -1e30
f32, bf16 = jnp.float32, jnp.bfloat16
VMEM_LIMIT = 60 * 1024 * 1024


def params(n=1):
    return pltpu.CompilerParams(
        dimension_semantics=("arbitrary",) * n, vmem_limit_bytes=VMEM_LIMIT
    )


def dot_last(left, right):
    return lax.dot_general(left, right, (((1,), (1,)), ((), ())), preferred_element_type=f32)


def dot_first(left, right):
    return lax.dot_general(left, right, (((0,), (0,)), ((), ())), preferred_element_type=f32)


def dot(left, right):
    return lax.dot_general(left, right, (((1,), (0,)), ((), ())), preferred_element_type=f32)


def keyval_body(x_ref, wk_ref, wv_ref, out_ref):
    pieces = []
    for h in range(wk_ref.shape[1] // HEAD):
        pieces += [wk_ref[:, h * HEAD : (h + 1) * HEAD], wv_ref[:, h * HEAD : (h + 1) * HEAD]]
    out_ref[...] = dot(x_ref[...], jnp.concatenate(pieces, axis=1)).astype(bf16)


def keyval_rows(x, w_key, w_value):
    rows, width = x.shape
    cols = 256
    return pl.pallas_call(
        keyval_body,
        grid=(w_key.shape[1] // cols,),
        in_specs=[
            pl.BlockSpec((rows, width), lambda j: (0, 0)),
            pl.BlockSpec((width, cols), lambda j: (0, j)),
            pl.BlockSpec((width, cols), lambda j: (0, j)),
        ],
        out_specs=pl.BlockSpec((rows, 2 * cols), lambda j: (0, j)),
        out_shape=jax.ShapeDtypeStruct((rows, 2 * w_key.shape[1]), bf16),
        compiler_params=params(),
        name="keyval",
    )(x, w_key, w_value)


def send_body(pick_ref, kv_ref, out_ref, sem):
    def copy(i):
        at = pl.multiple_of(pick_ref[i] * TOK, TOK)
        return pltpu.make_async_copy(
            kv_ref.at[pl.ds(at, TOK), :], out_ref.at[pl.ds(i * TOK, TOK), :], sem.at[i]
        )

    for i in range(BLOCKS * CAP):
        copy(i).start()
    for i in range(BLOCKS * CAP):
        copy(i).wait()


def named_frames(pick, kv):
    width = kv.shape[1]
    return pl.pallas_call(
        send_body,
        grid_spec=pltpu.PrefetchScalarGridSpec(
            num_scalar_prefetch=1,
            grid=(1,),
            in_specs=[pl.BlockSpec((ROWS, width), lambda i, *_: (0, 0))],
            out_specs=pl.BlockSpec(memory_space=pl.ANY),
            scratch_shapes=[pltpu.SemaphoreType.DMA((BLOCKS * CAP,))],
        ),
        out_shape=jax.ShapeDtypeStruct((BLOCKS * CAP * TOK, width), bf16),
        compiler_params=params(),
        name="send",
    )(pick, kv)


def attend_body(
    read_ref, add_ref, bias_ref, q_ref, g_ref, own_ref, prev_ref, slot_ref, *refs
):
    attend_head(
        read_ref, add_ref, bias_ref, q_ref, g_ref, own_ref, prev_ref, slot_ref, *refs[-13:]
    )


def attend_head(
    read_ref, add_ref, bias_ref, q_ref, g_ref, own_ref, prev_ref, slot_ref,
    o_ref, dq_ref, down_ref, rim_ref, dslot_ref,
    acc_own, acc_prev, acc_slot, kv_scr, s_scr, gp_scr, half_scr, ds_scr,
):
    scale = HEAD ** (-0.5)
    acc_own[...] = jnp.zeros_like(acc_own)
    acc_prev[...] = jnp.zeros_like(acc_prev)
    acc_slot[...] = jnp.zeros_like(acc_slot)
    spans = [slice(f * TOK, (f + 1) * TOK) for f in range(FRAMES)]
    for f, rows in enumerate(spans):
        at = 0
        if f < BAND:
            at = (BAND - f) * TOK
            kv_scr[f, :at, :] = prev_ref[f * TOK : BAND * TOK, :]
        kv_scr[f, at : (BAND + 1) * TOK, :] = own_ref[max(f - BAND, 0) * TOK : (f + 1) * TOK, :]
        for m in range(MEM):
            at = pl.multiple_of(read_ref[f * MEM + m] * TOK, TOK)
            kv_scr[f, (BAND + 1 + m) * TOK : (BAND + 2 + m) * TOK, :] = slot_ref[pl.ds(at, TOK), :]
    for f, rows in enumerate(spans):
        s_scr[rows, :] = dot_last(q_ref[rows, :], kv_scr[f, :, :HEAD]) * scale + bias_ref[f : f + 1, :]
        gp_scr[rows, :] = dot_last(g_ref[rows, :], kv_scr[f, :, HEAD:])
    for rows in spans:
        s = s_scr[rows, :]
        gp = gp_scr[rows, :]
        e = jnp.exp(s - jnp.max(s, axis=1, keepdims=True))
        w = e * (1.0 / jnp.sum(e, axis=1, keepdims=True))
        half_scr[rows, :] = w.astype(bf16)
        ds_scr[rows, :] = (w * (gp - jnp.sum(w * gp, axis=1, keepdims=True))).astype(bf16)
    for f, rows in enumerate(spans):
        o_ref[rows, :] = dot(half_scr[rows, :], kv_scr[f, :, HEAD:]).astype(bf16)
        dq_ref[rows, :] = (dot(ds_scr[rows, :], kv_scr[f, :, :HEAD]) * scale).astype(bf16)
    for f, rows in enumerate(spans):
        dk = dot_first(ds_scr[rows, :], q_ref[rows, :]) * scale
        dv = dot_first(half_scr[rows, :], g_ref[rows, :])
        start = 0
        own = slice(max(f - BAND, 0) * TOK, (f + 1) * TOK)
        if f < BAND:
            start = (BAND - f) * TOK
            prev = slice(f * TOK, BAND * TOK)
            acc_prev[prev, :HEAD] += dk[:start]
            acc_prev[prev, HEAD:] += dv[:start]
        acc_own[own, :HEAD] += dk[start : (BAND + 1) * TOK]
        acc_own[own, HEAD:] += dv[start : (BAND + 1) * TOK]
        spots = [pl.multiple_of(add_ref[f * MEM + m] * TOK, TOK) for m in range(MEM)]
        base = (BAND + 1) * TOK
        for d, cols in ((dk, slice(0, HEAD)), (dv, slice(HEAD, 2 * HEAD))):
            olds = [acc_slot[pl.ds(at, TOK), cols] for at in spots]
            for m, at in enumerate(spots):
                acc_slot[pl.ds(at, TOK), cols] = olds[m] + d[base + m * TOK : base + (m + 1) * TOK]
    down_ref[...] = acc_own[...]
    rim_ref[...] = acc_prev[...].astype(bf16)
    dslot_ref[...] = acc_slot[: SPARE * TOK, :].astype(bf16)


def attend(read, add, bias, q, g, own, prev, slots, first, heads, written):
    col = lambda rows, width: pl.BlockSpec((rows, width), lambda h, *_: (0, h))
    src = lambda rows, width: pl.BlockSpec((rows, width), lambda h, *_: (0, h + first))
    return pl.pallas_call(
        attend_body,
        grid_spec=pltpu.PrefetchScalarGridSpec(
            num_scalar_prefetch=2,
            grid=(heads,),
            in_specs=[
                pl.BlockSpec(bias.shape, lambda h, *_: (0, 0)),
                src(ROWS, HEAD), src(ROWS, HEAD),
                src(ROWS, 2 * HEAD), src(BAND * TOK, 2 * HEAD), src(SPARE * TOK, 2 * HEAD),
            ] + [pl.BlockSpec(memory_space=pl.ANY)] * len(written),
            out_specs=[
                src(ROWS, HEAD), src(ROWS, HEAD),
                col(ROWS, 2 * HEAD), col(BAND * TOK, 2 * HEAD), col(SPARE * TOK, 2 * HEAD),
            ],
            scratch_shapes=[
                pltpu.VMEM((ROWS, 2 * HEAD), f32),
                pltpu.VMEM((BAND * TOK, 2 * HEAD), f32),
                pltpu.VMEM(((SPARE + 1) * TOK, 2 * HEAD), f32),
                pltpu.VMEM((FRAMES, KEYS, 2 * HEAD), bf16),
                pltpu.VMEM((ROWS, KEYS), f32),
                pltpu.VMEM((ROWS, KEYS), f32),
                pltpu.VMEM((ROWS, KEYS), bf16),
                pltpu.VMEM((ROWS, KEYS), bf16),
            ],
        ),
        out_shape=[
            jax.ShapeDtypeStruct(q.shape, bf16),
            jax.ShapeDtypeStruct(q.shape, bf16),
            jax.ShapeDtypeStruct((ROWS, 2 * heads * HEAD), f32),
            jax.ShapeDtypeStruct((BAND * TOK, 2 * heads * HEAD), bf16),
            jax.ShapeDtypeStruct((SPARE * TOK, 2 * heads * HEAD), bf16),
        ],
        input_output_aliases={8 + k: k for k in range(len(written))},
        compiler_params=params(),
        name="attend",
    )(read, add, bias, q, g, own, prev, slots, *written)


def collect_body(pick_ref, own_ref, rim_ref, back_ref, out_ref, acc):
    acc[:ROWS, :] = own_ref[...]
    acc[ROWS:, :] = jnp.zeros_like(acc[ROWS:, :])
    tail = slice((FRAMES - BAND) * TOK, ROWS)
    acc[tail, :] += rim_ref[...].astype(f32)
    for i in range(BLOCKS * CAP):
        at = pl.multiple_of(pick_ref[i] * TOK, TOK)
        acc[pl.ds(at, TOK), :] += back_ref[i * TOK : (i + 1) * TOK, :].astype(f32)
    for h in range(own_ref.shape[1] // (2 * HEAD)):
        for kind in range(2):
            left = (2 * h + kind) * HEAD
            out_ref[kind, :, h * HEAD : (h + 1) * HEAD] = acc[:ROWS, left : left + HEAD].astype(bf16)


def collect(pick, own, rim, back):
    width = own.shape[1]
    cols = 2 * HEAD
    col = lambda rows, w: pl.BlockSpec((rows, w), lambda h, *_: (0, h))
    return pl.pallas_call(
        collect_body,
        grid_spec=pltpu.PrefetchScalarGridSpec(
            num_scalar_prefetch=1,
            grid=(width // cols,),
            in_specs=[col(ROWS, cols), col(BAND * TOK, cols), col(SPARE * TOK, cols)],
            out_specs=pl.BlockSpec((2, ROWS, cols // 2), lambda h, *_: (0, 0, h)),
            scratch_shapes=[pltpu.VMEM((ROWS + TOK, cols), f32)],
        ),
        out_shape=jax.ShapeDtypeStruct((2, ROWS, width // 2), bf16),
        compiler_params=params(),
        name="collect",
    )(pick, own, rim, back)


LANES = HEAD


def taken(right):
    if right.ndim == 3:
        rows, n = right.shape[1:]
        return n, pl.BlockSpec((None, rows, n), lambda i, s, *_: (s[1], 0, 0))
    rows, n = right.shape
    return n // 2, pl.BlockSpec((rows, n // 2), lambda i, s, *_: (0, s[1]))


def packed_rows(rows, n):
    return rows * n // LANES


def packed(part):
    return jnp.concatenate([part[:, at : at + LANES] for at in range(0, part.shape[1], LANES)], axis=0)


def partial_call(pairs, scalars, got=None, by_chip=True, extra=None):
    per = 8
    steps = BLOCKS // per
    chips = CHIPS if by_chip else 1
    cuts = [taken(right) for _, right in pairs]
    across = [left.shape[0] == right.shape[-2] for left, right in pairs]
    shards = [left.shape[1 if a else 0] // BLOCKS for (left, _), a in zip(pairs, across)]
    height = sum(packed_rows(s // chips, n) for (n, _), s in zip(cuts, shards))
    keep = got is not None

    def body(chip_ref, *refs):
        factors, refs = refs[: 2 * len(pairs)], refs[2 * len(pairs) :]
        totals = refs[-len(pairs) :]
        for k, total in enumerate(totals):
            product = dot_first if across[k] else dot
            total[...] = product(factors[2 * k][...], factors[2 * k + 1][...])

        def write(half):
            for t in range(per):
                for d in range(chips):
                    c = lax.rem(chip_ref[0] + d, CHIPS) if keep and by_chip else d
                    parts = []
                    for total, shard in zip(totals, shards):
                        piece = shard // chips
                        first = t * shard + c * piece
                        if keep and by_chip:
                            first = pl.multiple_of(first, piece)
                        parts.append(packed(total[pl.ds(first, piece), :]))
                    part = parts[0] if len(parts) == 1 else jnp.concatenate(parts, axis=0)
                    if not by_chip:
                        if keep:
                            part = part + refs[0][t].astype(f32)
                        out_ref = refs[-1 - len(totals)]
                        if extra is None:
                            out_ref[t] = part.astype(bf16)
                        else:
                            more = extra.shape[1]
                            out_ref[t, :more, :] = refs[1][t]
                            out_ref[t, more:, :] = part.astype(bf16)
                    elif keep:
                        part = part + refs[0][c, t].astype(f32)
                        refs[1 + 2 * d + half][t] = part.astype(bf16)
                    else:
                        refs[0][c, t] = part.astype(bf16)

        if keep and by_chip:
            early = pl.program_id(0) < steps // 2
            pl.when(early)(lambda: write(0))
            pl.when(jnp.logical_not(early))(lambda: write(1))
        else:
            write(0)

    if by_chip:
        whole = pl.BlockSpec((CHIPS, per, height, LANES), lambda i, *_: (0, i, 0, 0))
        shape = (CHIPS, BLOCKS, height, LANES)
    else:
        whole = pl.BlockSpec((per, height, LANES), lambda i, *_: (i, 0, 0))
        shape = (BLOCKS, height, LANES)
    in_specs, operands = [], []
    for (left, right), shard, (_, spec), a in zip(pairs, shards, cuts, across):
        if a:
            in_specs += [pl.BlockSpec((left.shape[0], per * shard), lambda i, *_: (0, i)), spec]
        else:
            in_specs += [pl.BlockSpec((per * shard, left.shape[1]), lambda i, *_: (i, 0)), spec]
        operands += [left, right]
    out_specs, out_shape = whole, jax.ShapeDtypeStruct(shape, bf16)
    if keep:
        in_specs.append(whole)
        operands.append(got)
        if extra is not None:
            more = extra.shape[1]
            in_specs.append(pl.BlockSpec((per, more, LANES), lambda i, *_: (i, 0, 0)))
            operands.append(extra)
            out_specs = pl.BlockSpec((per, more + height, LANES), lambda i, *_: (i, 0, 0))
            out_shape = jax.ShapeDtypeStruct((BLOCKS, more + height, LANES), bf16)
        if by_chip:
            halves = [
                pl.BlockSpec((per, height, LANES), lambda i, *_: (jnp.minimum(i, steps // 2 - 1), 0, 0)),
                pl.BlockSpec((per, height, LANES), lambda i, *_: (jnp.maximum(i - steps // 2, 0), 0, 0)),
            ]
            out_specs = halves * CHIPS
            out_shape = [jax.ShapeDtypeStruct((BLOCKS // 2, height, LANES), bf16)] * (2 * CHIPS)
    return pl.pallas_call(
        body,
        grid_spec=pltpu.PrefetchScalarGridSpec(
            num_scalar_prefetch=1,
            grid=(steps,),
            in_specs=in_specs,
            out_specs=out_specs,
            scratch_shapes=[
                pltpu.VMEM((per * s, n), f32) for (n, _), s in zip(cuts, shards)
            ],
        ),
        out_shape=out_shape,
        compiler_params=params(),
    )(scalars, *operands)


def other_core(x):
    return lax.ppermute(x, "roll", [(i, i ^ 1) for i in range(lax.axis_size("roll"))])


def from_behind(block, distance):
    return lax.ppermute(
        block, "tm", [(i - distance, i) for i in range(BLOCKS) if 0 <= i - distance < BLOCKS]
    )


def exchange(x, axis="tm", groups=None):
    return lax.all_to_all(
        x, axis, split_axis=0, concat_axis=0, tiled=True, axis_index_groups=groups
    )


def summed(parts):
    return jnp.sum(parts.astype(f32), axis=0).astype(bf16)


def along_chips(x, d):
    n = 2 * CHIPS
    return lax.ppermute(x, "roll", [(i, (i + 2 * d) % n) for i in range(n)])


def plus(a, b):
    return (a.astype(f32) + b.astype(f32)).astype(bf16)


def over_chips(pieces):
    own0, own1, next0, next1, far0, far1, last0, last1 = pieces
    up, down = along_chips(far0, 1), along_chips(far1, -1)
    from_next, from_last = along_chips(next1, 1), along_chips(last0, -1)
    came0 = along_chips(plus(next0, up), 1)
    came1 = along_chips(plus(last1, down), -1)
    half0 = own0.astype(f32) + from_last.astype(f32) + came0.astype(f32)
    half1 = own1.astype(f32) + from_next.astype(f32) + came1.astype(f32)
    return jnp.concatenate([half0.astype(bf16), half1.astype(bf16)], axis=0)


def everyone(x, ordered, scalars):
    came = [x] + [along_chips(x, d) for d in range(1, CHIPS)]
    rows = x.shape[0]

    def body(s_ref, *refs):
        out_ref = refs[-1]
        for d in range(CHIPS):
            at = pl.multiple_of(lax.rem(s_ref[0] + CHIPS - d, CHIPS) * ordered, ordered)
            out_ref[pl.ds(at, ordered), :] = refs[d][:ordered, :]
        if ordered < rows:
            total = refs[0][ordered:, :].astype(f32)
            for d in range(1, CHIPS):
                total = total + refs[d][ordered:, :].astype(f32)
            out_ref[CHIPS * ordered :, :] = total.astype(bf16)

    height = CHIPS * ordered + rows - ordered
    whole = lambda n: pl.BlockSpec((n, LANES), lambda i, *_: (0, 0))
    mine = pl.pallas_call(
        body,
        grid_spec=pltpu.PrefetchScalarGridSpec(
            num_scalar_prefetch=1, grid=(1,), in_specs=[whole(rows)] * CHIPS, out_specs=whole(height)
        ),
        out_shape=jax.ShapeDtypeStruct((height, LANES), bf16),
        compiler_params=params(),
        name="gathered",
    )(scalars, *came)
    other = other_core(mine)
    return mine, other


def assembled(mine, other, scalars, shapes, places):
    height = mine.shape[0]

    def body(s_ref, mine_ref, other_ref, *out_refs):
        def write(sources):
            for core, source in enumerate(sources):
                for k, row, column, at, rows in places[core]:
                    out_refs[k][row : row + rows, column : column + LANES] = source[at : at + rows, :].astype(f32)

        pl.when(s_ref[1] == 0)(lambda: write((mine_ref, other_ref)))
        pl.when(s_ref[1] == 1)(lambda: write((other_ref, mine_ref)))

    whole = lambda shape: pl.BlockSpec(shape, lambda i, *_: (0, 0))
    return pl.pallas_call(
        body,
        grid_spec=pltpu.PrefetchScalarGridSpec(
            num_scalar_prefetch=1, grid=(1,),
            in_specs=[whole((height, LANES))] * 2, out_specs=[whole(s) for s in shapes],
        ),
        out_shape=[jax.ShapeDtypeStruct(s, f32) for s in shapes],
        compiler_params=params(),
    )(scalars, mine, other)


def slots_exchange(x):
    return exchange(x.reshape(BLOCKS, CAP * TOK, x.shape[1])).reshape(x.shape)


def step(inputs, cotangent, memory_lists, w_query, w_key, w_value, w_output):
    model_width = inputs.shape[-1]
    inner = w_query.shape[1]
    half = inner // 2
    position = lax.axis_index("tm")
    core = lax.axis_index("roll") % 2
    chip = lax.axis_index("roll") // 2
    keeping = jnp.stack([chip, core]).astype(jnp.int32)
    sending = jnp.stack([chip, 1 - core]).astype(jnp.int32)
    x = inputs.reshape(ROWS, model_width)
    cot = cotangent.reshape(ROWS, model_width)
    x_t = x.T
    recalled = memory_lists[0]
    first_frame = position * FRAMES

    targets = jnp.arange(BLOCKS * FRAMES, dtype=jnp.int32)
    wanted = jnp.any(recalled.reshape(-1, 1) == targets[None, :], axis=0)
    wanted = wanted.astype(jnp.int32).reshape(BLOCKS, FRAMES)
    asked = exchange(wanted)

    x_before = from_behind(x[(FRAMES - BAND) * TOK :], 1)
    keyval = keyval_rows(x, w_key, w_value)
    before = keyval_rows(x_before, w_key, w_value)
    queries = jnp.dot(x, w_query, preferred_element_type=f32).astype(bf16)
    grad_heads = dot_last(cot, w_output).astype(bf16)

    slot_rank = jnp.cumsum(wanted, axis=1) - 1
    slot_table = (jnp.arange(BLOCKS, dtype=jnp.int32)[:, None] * CAP + slot_rank).reshape(-1)
    mem_ok = recalled >= 0
    flat = jnp.where(mem_ok, recalled, 0).reshape(-1)
    hit = flat[:, None] == targets[None, :]
    slot_ids = jnp.sum(jnp.where(hit, slot_table[None, :], 0), axis=1)
    ok_flat = mem_ok.reshape(-1)
    read = jnp.clip(jnp.where(ok_flat, slot_ids, 0), 0, SPARE - 1)
    add = jnp.clip(jnp.where(ok_flat, slot_ids, SPARE), 0, SPARE)
    band_index = (
        jnp.arange(FRAMES, dtype=jnp.int32)[:, None] + jnp.arange(BAND + 1, dtype=jnp.int32)[None, :]
    )
    band_ok = first_frame + band_index - BAND >= 0
    key_valid = jnp.concatenate([band_ok, mem_ok], axis=1)
    bias = jnp.repeat(jnp.where(key_valid, 0.0, masked_score).astype(f32), TOK, axis=1)

    asked_rank = jnp.cumsum(asked, axis=1) - 1
    places = jnp.arange(CAP, dtype=jnp.int32)[None, :, None]
    chosen = (asked[:, None, :] > 0) & (asked_rank[:, None, :] == places)
    frame_no = jnp.arange(FRAMES, dtype=jnp.int32)[None, None, :]
    pick = jnp.sum(jnp.where(chosen, frame_no, 0), axis=2).reshape(-1)
    pick_add = jnp.where(jnp.any(chosen, axis=2).reshape(-1), pick, FRAMES)

    outgoing = named_frames(pick, keyval)
    slots = slots_exchange(outgoing)
    owns, passed, returned = [], [], []
    written, first = (), 0
    for count in SPLIT:
        *written, own_g, rim_g, dslot_g = attend(
            read, add, bias, queries, grad_heads, keyval, before, slots, first, count, written
        )
        passed.append(from_behind(rim_g, -1))
        returned.append(slots_exchange(dslot_g))
        owns.append(own_g)
        first += count

    heads_out, grad_query = written
    sent = partial_call([(x_t, grad_query), (heads_out, cot)], sending)
    got = other_core(sent)
    kept = partial_call([(x_t, grad_query), (heads_out, cot)], keeping, got)
    sum_qo = over_chips(kept)
    share_qo = summed(exchange(sum_qo))
    mine, other = everyone(share_qo, share_qo.shape[0], keeping)
    attended = jnp.dot(heads_out, w_output, preferred_element_type=f32).astype(bf16)
    grad_input = dot_last(grad_query, w_query)
    piece, o_piece = model_width // BLOCKS // CHIPS, inner // BLOCKS // CHIPS
    half_out = model_width // 2
    places = []
    for c in range(2):
        found = []
        for j in range(CHIPS):
            at = j * share_qo.shape[0]
            for k, rows, width in ((0, piece, half), (1, o_piece, half_out)):
                for column in range(c * width, (c + 1) * width, LANES):
                    found.append((k, j * rows, column, at, rows))
                    at += rows
        places.append(found)
    total_q, total_o = assembled(
        mine, other, keeping,
        [(model_width // BLOCKS, inner), (inner // BLOCKS, model_width)], places,
    )

    dks, dvs, sums = [], [], []
    for g, count in enumerate(SPLIT):
        last = g == len(SPLIT) - 1
        dkv = collect(pick_add, owns[g], passed[g], returned[g])
        dks.append(dkv[0])
        dvs.append(dkv[1])
        sent = partial_call([(x_t, dkv)], sending, by_chip=not last)
        got = other_core(sent)
        extra = jnp.concatenate(sums, axis=1) if last else None
        kept = partial_call([(x_t, dkv)], keeping, got, not last, extra)
        if not last:
            sums.append(over_chips(kept))
    late = summed(exchange(kept))
    ordered = sum(packed_rows(piece, count * HEAD) for count in SPLIT[:-1])
    mine, other = everyone(late, ordered, keeping)
    places, shard = [], model_width // BLOCKS
    for c in range(2):
        found, first = [], sum(SPLIT[:-1])
        for j in range(CHIPS):
            for h in range(first):
                found.append((c, j * piece, h * HEAD, j * ordered + h * piece, piece))
        for h in range(first, HEADS):
            found.append((c, 0, h * HEAD, CHIPS * ordered + (h - first) * shard, shard))
        places.append(found)
    total_k, total_v = assembled(mine, other, keeping, [(shard, inner)] * 2, places)
    grad_input = (
        grad_input
        + dot_last(jnp.concatenate(dks, axis=1), w_key)
        + dot_last(jnp.concatenate(dvs, axis=1), w_value)
    )
    shape = (1, FRAMES, TOK, model_width)
    return (
        attended.reshape(shape),
        grad_input.astype(bf16).reshape(shape),
        total_q,
        total_k,
        total_v,
        total_o,
    )


def solution(mesh):
    block = P("roll", "tm", None, None)
    return jax.shard_map(
        step,
        mesh=mesh,
        in_specs=(block, block, P("roll", "tm", None), P(), P(), P(), P()),
        out_specs=(block, block, P("tm", None), P("tm", None), P("tm", None), P("tm", None)),
        check_vma=False,
    )
```

```python
import functools

import jax
import jax.numpy as jnp
from jax import lax
from jax.experimental import pallas as pl
from jax.experimental.pallas import tpu as pltpu
from jax.sharding import PartitionSpec as P


HEADS = 8
HEAD = 128
BAND = 4
MEM = 8
CAP = 3
FRAMES = 8
TOK = 32
BLOCKS = 16
ROWS = FRAMES * TOK
SPLIT = (4, 4)
KEYS = (BAND + 1 + MEM) * TOK
CHIPS = 4
SPARE = BLOCKS * CAP
masked_score = -1e30
f32, bf16 = jnp.float32, jnp.bfloat16
VMEM_LIMIT = 60 * 1024 * 1024


def params(n=1):
    return pltpu.CompilerParams(
        dimension_semantics=("arbitrary",) * n, vmem_limit_bytes=VMEM_LIMIT
    )


def dot_last(left, right):
    return lax.dot_general(left, right, (((1,), (1,)), ((), ())), preferred_element_type=f32)


def dot_first(left, right):
    return lax.dot_general(left, right, (((0,), (0,)), ((), ())), preferred_element_type=f32)


def dot(left, right):
    return lax.dot_general(left, right, (((1,), (0,)), ((), ())), preferred_element_type=f32)


def keyval_body(x_ref, wk_ref, wv_ref, out_ref):
    pieces = []
    for h in range(wk_ref.shape[1] // HEAD):
        pieces += [wk_ref[:, h * HEAD : (h + 1) * HEAD], wv_ref[:, h * HEAD : (h + 1) * HEAD]]
    out_ref[...] = dot(x_ref[...], jnp.concatenate(pieces, axis=1)).astype(bf16)


def keyval_rows(x, w_key, w_value):
    rows, width = x.shape
    cols = 256
    return pl.pallas_call(
        keyval_body,
        grid=(w_key.shape[1] // cols,),
        in_specs=[
            pl.BlockSpec((rows, width), lambda j: (0, 0)),
            pl.BlockSpec((width, cols), lambda j: (0, j)),
            pl.BlockSpec((width, cols), lambda j: (0, j)),
        ],
        out_specs=pl.BlockSpec((rows, 2 * cols), lambda j: (0, j)),
        out_shape=jax.ShapeDtypeStruct((rows, 2 * w_key.shape[1]), bf16),
        compiler_params=params(),
        name="keyval",
    )(x, w_key, w_value)


def send_body(pick_ref, kv_ref, out_ref, sem):
    def copy(i):
        at = pl.multiple_of(pick_ref[i] * TOK, TOK)
        return pltpu.make_async_copy(
            kv_ref.at[pl.ds(at, TOK), :], out_ref.at[pl.ds(i * TOK, TOK), :], sem.at[i]
        )

    for i in range(BLOCKS * CAP):
        copy(i).start()
    for i in range(BLOCKS * CAP):
        copy(i).wait()


def named_frames(pick, kv):
    width = kv.shape[1]
    return pl.pallas_call(
        send_body,
        grid_spec=pltpu.PrefetchScalarGridSpec(
            num_scalar_prefetch=1,
            grid=(1,),
            in_specs=[pl.BlockSpec((ROWS, width), lambda i, *_: (0, 0))],
            out_specs=pl.BlockSpec(memory_space=pl.ANY),
            scratch_shapes=[pltpu.SemaphoreType.DMA((BLOCKS * CAP,))],
        ),
        out_shape=jax.ShapeDtypeStruct((BLOCKS * CAP * TOK, width), bf16),
        compiler_params=params(),
        name="send",
    )(pick, kv)


def attend_body(
    read_ref, add_ref, bias_ref, q_ref, g_ref, own_ref, prev_ref, slot_ref, *refs
):
    attend_head(
        read_ref, add_ref, bias_ref, q_ref, g_ref, own_ref, prev_ref, slot_ref, *refs[-13:]
    )


def attend_head(
    read_ref, add_ref, bias_ref, q_ref, g_ref, own_ref, prev_ref, slot_ref,
    o_ref, dq_ref, down_ref, rim_ref, dslot_ref,
    acc_own, acc_prev, acc_slot, kv_scr, s_scr, gp_scr, half_scr, ds_scr,
):
    scale = HEAD ** (-0.5)
    acc_own[...] = jnp.zeros_like(acc_own)
    acc_prev[...] = jnp.zeros_like(acc_prev)
    acc_slot[...] = jnp.zeros_like(acc_slot)
    spans = [slice(f * TOK, (f + 1) * TOK) for f in range(FRAMES)]
    for f, rows in enumerate(spans):
        at = 0
        if f < BAND:
            at = (BAND - f) * TOK
            kv_scr[f, :at, :] = prev_ref[f * TOK : BAND * TOK, :]
        kv_scr[f, at : (BAND + 1) * TOK, :] = own_ref[max(f - BAND, 0) * TOK : (f + 1) * TOK, :]
        for m in range(MEM):
            at = pl.multiple_of(read_ref[f * MEM + m] * TOK, TOK)
            kv_scr[f, (BAND + 1 + m) * TOK : (BAND + 2 + m) * TOK, :] = slot_ref[pl.ds(at, TOK), :]
    for f, rows in enumerate(spans):
        s_scr[rows, :] = dot_last(q_ref[rows, :], kv_scr[f, :, :HEAD]) * scale + bias_ref[f : f + 1, :]
        gp_scr[rows, :] = dot_last(g_ref[rows, :], kv_scr[f, :, HEAD:])
    for rows in spans:
        s = s_scr[rows, :]
        gp = gp_scr[rows, :]
        e = jnp.exp(s - jnp.max(s, axis=1, keepdims=True))
        w = e * (1.0 / jnp.sum(e, axis=1, keepdims=True))
        half_scr[rows, :] = w.astype(bf16)
        ds_scr[rows, :] = (w * (gp - jnp.sum(w * gp, axis=1, keepdims=True))).astype(bf16)
    for f, rows in enumerate(spans):
        o_ref[rows, :] = dot(half_scr[rows, :], kv_scr[f, :, HEAD:]).astype(bf16)
        dq_ref[rows, :] = (dot(ds_scr[rows, :], kv_scr[f, :, :HEAD]) * scale).astype(bf16)
    for f, rows in enumerate(spans):
        dk = dot_first(ds_scr[rows, :], q_ref[rows, :]) * scale
        dv = dot_first(half_scr[rows, :], g_ref[rows, :])
        start = 0
        own = slice(max(f - BAND, 0) * TOK, (f + 1) * TOK)
        if f < BAND:
            start = (BAND - f) * TOK
            prev = slice(f * TOK, BAND * TOK)
            acc_prev[prev, :HEAD] += dk[:start]
            acc_prev[prev, HEAD:] += dv[:start]
        acc_own[own, :HEAD] += dk[start : (BAND + 1) * TOK]
        acc_own[own, HEAD:] += dv[start : (BAND + 1) * TOK]
        spots = [pl.multiple_of(add_ref[f * MEM + m] * TOK, TOK) for m in range(MEM)]
        base = (BAND + 1) * TOK
        for d, cols in ((dk, slice(0, HEAD)), (dv, slice(HEAD, 2 * HEAD))):
            olds = [acc_slot[pl.ds(at, TOK), cols] for at in spots]
            for m, at in enumerate(spots):
                acc_slot[pl.ds(at, TOK), cols] = olds[m] + d[base + m * TOK : base + (m + 1) * TOK]
    down_ref[...] = acc_own[...]
    rim_ref[...] = acc_prev[...].astype(bf16)
    dslot_ref[...] = acc_slot[: SPARE * TOK, :].astype(bf16)


def attend(read, add, bias, q, g, own, prev, slots, first, heads, written):
    col = lambda rows, width: pl.BlockSpec((rows, width), lambda h, *_: (0, h))
    src = lambda rows, width: pl.BlockSpec((rows, width), lambda h, *_: (0, h + first))
    return pl.pallas_call(
        attend_body,
        grid_spec=pltpu.PrefetchScalarGridSpec(
            num_scalar_prefetch=2,
            grid=(heads,),
            in_specs=[
                pl.BlockSpec(bias.shape, lambda h, *_: (0, 0)),
                src(ROWS, HEAD), src(ROWS, HEAD),
                src(ROWS, 2 * HEAD), src(BAND * TOK, 2 * HEAD), src(SPARE * TOK, 2 * HEAD),
            ] + [pl.BlockSpec(memory_space=pl.ANY)] * len(written),
            out_specs=[
                src(ROWS, HEAD), src(ROWS, HEAD),
                col(ROWS, 2 * HEAD), col(BAND * TOK, 2 * HEAD), col(SPARE * TOK, 2 * HEAD),
            ],
            scratch_shapes=[
                pltpu.VMEM((ROWS, 2 * HEAD), f32),
                pltpu.VMEM((BAND * TOK, 2 * HEAD), f32),
                pltpu.VMEM(((SPARE + 1) * TOK, 2 * HEAD), f32),
                pltpu.VMEM((FRAMES, KEYS, 2 * HEAD), bf16),
                pltpu.VMEM((ROWS, KEYS), f32),
                pltpu.VMEM((ROWS, KEYS), f32),
                pltpu.VMEM((ROWS, KEYS), bf16),
                pltpu.VMEM((ROWS, KEYS), bf16),
            ],
        ),
        out_shape=[
            jax.ShapeDtypeStruct(q.shape, bf16),
            jax.ShapeDtypeStruct(q.shape, bf16),
            jax.ShapeDtypeStruct((ROWS, 2 * heads * HEAD), f32),
            jax.ShapeDtypeStruct((BAND * TOK, 2 * heads * HEAD), bf16),
            jax.ShapeDtypeStruct((SPARE * TOK, 2 * heads * HEAD), bf16),
        ],
        input_output_aliases={8 + k: k for k in range(len(written))},
        compiler_params=params(),
        name="attend",
    )(read, add, bias, q, g, own, prev, slots, *written)


def collect_body(pick_ref, own_ref, rim_ref, back_ref, out_ref, acc):
    acc[:ROWS, :] = own_ref[...]
    acc[ROWS:, :] = jnp.zeros_like(acc[ROWS:, :])
    tail = slice((FRAMES - BAND) * TOK, ROWS)
    acc[tail, :] += rim_ref[...].astype(f32)
    for i in range(BLOCKS * CAP):
        at = pl.multiple_of(pick_ref[i] * TOK, TOK)
        acc[pl.ds(at, TOK), :] += back_ref[i * TOK : (i + 1) * TOK, :].astype(f32)
    for h in range(own_ref.shape[1] // (2 * HEAD)):
        for kind in range(2):
            left = (2 * h + kind) * HEAD
            out_ref[kind, :, h * HEAD : (h + 1) * HEAD] = acc[:ROWS, left : left + HEAD].astype(bf16)


def collect(pick, own, rim, back):
    width = own.shape[1]
    cols = 2 * HEAD
    col = lambda rows, w: pl.BlockSpec((rows, w), lambda h, *_: (0, h))
    return pl.pallas_call(
        collect_body,
        grid_spec=pltpu.PrefetchScalarGridSpec(
            num_scalar_prefetch=1,
            grid=(width // cols,),
            in_specs=[col(ROWS, cols), col(BAND * TOK, cols), col(SPARE * TOK, cols)],
            out_specs=pl.BlockSpec((2, ROWS, cols // 2), lambda h, *_: (0, 0, h)),
            scratch_shapes=[pltpu.VMEM((ROWS + TOK, cols), f32)],
        ),
        out_shape=jax.ShapeDtypeStruct((2, ROWS, width // 2), bf16),
        compiler_params=params(),
        name="collect",
    )(pick, own, rim, back)


LANES = HEAD


def taken(right):
    if right.ndim == 3:
        rows, n = right.shape[1:]
        return n, pl.BlockSpec((None, rows, n), lambda i, s, *_: (s[1], 0, 0))
    rows, n = right.shape
    return n // 2, pl.BlockSpec((rows, n // 2), lambda i, s, *_: (0, s[1]))


def packed_rows(rows, n):
    return rows * n // LANES


def packed(part):
    return jnp.concatenate([part[:, at : at + LANES] for at in range(0, part.shape[1], LANES)], axis=0)


def partial_call(pairs, scalars, got=None, by_chip=True, extra=()):
    per = 8
    steps = BLOCKS // per
    chips = CHIPS if by_chip else 1
    cuts = [taken(right) for _, right in pairs]
    across = [left.shape[0] == right.shape[-2] for left, right in pairs]
    shards = [left.shape[1 if a else 0] // BLOCKS for (left, _), a in zip(pairs, across)]
    height = sum(packed_rows(s // chips, n) for (n, _), s in zip(cuts, shards))
    keep = got is not None

    def body(chip_ref, *refs):
        factors, refs = refs[: 2 * len(pairs)], refs[2 * len(pairs) :]
        totals = refs[-len(pairs) :]
        for k, total in enumerate(totals):
            product = dot_first if across[k] else dot
            total[...] = product(factors[2 * k][...], factors[2 * k + 1][...])

        def write(half):
            for t in range(per):
                for d in range(chips):
                    c = lax.rem(chip_ref[0] + d, CHIPS) if keep and by_chip else d
                    parts = []
                    for total, shard in zip(totals, shards):
                        piece = shard // chips
                        first = t * shard + c * piece
                        if keep and by_chip:
                            first = pl.multiple_of(first, piece)
                        parts.append(packed(total[pl.ds(first, piece), :]))
                    part = parts[0] if len(parts) == 1 else jnp.concatenate(parts, axis=0)
                    if not by_chip:
                        if keep:
                            part = part + refs[0][t].astype(f32)
                        out_ref = refs[-1 - len(totals)]
                        out_ref[t, out_ref.shape[1] - height :, :] = part.astype(bf16)
                    elif keep:
                        part = part + refs[0][c, t].astype(f32)
                        refs[1 + 2 * d + half][t] = part.astype(bf16)
                    else:
                        refs[0][c, t] = part.astype(bf16)

        if keep and by_chip:
            early = pl.program_id(0) < steps // 2
            pl.when(early)(lambda: write(0))
            pl.when(jnp.logical_not(early))(lambda: write(1))
        else:
            write(0)

        def add(half):
            out_ref, at = refs[-1 - len(totals)], 0
            for u, sums in enumerate(extra):
                terms = refs[1 + 6 * u + 3 * half : 4 + 6 * u + 3 * half]
                size = sums[0][0].shape[1]
                for t in range(per):
                    total = sum(term[t].astype(f32) for term in terms)
                    out_ref[t, at : at + size, :] = total.astype(bf16)
                at += size

        if extra:
            for half in range(2):
                pl.when(pl.program_id(0) == half)(functools.partial(add, half))

    if by_chip:
        whole = pl.BlockSpec((CHIPS, per, height, LANES), lambda i, *_: (0, i, 0, 0))
        shape = (CHIPS, BLOCKS, height, LANES)
    else:
        whole = pl.BlockSpec((per, height, LANES), lambda i, *_: (i, 0, 0))
        shape = (BLOCKS, height, LANES)
    in_specs, operands = [], []
    for (left, right), shard, (_, spec), a in zip(pairs, shards, cuts, across):
        if a:
            in_specs += [pl.BlockSpec((left.shape[0], per * shard), lambda i, *_: (0, i)), spec]
        else:
            in_specs += [pl.BlockSpec((per * shard, left.shape[1]), lambda i, *_: (i, 0)), spec]
        operands += [left, right]
    out_specs, out_shape = whole, jax.ShapeDtypeStruct(shape, bf16)
    if keep:
        in_specs.append(whole)
        operands.append(got)
        more = 0
        for sums in extra:
            more += sums[0][0].shape[1]
            for term in (*sums[0], *sums[1]):
                in_specs.append(pl.BlockSpec(term.shape, lambda i, *_: (0, 0, 0)))
                operands.append(term)
        if extra:
            assert steps == 2
            out_specs = pl.BlockSpec((per, more + height, LANES), lambda i, *_: (i, 0, 0))
            out_shape = jax.ShapeDtypeStruct((BLOCKS, more + height, LANES), bf16)
        if by_chip:
            halves = [
                pl.BlockSpec((per, height, LANES), lambda i, *_: (jnp.minimum(i, steps // 2 - 1), 0, 0)),
                pl.BlockSpec((per, height, LANES), lambda i, *_: (jnp.maximum(i - steps // 2, 0), 0, 0)),
            ]
            out_specs = halves * CHIPS
            out_shape = [jax.ShapeDtypeStruct((BLOCKS // 2, height, LANES), bf16)] * (2 * CHIPS)
    return pl.pallas_call(
        body,
        grid_spec=pltpu.PrefetchScalarGridSpec(
            num_scalar_prefetch=1,
            grid=(steps,),
            in_specs=in_specs,
            out_specs=out_specs,
            scratch_shapes=[
                pltpu.VMEM((per * s, n), f32) for (n, _), s in zip(cuts, shards)
            ],
        ),
        out_shape=out_shape,
        compiler_params=params(),
    )(scalars, *operands)


def input_gradient(dq, dkvs, w_query, w_key, w_value):
    rows, inner = dq.shape
    width = w_query.shape[0]
    cut = 512

    def body(dq_ref, wq_ref, wk_ref, wv_ref, *refs):
        total = dot_last(dq_ref[...], wq_ref[...])
        at = 0
        for ref in refs[:-1]:
            n = ref.shape[2]
            for kind, weights in enumerate((wk_ref, wv_ref)):
                total = total + dot_last(ref[kind], weights[:, at : at + n])
            at += n
        refs[-1][...] = total.astype(bf16)

    weights = pl.BlockSpec((cut, inner), lambda j: (j, 0))
    return pl.pallas_call(
        body,
        grid=(width // cut,),
        in_specs=[pl.BlockSpec((rows, inner), lambda j: (0, 0)), weights, weights, weights]
        + [pl.BlockSpec(d.shape, lambda j: (0, 0, 0)) for d in dkvs],
        out_specs=pl.BlockSpec((rows, cut), lambda j: (0, j)),
        out_shape=jax.ShapeDtypeStruct((rows, width), bf16),
        compiler_params=params(),
        name="input_gradient",
    )(dq, w_query, w_key, w_value, *dkvs)


def other_core(x):
    return lax.ppermute(x, "roll", [(i, i ^ 1) for i in range(lax.axis_size("roll"))])


def from_behind(block, distance):
    return lax.ppermute(
        block, "tm", [(i - distance, i) for i in range(BLOCKS) if 0 <= i - distance < BLOCKS]
    )


def exchange(x, axis="tm", groups=None):
    return lax.all_to_all(
        x, axis, split_axis=0, concat_axis=0, tiled=True, axis_index_groups=groups
    )


def summed(parts):
    return jnp.sum(parts.astype(f32), axis=0).astype(bf16)


def along_chips(x, d):
    n = 2 * CHIPS
    return lax.ppermute(x, "roll", [(i, (i + 2 * d) % n) for i in range(n)])


def plus(a, b):
    return (a.astype(f32) + b.astype(f32)).astype(bf16)


def over_chips(pieces):
    own0, own1, next0, next1, far0, far1, last0, last1 = pieces
    up, down = along_chips(far0, 1), along_chips(far1, -1)
    from_next, from_last = along_chips(next1, 1), along_chips(last0, -1)
    came0 = along_chips(plus(next0, up), 1)
    came1 = along_chips(plus(last1, down), -1)
    return (own0, from_last, came0), (own1, from_next, came1)


def everyone(x, ordered, scalars):
    came = [x] + [along_chips(x, d) for d in range(1, CHIPS)]
    rows = x.shape[0]

    def body(s_ref, *refs):
        out_ref = refs[-1]
        for d in range(CHIPS):
            at = pl.multiple_of(lax.rem(s_ref[0] + CHIPS - d, CHIPS) * ordered, ordered)
            out_ref[pl.ds(at, ordered), :] = refs[d][:ordered, :]
        if ordered < rows:
            total = refs[0][ordered:, :].astype(f32)
            for d in range(1, CHIPS):
                total = total + refs[d][ordered:, :].astype(f32)
            out_ref[CHIPS * ordered :, :] = total.astype(bf16)

    height = CHIPS * ordered + rows - ordered
    whole = lambda n: pl.BlockSpec((n, LANES), lambda i, *_: (0, 0))
    mine = pl.pallas_call(
        body,
        grid_spec=pltpu.PrefetchScalarGridSpec(
            num_scalar_prefetch=1, grid=(1,), in_specs=[whole(rows)] * CHIPS, out_specs=whole(height)
        ),
        out_shape=jax.ShapeDtypeStruct((height, LANES), bf16),
        compiler_params=params(),
        name="gathered",
    )(scalars, *came)
    other = other_core(mine)
    return mine, other


def assembled(mine, other, scalars, shapes, places):
    height = mine.shape[0]

    def body(s_ref, mine_ref, other_ref, *out_refs):
        def write(sources):
            for core, source in enumerate(sources):
                for k, row, column, at, rows in places[core]:
                    out_refs[k][row : row + rows, column : column + LANES] = source[at : at + rows, :].astype(f32)

        pl.when(s_ref[1] == 0)(lambda: write((mine_ref, other_ref)))
        pl.when(s_ref[1] == 1)(lambda: write((other_ref, mine_ref)))

    whole = lambda shape: pl.BlockSpec(shape, lambda i, *_: (0, 0))
    return pl.pallas_call(
        body,
        grid_spec=pltpu.PrefetchScalarGridSpec(
            num_scalar_prefetch=1, grid=(1,),
            in_specs=[whole((height, LANES))] * 2, out_specs=[whole(s) for s in shapes],
        ),
        out_shape=[jax.ShapeDtypeStruct(s, f32) for s in shapes],
        compiler_params=params(),
    )(scalars, mine, other)


def slots_exchange(x):
    return exchange(x.reshape(BLOCKS, CAP * TOK, x.shape[1])).reshape(x.shape)


def step(inputs, cotangent, memory_lists, w_query, w_key, w_value, w_output):
    model_width = inputs.shape[-1]
    inner = w_query.shape[1]
    half = inner // 2
    position = lax.axis_index("tm")
    core = lax.axis_index("roll") % 2
    chip = lax.axis_index("roll") // 2
    keeping = jnp.stack([chip, core]).astype(jnp.int32)
    sending = jnp.stack([chip, 1 - core]).astype(jnp.int32)
    x = inputs.reshape(ROWS, model_width)
    cot = cotangent.reshape(ROWS, model_width)
    x_t = x.T
    recalled = memory_lists[0]
    first_frame = position * FRAMES

    targets = jnp.arange(BLOCKS * FRAMES, dtype=jnp.int32)
    wanted = jnp.any(recalled.reshape(-1, 1) == targets[None, :], axis=0)
    wanted = wanted.astype(jnp.int32).reshape(BLOCKS, FRAMES)
    asked = exchange(wanted)

    x_before = from_behind(x[(FRAMES - BAND) * TOK :], 1)
    keyval = keyval_rows(x, w_key, w_value)
    before = keyval_rows(x_before, w_key, w_value)
    queries = jnp.dot(x, w_query, preferred_element_type=f32).astype(bf16)
    grad_heads = dot_last(cot, w_output).astype(bf16)

    slot_rank = jnp.cumsum(wanted, axis=1) - 1
    slot_table = (jnp.arange(BLOCKS, dtype=jnp.int32)[:, None] * CAP + slot_rank).reshape(-1)
    mem_ok = recalled >= 0
    flat = jnp.where(mem_ok, recalled, 0).reshape(-1)
    hit = flat[:, None] == targets[None, :]
    slot_ids = jnp.sum(jnp.where(hit, slot_table[None, :], 0), axis=1)
    ok_flat = mem_ok.reshape(-1)
    read = jnp.clip(jnp.where(ok_flat, slot_ids, 0), 0, SPARE - 1)
    add = jnp.clip(jnp.where(ok_flat, slot_ids, SPARE), 0, SPARE)
    band_index = (
        jnp.arange(FRAMES, dtype=jnp.int32)[:, None] + jnp.arange(BAND + 1, dtype=jnp.int32)[None, :]
    )
    band_ok = first_frame + band_index - BAND >= 0
    key_valid = jnp.concatenate([band_ok, mem_ok], axis=1)
    bias = jnp.repeat(jnp.where(key_valid, 0.0, masked_score).astype(f32), TOK, axis=1)

    asked_rank = jnp.cumsum(asked, axis=1) - 1
    places = jnp.arange(CAP, dtype=jnp.int32)[None, :, None]
    chosen = (asked[:, None, :] > 0) & (asked_rank[:, None, :] == places)
    frame_no = jnp.arange(FRAMES, dtype=jnp.int32)[None, None, :]
    pick = jnp.sum(jnp.where(chosen, frame_no, 0), axis=2).reshape(-1)
    pick_add = jnp.where(jnp.any(chosen, axis=2).reshape(-1), pick, FRAMES)

    outgoing = named_frames(pick, keyval)
    slots = slots_exchange(outgoing)
    owns, passed, returned = [], [], []
    written, first = (), 0
    for count in SPLIT:
        *written, own_g, rim_g, dslot_g = attend(
            read, add, bias, queries, grad_heads, keyval, before, slots, first, count, written
        )
        passed.append(from_behind(rim_g, -1))
        returned.append(slots_exchange(dslot_g))
        owns.append(own_g)
        first += count

    heads_out, grad_query = written
    sent = partial_call([(x_t, grad_query), (heads_out, cot)], sending)
    got = other_core(sent)
    kept = partial_call([(x_t, grad_query), (heads_out, cot)], keeping, got)
    sum_qo = over_chips(kept)
    attended = jnp.dot(heads_out, w_output, preferred_element_type=f32).astype(bf16)
    dkvs, sums = [], [sum_qo]
    for g, count in enumerate(SPLIT):
        last = g == len(SPLIT) - 1
        dkv = collect(pick_add, owns[g], passed[g], returned[g])
        dkvs.append(dkv)
        sent = partial_call([(x_t, dkv)], sending, by_chip=not last)
        got = other_core(sent)
        kept = partial_call([(x_t, dkv)], keeping, got, not last, sums if last else ())
        if not last:
            sums.append(over_chips(kept))
    late = summed(exchange(kept))
    grad_input = input_gradient(grad_query, dkvs, w_query, w_key, w_value)
    ordered = sum(sums[0][0].shape[1] for sums in sums)
    mine, other = everyone(late, ordered, keeping)
    shard, o_shard = model_width // BLOCKS, inner // BLOCKS
    piece, o_piece = shard // CHIPS, o_shard // CHIPS
    places = []
    for c in range(2):
        found, first = [], sum(SPLIT[:-1])
        for j in range(CHIPS):
            at = j * ordered
            for k, rows, width in ((0, piece, half), (1, o_piece, model_width // 2)):
                for column in range(c * width, (c + 1) * width, LANES):
                    found.append((k, j * rows, column, at, rows))
                    at += rows
            for h in range(first):
                found.append((2 + c, j * piece, h * HEAD, at, piece))
                at += piece
        for h in range(first, HEADS):
            found.append((2 + c, 0, h * HEAD, CHIPS * ordered + (h - first) * shard, shard))
        places.append(found)
    total_q, total_o, total_k, total_v = assembled(
        mine, other, keeping,
        [(shard, inner), (o_shard, model_width), (shard, inner), (shard, inner)], places,
    )
    shape = (1, FRAMES, TOK, model_width)
    return (
        attended.reshape(shape),
        grad_input.reshape(shape),
        total_q,
        total_k,
        total_v,
        total_o,
    )


def solution(mesh):
    block = P("roll", "tm", None, None)
    return jax.shard_map(
        step,
        mesh=mesh,
        in_specs=(block, block, P("roll", "tm", None), P(), P(), P(), P()),
        out_specs=(block, block, P("tm", None), P("tm", None), P("tm", None), P("tm", None)),
        check_vma=False,
    )
```

```python
import functools

import jax
import jax.numpy as jnp
from jax import lax
from jax.experimental import pallas as pl
from jax.experimental.pallas import tpu as pltpu
from jax.sharding import PartitionSpec as P


HEADS = 8
HEAD = 128
BAND = 4
MEM = 8
CAP = 3
FRAMES = 8
TOK = 32
BLOCKS = 16
ROWS = FRAMES * TOK
SPLIT = (4, 4)
KEYS = (BAND + 1 + MEM) * TOK
CHIPS = 4
SPARE = BLOCKS * CAP
masked_score = -1e30
f32, bf16 = jnp.float32, jnp.bfloat16
VMEM_LIMIT = 60 * 1024 * 1024


def params(n=1):
    return pltpu.CompilerParams(
        dimension_semantics=("arbitrary",) * n, vmem_limit_bytes=VMEM_LIMIT
    )


def dot_last(left, right):
    return lax.dot_general(left, right, (((1,), (1,)), ((), ())), preferred_element_type=f32)


def dot_first(left, right):
    return lax.dot_general(left, right, (((0,), (0,)), ((), ())), preferred_element_type=f32)


def dot(left, right):
    return lax.dot_general(left, right, (((1,), (0,)), ((), ())), preferred_element_type=f32)


def keyval_body(x_ref, wk_ref, wv_ref, out_ref):
    pieces = []
    for h in range(wk_ref.shape[1] // HEAD):
        pieces += [wk_ref[:, h * HEAD : (h + 1) * HEAD], wv_ref[:, h * HEAD : (h + 1) * HEAD]]
    out_ref[...] = dot(x_ref[...], jnp.concatenate(pieces, axis=1)).astype(bf16)


def keyval_rows(x, w_key, w_value):
    rows, width = x.shape
    cols = 256
    return pl.pallas_call(
        keyval_body,
        grid=(w_key.shape[1] // cols,),
        in_specs=[
            pl.BlockSpec((rows, width), lambda j: (0, 0)),
            pl.BlockSpec((width, cols), lambda j: (0, j)),
            pl.BlockSpec((width, cols), lambda j: (0, j)),
        ],
        out_specs=pl.BlockSpec((rows, 2 * cols), lambda j: (0, j)),
        out_shape=jax.ShapeDtypeStruct((rows, 2 * w_key.shape[1]), bf16),
        compiler_params=params(),
    )(x, w_key, w_value)


def send_body(pick_ref, kv_ref, out_ref, sem):
    def copy(i):
        at = pl.multiple_of(pick_ref[i] * TOK, TOK)
        return pltpu.make_async_copy(
            kv_ref.at[pl.ds(at, TOK), :], out_ref.at[pl.ds(i * TOK, TOK), :], sem.at[i]
        )

    for i in range(BLOCKS * CAP):
        copy(i).start()
    for i in range(BLOCKS * CAP):
        copy(i).wait()


def named_frames(pick, kv):
    width = kv.shape[1]
    return pl.pallas_call(
        send_body,
        grid_spec=pltpu.PrefetchScalarGridSpec(
            num_scalar_prefetch=1,
            grid=(1,),
            in_specs=[pl.BlockSpec((ROWS, width), lambda i, *_: (0, 0))],
            out_specs=pl.BlockSpec(memory_space=pl.ANY),
            scratch_shapes=[pltpu.SemaphoreType.DMA((BLOCKS * CAP,))],
        ),
        out_shape=jax.ShapeDtypeStruct((BLOCKS * CAP * TOK, width), bf16),
        compiler_params=params(),
    )(pick, kv)


def attend_body(
    read_ref, add_ref, bias_ref, q_ref, g_ref, own_ref, prev_ref, slot_ref, *refs
):
    attend_head(
        read_ref, add_ref, bias_ref, q_ref, g_ref, own_ref, prev_ref, slot_ref, *refs[-13:]
    )


def attend_head(
    read_ref, add_ref, bias_ref, q_ref, g_ref, own_ref, prev_ref, slot_ref,
    o_ref, dq_ref, down_ref, rim_ref, dslot_ref,
    acc_own, acc_prev, acc_slot, kv_scr, s_scr, gp_scr, half_scr, ds_scr,
):
    scale = HEAD ** (-0.5)
    acc_own[...] = jnp.zeros_like(acc_own)
    acc_prev[...] = jnp.zeros_like(acc_prev)
    acc_slot[...] = jnp.zeros_like(acc_slot)
    spans = [slice(f * TOK, (f + 1) * TOK) for f in range(FRAMES)]
    for f, rows in enumerate(spans):
        at = 0
        if f < BAND:
            at = (BAND - f) * TOK
            kv_scr[f, :at, :] = prev_ref[f * TOK : BAND * TOK, :]
        kv_scr[f, at : (BAND + 1) * TOK, :] = own_ref[max(f - BAND, 0) * TOK : (f + 1) * TOK, :]
        for m in range(MEM):
            at = pl.multiple_of(read_ref[f * MEM + m] * TOK, TOK)
            kv_scr[f, (BAND + 1 + m) * TOK : (BAND + 2 + m) * TOK, :] = slot_ref[pl.ds(at, TOK), :]
    for f, rows in enumerate(spans):
        s_scr[rows, :] = dot_last(q_ref[rows, :], kv_scr[f, :, :HEAD]) * scale + bias_ref[f : f + 1, :]
        gp_scr[rows, :] = dot_last(g_ref[rows, :], kv_scr[f, :, HEAD:])
    for rows in spans:
        s = s_scr[rows, :]
        gp = gp_scr[rows, :]
        e = jnp.exp(s - jnp.max(s, axis=1, keepdims=True))
        w = e * (1.0 / jnp.sum(e, axis=1, keepdims=True))
        half_scr[rows, :] = w.astype(bf16)
        ds_scr[rows, :] = (w * (gp - jnp.sum(w * gp, axis=1, keepdims=True))).astype(bf16)
    for f, rows in enumerate(spans):
        o_ref[rows, :] = dot(half_scr[rows, :], kv_scr[f, :, HEAD:]).astype(bf16)
        dq_ref[rows, :] = (dot(ds_scr[rows, :], kv_scr[f, :, :HEAD]) * scale).astype(bf16)
    for f, rows in enumerate(spans):
        dk = dot_first(ds_scr[rows, :], q_ref[rows, :]) * scale
        dv = dot_first(half_scr[rows, :], g_ref[rows, :])
        start = 0
        own = slice(max(f - BAND, 0) * TOK, (f + 1) * TOK)
        if f < BAND:
            start = (BAND - f) * TOK
            prev = slice(f * TOK, BAND * TOK)
            acc_prev[prev, :HEAD] += dk[:start]
            acc_prev[prev, HEAD:] += dv[:start]
        acc_own[own, :HEAD] += dk[start : (BAND + 1) * TOK]
        acc_own[own, HEAD:] += dv[start : (BAND + 1) * TOK]
        spots = [pl.multiple_of(add_ref[f * MEM + m] * TOK, TOK) for m in range(MEM)]
        base = (BAND + 1) * TOK
        for d, cols in ((dk, slice(0, HEAD)), (dv, slice(HEAD, 2 * HEAD))):
            olds = [acc_slot[pl.ds(at, TOK), cols] for at in spots]
            for m, at in enumerate(spots):
                acc_slot[pl.ds(at, TOK), cols] = olds[m] + d[base + m * TOK : base + (m + 1) * TOK]
    down_ref[...] = acc_own[...]
    rim_ref[...] = acc_prev[...].astype(bf16)
    dslot_ref[...] = acc_slot[: SPARE * TOK, :].astype(bf16)


def attend(read, add, bias, q, g, own, prev, slots, first, heads, written):
    col = lambda rows, width: pl.BlockSpec((rows, width), lambda h, *_: (0, h))
    src = lambda rows, width: pl.BlockSpec((rows, width), lambda h, *_: (0, h + first))
    return pl.pallas_call(
        attend_body,
        grid_spec=pltpu.PrefetchScalarGridSpec(
            num_scalar_prefetch=2,
            grid=(heads,),
            in_specs=[
                pl.BlockSpec(bias.shape, lambda h, *_: (0, 0)),
                src(ROWS, HEAD), src(ROWS, HEAD),
                src(ROWS, 2 * HEAD), src(BAND * TOK, 2 * HEAD), src(SPARE * TOK, 2 * HEAD),
            ] + [pl.BlockSpec(memory_space=pl.ANY)] * len(written),
            out_specs=[
                src(ROWS, HEAD), src(ROWS, HEAD),
                col(ROWS, 2 * HEAD), col(BAND * TOK, 2 * HEAD), col(SPARE * TOK, 2 * HEAD),
            ],
            scratch_shapes=[
                pltpu.VMEM((ROWS, 2 * HEAD), f32),
                pltpu.VMEM((BAND * TOK, 2 * HEAD), f32),
                pltpu.VMEM(((SPARE + 1) * TOK, 2 * HEAD), f32),
                pltpu.VMEM((FRAMES, KEYS, 2 * HEAD), bf16),
                pltpu.VMEM((ROWS, KEYS), f32),
                pltpu.VMEM((ROWS, KEYS), f32),
                pltpu.VMEM((ROWS, KEYS), bf16),
                pltpu.VMEM((ROWS, KEYS), bf16),
            ],
        ),
        out_shape=[
            jax.ShapeDtypeStruct(q.shape, bf16),
            jax.ShapeDtypeStruct(q.shape, bf16),
            jax.ShapeDtypeStruct((ROWS, 2 * heads * HEAD), f32),
            jax.ShapeDtypeStruct((BAND * TOK, 2 * heads * HEAD), bf16),
            jax.ShapeDtypeStruct((SPARE * TOK, 2 * heads * HEAD), bf16),
        ],
        input_output_aliases={8 + k: k for k in range(len(written))},
        compiler_params=params(),
    )(read, add, bias, q, g, own, prev, slots, *written)


def collect_body(pick_ref, own_ref, rim_ref, back_ref, out_ref, *accs):
    for acc in accs:
        acc[...] = jnp.zeros_like(acc)
    for i in range(BLOCKS * CAP):
        acc = accs[i % len(accs)]
        at = pl.multiple_of(pick_ref[i] * TOK, TOK)
        acc[pl.ds(at, TOK), :] += back_ref[i * TOK : (i + 1) * TOK, :].astype(f32)
    acc = accs[0]
    acc[:ROWS, :] = own_ref[...] + sum(a[:ROWS, :] for a in accs)
    tail = slice((FRAMES - BAND) * TOK, ROWS)
    acc[tail, :] += rim_ref[...].astype(f32)
    for h in range(own_ref.shape[1] // (2 * HEAD)):
        for kind in range(2):
            left = (2 * h + kind) * HEAD
            out_ref[kind, :, h * HEAD : (h + 1) * HEAD] = acc[:ROWS, left : left + HEAD].astype(bf16)


def collect(pick, own, rim, back):
    width = own.shape[1]
    cols = 2 * HEAD
    col = lambda rows, w: pl.BlockSpec((rows, w), lambda h, *_: (0, h))
    return pl.pallas_call(
        collect_body,
        grid_spec=pltpu.PrefetchScalarGridSpec(
            num_scalar_prefetch=1,
            grid=(width // cols,),
            in_specs=[col(ROWS, cols), col(BAND * TOK, cols), col(SPARE * TOK, cols)],
            out_specs=pl.BlockSpec((2, ROWS, cols // 2), lambda h, *_: (0, 0, h)),
            scratch_shapes=[pltpu.VMEM((ROWS + TOK, cols), f32)] * 4,
        ),
        out_shape=jax.ShapeDtypeStruct((2, ROWS, width // 2), bf16),
        compiler_params=params(),
    )(pick, own, rim, back)


LANES = HEAD


def taken(right):
    if right.ndim == 3:
        rows, n = right.shape[1:]
        return n, pl.BlockSpec((None, rows, n), lambda i, s, *_: (s[1], 0, 0))
    rows, n = right.shape
    return n // 2, pl.BlockSpec((rows, n // 2), lambda i, s, *_: (0, s[1]))


def packed_rows(rows, n):
    return rows * n // LANES


def packed(part):
    return jnp.concatenate([part[:, at : at + LANES] for at in range(0, part.shape[1], LANES)], axis=0)


def partial_call(pairs, scalars, got=None, by_chip=True, extra=()):
    per = 8
    steps = BLOCKS // per
    chips = CHIPS if by_chip else 1
    cuts = [taken(right) for _, right in pairs]
    across = [left.shape[0] == right.shape[-2] for left, right in pairs]
    shards = [left.shape[1 if a else 0] // BLOCKS for (left, _), a in zip(pairs, across)]
    height = sum(packed_rows(s // chips, n) for (n, _), s in zip(cuts, shards))
    keep = got is not None

    def body(chip_ref, *refs):
        factors, refs = refs[: 2 * len(pairs)], refs[2 * len(pairs) :]
        totals = refs[-len(pairs) :]
        for k, total in enumerate(totals):
            product = dot_first if across[k] else dot
            total[...] = product(factors[2 * k][...], factors[2 * k + 1][...])

        def write(half):
            for t in range(per):
                for d in range(chips):
                    c = lax.rem(chip_ref[0] + d, CHIPS) if keep and by_chip else d
                    parts = []
                    for total, shard in zip(totals, shards):
                        piece = shard // chips
                        first = t * shard + c * piece
                        if keep and by_chip:
                            first = pl.multiple_of(first, piece)
                        parts.append(packed(total[pl.ds(first, piece), :]))
                    part = parts[0] if len(parts) == 1 else jnp.concatenate(parts, axis=0)
                    if not by_chip:
                        if keep:
                            part = part + refs[0][t].astype(f32)
                        out_ref = refs[-1 - len(totals)]
                        out_ref[t, out_ref.shape[1] - height :, :] = part.astype(bf16)
                    elif keep:
                        part = part + refs[0][c, t].astype(f32)
                        refs[1 + 2 * d + half][t] = part.astype(bf16)
                    else:
                        refs[0][c, t] = part.astype(bf16)

        if keep and by_chip:
            early = pl.program_id(0) < steps // 2
            pl.when(early)(lambda: write(0))
            pl.when(jnp.logical_not(early))(lambda: write(1))
        else:
            write(0)

        def add(half):
            out_ref, at = refs[-1 - len(totals)], 0
            for u, sums in enumerate(extra):
                terms = refs[1 + 6 * u + 3 * half : 4 + 6 * u + 3 * half]
                size = sums[0][0].shape[1]
                for t in range(per):
                    total = sum(term[t].astype(f32) for term in terms)
                    out_ref[t, at : at + size, :] = total.astype(bf16)
                at += size

        if extra:
            for half in range(2):
                pl.when(pl.program_id(0) == half)(functools.partial(add, half))

    if by_chip:
        whole = pl.BlockSpec((CHIPS, per, height, LANES), lambda i, *_: (0, i, 0, 0))
        shape = (CHIPS, BLOCKS, height, LANES)
    else:
        whole = pl.BlockSpec((per, height, LANES), lambda i, *_: (i, 0, 0))
        shape = (BLOCKS, height, LANES)
    in_specs, operands = [], []
    for (left, right), shard, (_, spec), a in zip(pairs, shards, cuts, across):
        if a:
            in_specs += [pl.BlockSpec((left.shape[0], per * shard), lambda i, *_: (0, i)), spec]
        else:
            in_specs += [pl.BlockSpec((per * shard, left.shape[1]), lambda i, *_: (i, 0)), spec]
        operands += [left, right]
    out_specs, out_shape = whole, jax.ShapeDtypeStruct(shape, bf16)
    if keep:
        in_specs.append(whole)
        operands.append(got)
        more = 0
        for sums in extra:
            more += sums[0][0].shape[1]
            for term in (*sums[0], *sums[1]):
                in_specs.append(pl.BlockSpec(term.shape, lambda i, *_: (0, 0, 0)))
                operands.append(term)
        if extra:
            assert steps == 2
            out_specs = pl.BlockSpec((per, more + height, LANES), lambda i, *_: (i, 0, 0))
            out_shape = jax.ShapeDtypeStruct((BLOCKS, more + height, LANES), bf16)
        if by_chip:
            halves = [
                pl.BlockSpec((per, height, LANES), lambda i, *_: (jnp.minimum(i, steps // 2 - 1), 0, 0)),
                pl.BlockSpec((per, height, LANES), lambda i, *_: (jnp.maximum(i - steps // 2, 0), 0, 0)),
            ]
            out_specs = halves * CHIPS
            out_shape = [jax.ShapeDtypeStruct((BLOCKS // 2, height, LANES), bf16)] * (2 * CHIPS)
    return pl.pallas_call(
        body,
        grid_spec=pltpu.PrefetchScalarGridSpec(
            num_scalar_prefetch=1,
            grid=(steps,),
            in_specs=in_specs,
            out_specs=out_specs,
            scratch_shapes=[
                pltpu.VMEM((per * s, n), f32) for (n, _), s in zip(cuts, shards)
            ],
        ),
        out_shape=out_shape,
        compiler_params=params(),
    )(scalars, *operands)


def input_gradient(dq, dkvs, w_query, w_key, w_value):
    rows, inner = dq.shape
    width = w_query.shape[0]
    cut = 512

    def body(dq_ref, wq_ref, wk_ref, wv_ref, *refs):
        total = dot_last(dq_ref[...], wq_ref[...])
        at = 0
        for ref in refs[:-1]:
            n = ref.shape[2]
            for kind, weights in enumerate((wk_ref, wv_ref)):
                total = total + dot_last(ref[kind], weights[:, at : at + n])
            at += n
        refs[-1][...] = total.astype(bf16)

    weights = pl.BlockSpec((cut, inner), lambda j: (j, 0))
    return pl.pallas_call(
        body,
        grid=(width // cut,),
        in_specs=[pl.BlockSpec((rows, inner), lambda j: (0, 0)), weights, weights, weights]
        + [pl.BlockSpec(d.shape, lambda j: (0, 0, 0)) for d in dkvs],
        out_specs=pl.BlockSpec((rows, cut), lambda j: (0, j)),
        out_shape=jax.ShapeDtypeStruct((rows, width), bf16),
        compiler_params=params(),
    )(dq, w_query, w_key, w_value, *dkvs)


def other_core(x):
    return lax.ppermute(x, "roll", [(i, i ^ 1) for i in range(lax.axis_size("roll"))])


def from_behind(block, distance):
    return lax.ppermute(
        block, "tm", [(i - distance, i) for i in range(BLOCKS) if 0 <= i - distance < BLOCKS]
    )


def exchange(x, axis="tm", groups=None):
    return lax.all_to_all(
        x, axis, split_axis=0, concat_axis=0, tiled=True, axis_index_groups=groups
    )


def summed(parts):
    return jnp.sum(parts.astype(f32), axis=0).astype(bf16)


def along_chips(x, d):
    n = 2 * CHIPS
    return lax.ppermute(x, "roll", [(i, (i + 2 * d) % n) for i in range(n)])


def plus(a, b):
    return (a.astype(f32) + b.astype(f32)).astype(bf16)


def over_chips(pieces):
    own0, own1, next0, next1, far0, far1, last0, last1 = pieces
    up, down = along_chips(far0, 1), along_chips(far1, -1)
    from_next, from_last = along_chips(next1, 1), along_chips(last0, -1)
    came0 = along_chips(plus(next0, up), 1)
    came1 = along_chips(plus(last1, down), -1)
    return (own0, from_last, came0), (own1, from_next, came1)


def over_blocks(x):
    return summed(exchange(x))


def combined(parts):
    sizes = [halves[0][0].shape[1] for halves in parts]
    per = BLOCKS // 2

    def body(*refs):
        out_ref = refs[-1]

        def write(half):
            at = 0
            for u, size in enumerate(sizes):
                terms = refs[6 * u + 3 * half : 6 * u + 3 * half + 3]
                out_ref[:, at : at + size, :] = sum(term[...].astype(f32) for term in terms).astype(bf16)
                at += size

        for half in range(2):
            pl.when(pl.program_id(0) == half)(functools.partial(write, half))

    operands = [term for halves in parts for terms in halves for term in terms]
    return pl.pallas_call(
        body,
        grid=(2,),
        in_specs=[pl.BlockSpec(term.shape, lambda i: (0, 0, 0)) for term in operands],
        out_specs=pl.BlockSpec((per, sum(sizes), LANES), lambda i: (i, 0, 0)),
        out_shape=jax.ShapeDtypeStruct((BLOCKS, sum(sizes), LANES), bf16),
        compiler_params=params(),
    )(*operands)


def everyone(x, ordered, scalars):
    came = [x] + [along_chips(x, d) for d in range(1, CHIPS)]
    rows = x.shape[0]

    def body(s_ref, *refs):
        out_ref = refs[-1]
        for d in range(CHIPS):
            at = pl.multiple_of(lax.rem(s_ref[0] + CHIPS - d, CHIPS) * ordered, ordered)
            out_ref[pl.ds(at, ordered), :] = refs[d][:ordered, :]
        if ordered < rows:
            total = refs[0][ordered:, :].astype(f32)
            for d in range(1, CHIPS):
                total = total + refs[d][ordered:, :].astype(f32)
            out_ref[CHIPS * ordered :, :] = total.astype(bf16)

    height = CHIPS * ordered + rows - ordered
    whole = lambda n: pl.BlockSpec((n, LANES), lambda i, *_: (0, 0))
    mine = pl.pallas_call(
        body,
        grid_spec=pltpu.PrefetchScalarGridSpec(
            num_scalar_prefetch=1, grid=(1,), in_specs=[whole(rows)] * CHIPS, out_specs=whole(height)
        ),
        out_shape=jax.ShapeDtypeStruct((height, LANES), bf16),
        compiler_params=params(),
    )(scalars, *came)
    other = other_core(mine)
    return mine, other


def assembled(mine, other, scalars, shapes, places):
    height = mine.shape[0]

    def body(s_ref, mine_ref, other_ref, *out_refs):
        def write(sources):
            for core, source in enumerate(sources):
                for k, row, column, at, rows in places[core]:
                    out_refs[k][row : row + rows, column : column + LANES] = source[at : at + rows, :].astype(f32)

        pl.when(s_ref[1] == 0)(lambda: write((mine_ref, other_ref)))
        pl.when(s_ref[1] == 1)(lambda: write((other_ref, mine_ref)))

    whole = lambda shape: pl.BlockSpec(shape, lambda i, *_: (0, 0))
    return pl.pallas_call(
        body,
        grid_spec=pltpu.PrefetchScalarGridSpec(
            num_scalar_prefetch=1, grid=(1,),
            in_specs=[whole((height, LANES))] * 2, out_specs=[whole(s) for s in shapes],
        ),
        out_shape=[jax.ShapeDtypeStruct(s, f32) for s in shapes],
        compiler_params=params(),
    )(scalars, mine, other)


def slots_exchange(x):
    return exchange(x.reshape(BLOCKS, CAP * TOK, x.shape[1])).reshape(x.shape)


def step(inputs, cotangent, memory_lists, w_query, w_key, w_value, w_output):
    model_width = inputs.shape[-1]
    inner = w_query.shape[1]
    half = inner // 2
    position = lax.axis_index("tm")
    core = lax.axis_index("roll") % 2
    chip = lax.axis_index("roll") // 2
    keeping = jnp.stack([chip, core]).astype(jnp.int32)
    sending = jnp.stack([chip, 1 - core]).astype(jnp.int32)
    x = inputs.reshape(ROWS, model_width)
    cot = cotangent.reshape(ROWS, model_width)
    x_t = x.T
    recalled = memory_lists[0]
    first_frame = position * FRAMES

    targets = jnp.arange(BLOCKS * FRAMES, dtype=jnp.int32)
    wanted = jnp.any(recalled.reshape(-1, 1) == targets[None, :], axis=0)
    wanted = wanted.astype(jnp.int32).reshape(BLOCKS, FRAMES)
    asked = exchange(wanted)

    x_before = from_behind(x[(FRAMES - BAND) * TOK :], 1)
    keyval = keyval_rows(x, w_key, w_value)
    before = keyval_rows(x_before, w_key, w_value)
    queries = jnp.dot(x, w_query, preferred_element_type=f32).astype(bf16)
    grad_heads = dot_last(cot, w_output).astype(bf16)

    slot_rank = jnp.cumsum(wanted, axis=1) - 1
    slot_table = (jnp.arange(BLOCKS, dtype=jnp.int32)[:, None] * CAP + slot_rank).reshape(-1)
    mem_ok = recalled >= 0
    flat = jnp.where(mem_ok, recalled, 0).reshape(-1)
    hit = flat[:, None] == targets[None, :]
    slot_ids = jnp.sum(jnp.where(hit, slot_table[None, :], 0), axis=1)
    ok_flat = mem_ok.reshape(-1)
    read = jnp.clip(jnp.where(ok_flat, slot_ids, 0), 0, SPARE - 1)
    add = jnp.clip(jnp.where(ok_flat, slot_ids, SPARE), 0, SPARE)
    band_index = (
        jnp.arange(FRAMES, dtype=jnp.int32)[:, None] + jnp.arange(BAND + 1, dtype=jnp.int32)[None, :]
    )
    band_ok = first_frame + band_index - BAND >= 0
    key_valid = jnp.concatenate([band_ok, mem_ok], axis=1)
    bias = jnp.repeat(jnp.where(key_valid, 0.0, masked_score).astype(f32), TOK, axis=1)

    asked_rank = jnp.cumsum(asked, axis=1) - 1
    places = jnp.arange(CAP, dtype=jnp.int32)[None, :, None]
    chosen = (asked[:, None, :] > 0) & (asked_rank[:, None, :] == places)
    frame_no = jnp.arange(FRAMES, dtype=jnp.int32)[None, None, :]
    pick = jnp.sum(jnp.where(chosen, frame_no, 0), axis=2).reshape(-1)
    pick_add = jnp.where(jnp.any(chosen, axis=2).reshape(-1), pick, FRAMES)

    outgoing = named_frames(pick, keyval)
    slots = slots_exchange(outgoing)
    owns, passed, returned = [], [], []
    written, first = (), 0
    for count in SPLIT:
        *written, own_g, rim_g, dslot_g = attend(
            read, add, bias, queries, grad_heads, keyval, before, slots, first, count, written
        )
        passed.append(from_behind(rim_g, -1))
        returned.append(slots_exchange(dslot_g))
        owns.append(own_g)
        first += count

    heads_out, grad_query = written
    sent = partial_call([(x_t, grad_query), (heads_out, cot)], sending)
    got = other_core(sent)
    kept = partial_call([(x_t, grad_query), (heads_out, cot)], keeping, got)
    sum_qo = over_chips(kept)
    share_qo = over_blocks(combined([sum_qo]))
    mine_qo, other_qo = everyone(share_qo, share_qo.shape[0], keeping)
    attended = jnp.dot(heads_out, w_output, preferred_element_type=f32).astype(bf16)
    dkvs, sums = [], []
    for g, count in enumerate(SPLIT):
        last = g == len(SPLIT) - 1
        dkv = collect(pick_add, owns[g], passed[g], returned[g])
        dkvs.append(dkv)
        sent = partial_call([(x_t, dkv)], sending, by_chip=not last)
        got = other_core(sent)
        kept = partial_call([(x_t, dkv)], keeping, got, not last, sums if last else ())
        if not last:
            sums.append(over_chips(kept))
    late = summed(exchange(kept))
    grad_input = input_gradient(grad_query, dkvs, w_query, w_key, w_value)
    ordered = sum(sums[0][0].shape[1] for sums in sums)
    mine, other = everyone(late, ordered, keeping)
    shard, o_shard = model_width // BLOCKS, inner // BLOCKS
    piece, o_piece = shard // CHIPS, o_shard // CHIPS
    qo_places, kv_places = [], []
    for c in range(2):
        found = []
        for j in range(CHIPS):
            at = j * share_qo.shape[0]
            for k, rows, width in ((0, piece, half), (1, o_piece, model_width // 2)):
                for column in range(c * width, (c + 1) * width, LANES):
                    found.append((k, j * rows, column, at, rows))
                    at += rows
        qo_places.append(found)
        found, first = [], sum(SPLIT[:-1])
        for j in range(CHIPS):
            for h in range(first):
                found.append((c, j * piece, h * HEAD, j * ordered + h * piece, piece))
        for h in range(first, HEADS):
            found.append((c, 0, h * HEAD, CHIPS * ordered + (h - first) * shard, shard))
        kv_places.append(found)
    total_q, total_o = assembled(mine_qo, other_qo, keeping, [(shard, inner), (o_shard, model_width)], qo_places
    )
    total_k, total_v = assembled(mine, other, keeping, [(shard, inner)] * 2, kv_places)
    shape = (1, FRAMES, TOK, model_width)
    return (
        attended.reshape(shape),
        grad_input.reshape(shape),
        total_q,
        total_k,
        total_v,
        total_o,
    )


def solution(mesh):
    block = P("roll", "tm", None, None)
    return jax.shard_map(
        step,
        mesh=mesh,
        in_specs=(block, block, P("roll", "tm", None), P(), P(), P(), P()),
        out_specs=(block, block, P("tm", None), P("tm", None), P("tm", None), P("tm", None)),
        check_vma=False,
    )
```

```python
import functools

import jax
import jax.numpy as jnp
from jax import lax
from jax.experimental import pallas as pl
from jax.experimental.pallas import tpu as pltpu
from jax.sharding import PartitionSpec as P


HEADS = 8
HEAD = 128
BAND = 4
MEM = 8
CAP = 3
FRAMES = 8
TOK = 32
BLOCKS = 16
ROWS = FRAMES * TOK
SPLIT = (4, 4)
KEYS = (BAND + 1 + MEM) * TOK
CHIPS = 4
SPARE = BLOCKS * CAP
masked_score = -1e30
f32, bf16 = jnp.float32, jnp.bfloat16
VMEM_LIMIT = 60 * 1024 * 1024


def params(n=1):
    return pltpu.CompilerParams(
        dimension_semantics=("arbitrary",) * n, vmem_limit_bytes=VMEM_LIMIT
    )


def dot_last(left, right):
    return lax.dot_general(left, right, (((1,), (1,)), ((), ())), preferred_element_type=f32)


def dot_first(left, right):
    return lax.dot_general(left, right, (((0,), (0,)), ((), ())), preferred_element_type=f32)


def dot(left, right):
    return lax.dot_general(left, right, (((1,), (0,)), ((), ())), preferred_element_type=f32)


def keyval_body(x_ref, wk_ref, wv_ref, out_ref):
    pieces = []
    for h in range(wk_ref.shape[1] // HEAD):
        pieces += [wk_ref[:, h * HEAD : (h + 1) * HEAD], wv_ref[:, h * HEAD : (h + 1) * HEAD]]
    out_ref[...] = dot(x_ref[...], jnp.concatenate(pieces, axis=1)).astype(bf16)


def keyval_rows(x, w_key, w_value):
    rows, width = x.shape
    cols = 256
    return pl.pallas_call(
        keyval_body,
        grid=(w_key.shape[1] // cols,),
        in_specs=[
            pl.BlockSpec((rows, width), lambda j: (0, 0)),
            pl.BlockSpec((width, cols), lambda j: (0, j)),
            pl.BlockSpec((width, cols), lambda j: (0, j)),
        ],
        out_specs=pl.BlockSpec((rows, 2 * cols), lambda j: (0, j)),
        out_shape=jax.ShapeDtypeStruct((rows, 2 * w_key.shape[1]), bf16),
        compiler_params=params(),
    )(x, w_key, w_value)


def send_body(pick_ref, kv_ref, out_ref, sem):
    def copy(i):
        at = pl.multiple_of(pick_ref[i] * TOK, TOK)
        return pltpu.make_async_copy(
            kv_ref.at[pl.ds(at, TOK), :], out_ref.at[pl.ds(i * TOK, TOK), :], sem.at[i]
        )

    for i in range(BLOCKS * CAP):
        copy(i).start()
    for i in range(BLOCKS * CAP):
        copy(i).wait()


def named_frames(pick, kv, block, width):
    return pl.pallas_call(
        send_body,
        grid_spec=pltpu.PrefetchScalarGridSpec(
            num_scalar_prefetch=1,
            grid=(1,),
            in_specs=[pl.BlockSpec((ROWS, width), lambda i, *_: (0, block))],
            out_specs=pl.BlockSpec(memory_space=pl.ANY),
            scratch_shapes=[pltpu.SemaphoreType.DMA((BLOCKS * CAP,))],
        ),
        out_shape=jax.ShapeDtypeStruct((BLOCKS * CAP * TOK, width), bf16),
        compiler_params=params(),
    )(pick, kv)


def attend_body(
    read_ref, add_ref, bias_ref, q_ref, g_ref, own_ref, prev_ref, slot_ref, *refs
):
    attend_head(
        read_ref, add_ref, bias_ref, q_ref, g_ref, own_ref, prev_ref, slot_ref, *refs[-13:]
    )


def attend_head(
    read_ref, add_ref, bias_ref, q_ref, g_ref, own_ref, prev_ref, slot_ref,
    o_ref, dq_ref, down_ref, rim_ref, dslot_ref,
    acc_own, acc_prev, acc_slot, kv_scr, s_scr, gp_scr, half_scr, ds_scr,
):
    scale = HEAD ** (-0.5)
    acc_own[...] = jnp.zeros_like(acc_own)
    acc_prev[...] = jnp.zeros_like(acc_prev)
    acc_slot[...] = jnp.zeros_like(acc_slot)
    spans = [slice(f * TOK, (f + 1) * TOK) for f in range(FRAMES)]
    for f, rows in enumerate(spans):
        at = 0
        if f < BAND:
            at = (BAND - f) * TOK
            kv_scr[f, :at, :] = prev_ref[f * TOK : BAND * TOK, :]
        kv_scr[f, at : (BAND + 1) * TOK, :] = own_ref[max(f - BAND, 0) * TOK : (f + 1) * TOK, :]
        for m in range(MEM):
            at = pl.multiple_of(read_ref[f * MEM + m] * TOK, TOK)
            kv_scr[f, (BAND + 1 + m) * TOK : (BAND + 2 + m) * TOK, :] = slot_ref[pl.ds(at, TOK), :]
    for f, rows in enumerate(spans):
        s_scr[rows, :] = dot_last(q_ref[rows, :], kv_scr[f, :, :HEAD]) * scale + bias_ref[f : f + 1, :]
        gp_scr[rows, :] = dot_last(g_ref[rows, :], kv_scr[f, :, HEAD:])
    for rows in spans:
        s = s_scr[rows, :]
        gp = gp_scr[rows, :]
        e = jnp.exp(s - jnp.max(s, axis=1, keepdims=True))
        w = e * (1.0 / jnp.sum(e, axis=1, keepdims=True))
        half_scr[rows, :] = w.astype(bf16)
        ds_scr[rows, :] = (w * (gp - jnp.sum(w * gp, axis=1, keepdims=True))).astype(bf16)
    for f, rows in enumerate(spans):
        o_ref[rows, :] = dot(half_scr[rows, :], kv_scr[f, :, HEAD:]).astype(bf16)
        dq_ref[rows, :] = (dot(ds_scr[rows, :], kv_scr[f, :, :HEAD]) * scale).astype(bf16)
    for f, rows in enumerate(spans):
        dk = dot_first(ds_scr[rows, :], q_ref[rows, :]) * scale
        dv = dot_first(half_scr[rows, :], g_ref[rows, :])
        start = 0
        own = slice(max(f - BAND, 0) * TOK, (f + 1) * TOK)
        if f < BAND:
            start = (BAND - f) * TOK
            prev = slice(f * TOK, BAND * TOK)
            acc_prev[prev, :HEAD] += dk[:start]
            acc_prev[prev, HEAD:] += dv[:start]
        acc_own[own, :HEAD] += dk[start : (BAND + 1) * TOK]
        acc_own[own, HEAD:] += dv[start : (BAND + 1) * TOK]
        spots = [pl.multiple_of(add_ref[f * MEM + m] * TOK, TOK) for m in range(MEM)]
        base = (BAND + 1) * TOK
        for d, cols in ((dk, slice(0, HEAD)), (dv, slice(HEAD, 2 * HEAD))):
            olds = [acc_slot[pl.ds(at, TOK), cols] for at in spots]
            for m, at in enumerate(spots):
                acc_slot[pl.ds(at, TOK), cols] = olds[m] + d[base + m * TOK : base + (m + 1) * TOK]
    down_ref[...] = acc_own[...]
    rim_ref[...] = acc_prev[...].astype(bf16)
    dslot_ref[...] = acc_slot[: SPARE * TOK, :].astype(bf16)


def attend(read, add, bias, q, g, own, prev, slots, first, heads, written):
    col = lambda rows, width: pl.BlockSpec((rows, width), lambda h, *_: (0, h))
    src = lambda rows, width: pl.BlockSpec((rows, width), lambda h, *_: (0, h + first))
    return pl.pallas_call(
        attend_body,
        grid_spec=pltpu.PrefetchScalarGridSpec(
            num_scalar_prefetch=2,
            grid=(heads,),
            in_specs=[
                pl.BlockSpec(bias.shape, lambda h, *_: (0, 0)),
                src(ROWS, HEAD), src(ROWS, HEAD),
                src(ROWS, 2 * HEAD), src(BAND * TOK, 2 * HEAD), col(SPARE * TOK, 2 * HEAD),
            ] + [pl.BlockSpec(memory_space=pl.ANY)] * len(written),
            out_specs=[
                src(ROWS, HEAD), src(ROWS, HEAD),
                col(ROWS, 2 * HEAD), col(BAND * TOK, 2 * HEAD), col(SPARE * TOK, 2 * HEAD),
            ],
            scratch_shapes=[
                pltpu.VMEM((ROWS, 2 * HEAD), f32),
                pltpu.VMEM((BAND * TOK, 2 * HEAD), f32),
                pltpu.VMEM(((SPARE + 1) * TOK, 2 * HEAD), f32),
                pltpu.VMEM((FRAMES, KEYS, 2 * HEAD), bf16),
                pltpu.VMEM((ROWS, KEYS), f32),
                pltpu.VMEM((ROWS, KEYS), f32),
                pltpu.VMEM((ROWS, KEYS), bf16),
                pltpu.VMEM((ROWS, KEYS), bf16),
            ],
        ),
        out_shape=[
            jax.ShapeDtypeStruct(q.shape, bf16),
            jax.ShapeDtypeStruct(q.shape, bf16),
            jax.ShapeDtypeStruct((ROWS, 2 * heads * HEAD), f32),
            jax.ShapeDtypeStruct((BAND * TOK, 2 * heads * HEAD), bf16),
            jax.ShapeDtypeStruct((SPARE * TOK, 2 * heads * HEAD), bf16),
        ],
        input_output_aliases={8 + k: k for k in range(len(written))},
        compiler_params=params(),
    )(read, add, bias, q, g, own, prev, slots, *written)


def collect_body(pick_ref, own_ref, rim_ref, back_ref, out_ref, *accs):
    for acc in accs:
        acc[...] = jnp.zeros_like(acc)
    for i in range(BLOCKS * CAP):
        acc = accs[i % len(accs)]
        at = pl.multiple_of(pick_ref[i] * TOK, TOK)
        acc[pl.ds(at, TOK), :] += back_ref[i * TOK : (i + 1) * TOK, :].astype(f32)
    acc = accs[0]
    acc[:ROWS, :] = own_ref[...] + sum(a[:ROWS, :] for a in accs)
    tail = slice((FRAMES - BAND) * TOK, ROWS)
    acc[tail, :] += rim_ref[...].astype(f32)
    for h in range(own_ref.shape[1] // (2 * HEAD)):
        for kind in range(2):
            left = (2 * h + kind) * HEAD
            out_ref[kind, :, h * HEAD : (h + 1) * HEAD] = acc[:ROWS, left : left + HEAD].astype(bf16)


def collect(pick, own, rim, back):
    width = own.shape[1]
    cols = 2 * HEAD
    col = lambda rows, w: pl.BlockSpec((rows, w), lambda h, *_: (0, h))
    return pl.pallas_call(
        collect_body,
        grid_spec=pltpu.PrefetchScalarGridSpec(
            num_scalar_prefetch=1,
            grid=(width // cols,),
            in_specs=[col(ROWS, cols), col(BAND * TOK, cols), col(SPARE * TOK, cols)],
            out_specs=pl.BlockSpec((2, ROWS, cols // 2), lambda h, *_: (0, 0, h)),
            scratch_shapes=[pltpu.VMEM((ROWS + TOK, cols), f32)] * 4,
        ),
        out_shape=jax.ShapeDtypeStruct((2, ROWS, width // 2), bf16),
        compiler_params=params(),
    )(pick, own, rim, back)


LANES = HEAD


def taken(right):
    if right.ndim == 3:
        rows, n = right.shape[1:]
        return n, pl.BlockSpec((None, rows, n), lambda i, s, *_: (s[1], 0, 0))
    rows, n = right.shape
    return n // 2, pl.BlockSpec((rows, n // 2), lambda i, s, *_: (0, s[1]))


def packed_rows(rows, n):
    return rows * n // LANES


def packed(part):
    return jnp.concatenate([part[:, at : at + LANES] for at in range(0, part.shape[1], LANES)], axis=0)


def partial_call(pairs, scalars, got=None, by_chip=True, extra=()):
    per = 8
    steps = BLOCKS // per
    chips = CHIPS if by_chip else 1
    cuts = [taken(right) for _, right in pairs]
    across = [left.shape[0] == right.shape[-2] for left, right in pairs]
    shards = [left.shape[1 if a else 0] // BLOCKS for (left, _), a in zip(pairs, across)]
    height = sum(packed_rows(s // chips, n) for (n, _), s in zip(cuts, shards))
    keep = got is not None

    def body(chip_ref, *refs):
        factors, refs = refs[: 2 * len(pairs)], refs[2 * len(pairs) :]
        totals = refs[-len(pairs) :]
        for k, total in enumerate(totals):
            product = dot_first if across[k] else dot
            total[...] = product(factors[2 * k][...], factors[2 * k + 1][...])

        def write(half):
            for t in range(per):
                for d in range(chips):
                    c = lax.rem(chip_ref[0] + d, CHIPS) if keep and by_chip else d
                    parts = []
                    for total, shard in zip(totals, shards):
                        piece = shard // chips
                        first = t * shard + c * piece
                        if keep and by_chip:
                            first = pl.multiple_of(first, piece)
                        parts.append(packed(total[pl.ds(first, piece), :]))
                    part = parts[0] if len(parts) == 1 else jnp.concatenate(parts, axis=0)
                    if not by_chip:
                        if keep:
                            part = part + refs[0][t].astype(f32)
                        out_ref = refs[-1 - len(totals)]
                        out_ref[t, out_ref.shape[1] - height :, :] = part.astype(bf16)
                    elif keep:
                        part = part + refs[0][c, t].astype(f32)
                        refs[1 + 2 * d + half][t] = part.astype(bf16)
                    else:
                        refs[0][c, t] = part.astype(bf16)

        if keep and by_chip:
            early = pl.program_id(0) < steps // 2
            pl.when(early)(lambda: write(0))
            pl.when(jnp.logical_not(early))(lambda: write(1))
        else:
            write(0)

        def add(half):
            out_ref, at = refs[-1 - len(totals)], 0
            for u, sums in enumerate(extra):
                terms = refs[1 + 6 * u + 3 * half : 4 + 6 * u + 3 * half]
                size = sums[0][0].shape[1]
                for t in range(per):
                    total = sum(term[t].astype(f32) for term in terms)
                    out_ref[t, at : at + size, :] = total.astype(bf16)
                at += size

        if extra:
            for half in range(2):
                pl.when(pl.program_id(0) == half)(functools.partial(add, half))

    if by_chip:
        whole = pl.BlockSpec((CHIPS, per, height, LANES), lambda i, *_: (0, i, 0, 0))
        shape = (CHIPS, BLOCKS, height, LANES)
    else:
        whole = pl.BlockSpec((per, height, LANES), lambda i, *_: (i, 0, 0))
        shape = (BLOCKS, height, LANES)
    in_specs, operands = [], []
    for (left, right), shard, (_, spec), a in zip(pairs, shards, cuts, across):
        if a:
            in_specs += [pl.BlockSpec((left.shape[0], per * shard), lambda i, *_: (0, i)), spec]
        else:
            in_specs += [pl.BlockSpec((per * shard, left.shape[1]), lambda i, *_: (i, 0)), spec]
        operands += [left, right]
    out_specs, out_shape = whole, jax.ShapeDtypeStruct(shape, bf16)
    if keep:
        in_specs.append(whole)
        operands.append(got)
        more = 0
        for sums in extra:
            more += sums[0][0].shape[1]
            for term in (*sums[0], *sums[1]):
                in_specs.append(pl.BlockSpec(term.shape, lambda i, *_: (0, 0, 0)))
                operands.append(term)
        if extra:
            assert steps == 2
            out_specs = pl.BlockSpec((per, more + height, LANES), lambda i, *_: (i, 0, 0))
            out_shape = jax.ShapeDtypeStruct((BLOCKS, more + height, LANES), bf16)
        if by_chip:
            halves = [
                pl.BlockSpec((per, height, LANES), lambda i, *_: (jnp.minimum(i, steps // 2 - 1), 0, 0)),
                pl.BlockSpec((per, height, LANES), lambda i, *_: (jnp.maximum(i - steps // 2, 0), 0, 0)),
            ]
            out_specs = halves * CHIPS
            out_shape = [jax.ShapeDtypeStruct((BLOCKS // 2, height, LANES), bf16)] * (2 * CHIPS)
    return pl.pallas_call(
        body,
        grid_spec=pltpu.PrefetchScalarGridSpec(
            num_scalar_prefetch=1,
            grid=(steps,),
            in_specs=in_specs,
            out_specs=out_specs,
            scratch_shapes=[
                pltpu.VMEM((per * s, n), f32) for (n, _), s in zip(cuts, shards)
            ],
        ),
        out_shape=out_shape,
        compiler_params=params(),
    )(scalars, *operands)


def input_gradient(dq, dkvs, w_query, w_key, w_value):
    rows, inner = dq.shape
    width = w_query.shape[0]
    cut = 512

    def body(dq_ref, wq_ref, wk_ref, wv_ref, *refs):
        total = dot_last(dq_ref[...], wq_ref[...])
        at = 0
        for ref in refs[:-1]:
            n = ref.shape[2]
            for kind, weights in enumerate((wk_ref, wv_ref)):
                total = total + dot_last(ref[kind], weights[:, at : at + n])
            at += n
        refs[-1][...] = total.astype(bf16)

    weights = pl.BlockSpec((cut, inner), lambda j: (j, 0))
    return pl.pallas_call(
        body,
        grid=(width // cut,),
        in_specs=[pl.BlockSpec((rows, inner), lambda j: (0, 0)), weights, weights, weights]
        + [pl.BlockSpec(d.shape, lambda j: (0, 0, 0)) for d in dkvs],
        out_specs=pl.BlockSpec((rows, cut), lambda j: (0, j)),
        out_shape=jax.ShapeDtypeStruct((rows, width), bf16),
        compiler_params=params(),
    )(dq, w_query, w_key, w_value, *dkvs)


def other_core(x):
    return lax.ppermute(x, "roll", [(i, i ^ 1) for i in range(lax.axis_size("roll"))])


def from_behind(block, distance):
    return lax.ppermute(
        block, "tm", [(i - distance, i) for i in range(BLOCKS) if 0 <= i - distance < BLOCKS]
    )


def exchange(x, axis="tm", groups=None):
    return lax.all_to_all(
        x, axis, split_axis=0, concat_axis=0, tiled=True, axis_index_groups=groups
    )


def summed(parts):
    return jnp.sum(parts.astype(f32), axis=0).astype(bf16)


def along_chips(x, d):
    n = 2 * CHIPS
    return lax.ppermute(x, "roll", [(i, (i + 2 * d) % n) for i in range(n)])


def plus(a, b):
    return (a.astype(f32) + b.astype(f32)).astype(bf16)


def over_chips(pieces):
    own0, own1, next0, next1, far0, far1, last0, last1 = pieces
    up, down = along_chips(far0, 1), along_chips(far1, -1)
    from_next, from_last = along_chips(next1, 1), along_chips(last0, -1)
    came0 = along_chips(plus(next0, up), 1)
    came1 = along_chips(plus(last1, down), -1)
    return (own0, from_last, came0), (own1, from_next, came1)


def over_blocks(x):
    return summed(exchange(x))


def combined(parts):
    sizes = [halves[0][0].shape[1] for halves in parts]
    per = BLOCKS // 2

    def body(*refs):
        out_ref = refs[-1]

        def write(half):
            at = 0
            for u, size in enumerate(sizes):
                terms = refs[6 * u + 3 * half : 6 * u + 3 * half + 3]
                out_ref[:, at : at + size, :] = sum(term[...].astype(f32) for term in terms).astype(bf16)
                at += size

        for half in range(2):
            pl.when(pl.program_id(0) == half)(functools.partial(write, half))

    operands = [term for halves in parts for terms in halves for term in terms]
    return pl.pallas_call(
        body,
        grid=(2,),
        in_specs=[pl.BlockSpec(term.shape, lambda i: (0, 0, 0)) for term in operands],
        out_specs=pl.BlockSpec((per, sum(sizes), LANES), lambda i: (i, 0, 0)),
        out_shape=jax.ShapeDtypeStruct((BLOCKS, sum(sizes), LANES), bf16),
        compiler_params=params(),
    )(*operands)


def everyone(x, ordered, scalars):
    came = [x] + [along_chips(x, d) for d in range(1, CHIPS)]
    rows = x.shape[0]

    def body(s_ref, *refs):
        out_ref = refs[-1]
        for d in range(CHIPS):
            at = pl.multiple_of(lax.rem(s_ref[0] + CHIPS - d, CHIPS) * ordered, ordered)
            out_ref[pl.ds(at, ordered), :] = refs[d][:ordered, :]
        if ordered < rows:
            total = refs[0][ordered:, :].astype(f32)
            for d in range(1, CHIPS):
                total = total + refs[d][ordered:, :].astype(f32)
            out_ref[CHIPS * ordered :, :] = total.astype(bf16)

    height = CHIPS * ordered + rows - ordered
    whole = lambda n: pl.BlockSpec((n, LANES), lambda i, *_: (0, 0))
    mine = pl.pallas_call(
        body,
        grid_spec=pltpu.PrefetchScalarGridSpec(
            num_scalar_prefetch=1, grid=(1,), in_specs=[whole(rows)] * CHIPS, out_specs=whole(height)
        ),
        out_shape=jax.ShapeDtypeStruct((height, LANES), bf16),
        compiler_params=params(),
    )(scalars, *came)
    other = other_core(mine)
    return mine, other


def assembled(mine, other, scalars, shapes, places):
    height = mine.shape[0]

    def body(s_ref, mine_ref, other_ref, *out_refs):
        def write(sources):
            for core, source in enumerate(sources):
                for k, row, column, at, rows in places[core]:
                    out_refs[k][row : row + rows, column : column + LANES] = source[at : at + rows, :].astype(f32)

        pl.when(s_ref[1] == 0)(lambda: write((mine_ref, other_ref)))
        pl.when(s_ref[1] == 1)(lambda: write((other_ref, mine_ref)))

    whole = lambda shape: pl.BlockSpec(shape, lambda i, *_: (0, 0))
    return pl.pallas_call(
        body,
        grid_spec=pltpu.PrefetchScalarGridSpec(
            num_scalar_prefetch=1, grid=(1,),
            in_specs=[whole((height, LANES))] * 2, out_specs=[whole(s) for s in shapes],
        ),
        out_shape=[jax.ShapeDtypeStruct(s, f32) for s in shapes],
        compiler_params=params(),
    )(scalars, mine, other)


def slots_exchange(x):
    return exchange(x.reshape(BLOCKS, CAP * TOK, x.shape[1])).reshape(x.shape)


def step(inputs, cotangent, memory_lists, w_query, w_key, w_value, w_output):
    model_width = inputs.shape[-1]
    inner = w_query.shape[1]
    half = inner // 2
    position = lax.axis_index("tm")
    core = lax.axis_index("roll") % 2
    chip = lax.axis_index("roll") // 2
    keeping = jnp.stack([chip, core]).astype(jnp.int32)
    sending = jnp.stack([chip, 1 - core]).astype(jnp.int32)
    x = inputs.reshape(ROWS, model_width)
    cot = cotangent.reshape(ROWS, model_width)
    x_t = x.T
    recalled = memory_lists[0]
    first_frame = position * FRAMES

    targets = jnp.arange(BLOCKS * FRAMES, dtype=jnp.int32)
    wanted = jnp.any(recalled.reshape(-1, 1) == targets[None, :], axis=0)
    wanted = wanted.astype(jnp.int32).reshape(BLOCKS, FRAMES)
    asked = exchange(wanted)

    x_before = from_behind(x[(FRAMES - BAND) * TOK :], 1)
    keyval = keyval_rows(x, w_key, w_value)
    before = keyval_rows(x_before, w_key, w_value)
    queries = jnp.dot(x, w_query, preferred_element_type=f32).astype(bf16)
    grad_heads = dot_last(cot, w_output).astype(bf16)

    slot_rank = jnp.cumsum(wanted, axis=1) - 1
    slot_table = (jnp.arange(BLOCKS, dtype=jnp.int32)[:, None] * CAP + slot_rank).reshape(-1)
    mem_ok = recalled >= 0
    flat = jnp.where(mem_ok, recalled, 0).reshape(-1)
    hit = flat[:, None] == targets[None, :]
    slot_ids = jnp.sum(jnp.where(hit, slot_table[None, :], 0), axis=1)
    ok_flat = mem_ok.reshape(-1)
    read = jnp.clip(jnp.where(ok_flat, slot_ids, 0), 0, SPARE - 1)
    add = jnp.clip(jnp.where(ok_flat, slot_ids, SPARE), 0, SPARE)
    band_index = (
        jnp.arange(FRAMES, dtype=jnp.int32)[:, None] + jnp.arange(BAND + 1, dtype=jnp.int32)[None, :]
    )
    band_ok = first_frame + band_index - BAND >= 0
    key_valid = jnp.concatenate([band_ok, mem_ok], axis=1)
    bias = jnp.repeat(jnp.where(key_valid, 0.0, masked_score).astype(f32), TOK, axis=1)

    asked_rank = jnp.cumsum(asked, axis=1) - 1
    places = jnp.arange(CAP, dtype=jnp.int32)[None, :, None]
    chosen = (asked[:, None, :] > 0) & (asked_rank[:, None, :] == places)
    frame_no = jnp.arange(FRAMES, dtype=jnp.int32)[None, None, :]
    pick = jnp.sum(jnp.where(chosen, frame_no, 0), axis=2).reshape(-1)
    pick_add = jnp.where(jnp.any(chosen, axis=2).reshape(-1), pick, FRAMES)

    slots, first = [], 0
    for count in SPLIT:
        assert first % count == 0
        outgoing = named_frames(pick, keyval, first // count, 2 * HEAD * count)
        slots.append(slots_exchange(outgoing))
        first += count
    owns, passed, returned = [], [], []
    written, first = (), 0
    for g, count in enumerate(SPLIT):
        *written, own_g, rim_g, dslot_g = attend(
            read, add, bias, queries, grad_heads, keyval, before, slots[g], first, count, written
        )
        passed.append(from_behind(rim_g, -1))
        returned.append(slots_exchange(dslot_g))
        owns.append(own_g)
        first += count

    heads_out, grad_query = written
    sent = partial_call([(x_t, grad_query), (heads_out, cot)], sending)
    got = other_core(sent)
    kept = partial_call([(x_t, grad_query), (heads_out, cot)], keeping, got)
    sum_qo = over_chips(kept)
    share_qo = over_blocks(combined([sum_qo]))
    mine_qo, other_qo = everyone(share_qo, share_qo.shape[0], keeping)
    attended = jnp.dot(heads_out, w_output, preferred_element_type=f32).astype(bf16)
    dkvs, sums = [], []
    for g, count in enumerate(SPLIT):
        last = g == len(SPLIT) - 1
        dkv = collect(pick_add, owns[g], passed[g], returned[g])
        dkvs.append(dkv)
        sent = partial_call([(x_t, dkv)], sending, by_chip=not last)
        got = other_core(sent)
        kept = partial_call([(x_t, dkv)], keeping, got, not last, sums if last else ())
        if not last:
            sums.append(over_chips(kept))
    late = summed(exchange(kept))
    grad_input = input_gradient(grad_query, dkvs, w_query, w_key, w_value)
    ordered = sum(sums[0][0].shape[1] for sums in sums)
    mine, other = everyone(late, ordered, keeping)
    shard, o_shard = model_width // BLOCKS, inner // BLOCKS
    piece, o_piece = shard // CHIPS, o_shard // CHIPS
    qo_places, kv_places = [], []
    for c in range(2):
        found = []
        for j in range(CHIPS):
            at = j * share_qo.shape[0]
            for k, rows, width in ((0, piece, half), (1, o_piece, model_width // 2)):
                for column in range(c * width, (c + 1) * width, LANES):
                    found.append((k, j * rows, column, at, rows))
                    at += rows
        qo_places.append(found)
        found, first = [], sum(SPLIT[:-1])
        for j in range(CHIPS):
            for h in range(first):
                found.append((c, j * piece, h * HEAD, j * ordered + h * piece, piece))
        for h in range(first, HEADS):
            found.append((c, 0, h * HEAD, CHIPS * ordered + (h - first) * shard, shard))
        kv_places.append(found)
    total_q, total_o = assembled(mine_qo, other_qo, keeping, [(shard, inner), (o_shard, model_width)], qo_places
    )
    total_k, total_v = assembled(mine, other, keeping, [(shard, inner)] * 2, kv_places)
    shape = (1, FRAMES, TOK, model_width)
    return (
        attended.reshape(shape),
        grad_input.reshape(shape),
        total_q,
        total_k,
        total_v,
        total_o,
    )


def solution(mesh):
    block = P("roll", "tm", None, None)
    return jax.shard_map(
        step,
        mesh=mesh,
        in_specs=(block, block, P("roll", "tm", None), P(), P(), P(), P()),
        out_specs=(block, block, P("tm", None), P("tm", None), P("tm", None), P("tm", None)),
        check_vma=False,
    )
```
